128 devices in a mesh: attn: 4 (over x), expert: 32 (over z, y, core).
Axes of the slice: x: 4, y: 4, z: 4, core: 2. Of those that a mesh axis runs over, the one named last changes fastest.
Arguments:
- tokens: bfloat16 [4096, 2880], P(('attn', 'expert')), may hold values from -6 to 6
- expert_ids: int32 [4096, 4], P(('attn', 'expert')), may hold values from 0 to 31, all different within a row; in each aligned block of 32 rows (0 to 31, 32 to 63, ...) at most 12 rows name the same one
- gate_probs: float32 [4096, 4], P(('attn', 'expert')), may hold values from 0.05 to 0.6
- shed_blocks: int32 [32], replicated, may hold values from 0 to 4, as said below
- partner: int32 [32], replicated, may hold values from 0 to 31, as said below
- gate_weight: bfloat16 [32, 2880, 2880], P('expert', None, 'attn'), may hold values from -0.109375 to 0.109375
- up_weight: bfloat16 [32, 2880, 2880], P('expert', None, 'attn'), may hold values from -0.109375 to 0.109375
- down_weight: bfloat16 [32, 2880, 2880], P('expert', 'attn'), may hold values from -0.109375 to 0.109375
Outputs:
- moe_out: bfloat16 [4096, 2880], P(('attn', 'expert'))
The draws below stay inside these ranges and needn't reach their ends.
Inputs may be any that keep to these rules, and one draw needn't show every extreme that they name: `expert_ids`: in the rows of one device, no expert is named by more than 12 rows; the 4 experts of a token differ. `shed_blocks`: some expert has exactly 4. partner pairs the experts: partner[partner[e]] = e and partner[e] != e.
All inputs are finite; a program needn't handle non-finite values.
Results may differ from the reference program's by a relative error of at most 0.0081.
Values may be sent and summed in bfloat16 or wider, within the bound.
No kernel may reach another device: no remote copies, remote signals or barrier semaphores. Data moves between devices by JAX's collectives and lax.ppermute only.
A program may use at most 128 MiB of HBM per device.

```python
import math
import jax
import jax.numpy as jnp
import numpy as np
from jax import lax

D = 2880
FF = 2880
TOP = 4
SHED_MOST = 4
TOK_DEV = 32
TOKENS = 4096
EXPERTS = 32
MOST = 12
N_ATTN = 4


def draw_shed_blocks(key, part):
    first = jax.random.fold_in(key, 11)
    second = jax.random.fold_in(key, 12)
    values = jax.random.randint(first, (EXPERTS,), 0, SHED_MOST + 1).astype(jnp.int32)
    chosen = jax.random.randint(second, (), 0, EXPERTS)
    return values.at[chosen].set(SHED_MOST).astype(jnp.int32)


def draw_partner(key, part):
    shuffled = jax.random.permutation(jax.random.fold_in(key, 21), EXPERTS).astype(jnp.int32)
    left_side = shuffled[0::2]
    right_side = shuffled[1::2]
    paired = jnp.zeros((EXPERTS,), jnp.int32).at[left_side].set(right_side).at[right_side].set(left_side)
    return paired.astype(jnp.int32)


def block_scale(stream_key, shape, pieces, least, high):
    factor_of, own = 1.0, jax.random.fold_in(stream_key, 6)
    for dim, shards_of in pieces:
        draws = jnp.exp(jax.random.uniform(jax.random.fold_in(own, dim), (shards_of,), jnp.float32, least / len(pieces), high / len(pieces)))
        factor_of = factor_of * jnp.repeat(draws, shape[dim] // shards_of).reshape([-1 if axis == dim else 1 for axis in range(len(shape))])
    return factor_of


def routed_block(key, own, number, rows, number_of, top, most, skew):
    ranking = jax.random.permutation(key, number_of)
    heavy_load, common = load_shares(number_of, rows * top, most, skew, True), load_shares(number_of, rows * top, most, skew, False)
    places = jnp.arange(number_of)

    def named(lengths, rotation):
        used = int((lengths > 0).sum())
        fixed = max(1, used // 4)
        shifted = fixed + (places - fixed + rotation * (used - fixed)) % max(1, number_of - fixed)
        return jnp.zeros((number_of,), jnp.int32).at[ranking[jnp.where(places < fixed, places, shifted)]].set(jnp.asarray(lengths, jnp.int32))

    lengths = jnp.where(number % 4 == 0, named(heavy_load, number // 4), named(common, number - number // 4 - 1))
    mixed = jax.random.permutation(jax.random.fold_in(own, 3), number_of)
    source_of, receiver = mixed[0:number_of // 2 * 2:2], mixed[1:number_of // 2 * 2:2]
    margin = jnp.minimum(lengths[source_of] - 1, most - lengths[receiver]) // 2
    margin = jnp.where((source_of == ranking[0]) | (receiver == ranking[0]) | (lengths[receiver] == 0), 0, jnp.maximum(margin, 0))
    shifted = jax.random.randint(jax.random.fold_in(own, 4), (number_of // 2,), 0, 1 << 20) % (margin + 1)
    lengths = lengths.at[source_of].add(-shifted).at[receiver].add(shifted)
    labels = jnp.searchsorted(jnp.cumsum(lengths), jnp.arange(rows * top), side="right").astype(jnp.int32)
    listing = labels.reshape(top, rows).T
    listing = listing[jax.random.permutation(jax.random.fold_in(own, 1), rows)]
    rotation = jax.random.randint(jax.random.fold_in(own, 2), (rows, 1), 0, top)
    return jnp.take_along_axis(listing, (jnp.arange(top)[None, :] + rotation) % top, axis=1)


def load_shares(amount, total, reach, slope, full):
    portions = [(1 << 20) // math.isqrt(standing ** slope) + 1 for standing in range(1, amount + 1)]
    largest = reach if full else min(reach, max(-(-total // amount), total * portions[0] // sum(portions)))
    least = 1 if total - largest >= amount - 1 else 0
    holding, spare = [largest] + [least] * (amount - 1), total - largest - least * (amount - 1)
    while spare > 0:
        free = [i for i in range(1, amount) if holding[i] < largest] or [i for i in range(1, amount) if holding[i] < reach]
        pool, remaining = sum([portions[i] for i in free]), spare
        for i in free:
            addition = min(reach - holding[i], max(1, remaining * portions[i] // pool), spare)
            holding[i] = holding[i] + addition
            spare = spare - addition
    return np.array(holding)


def gaussian(key, extent, scale, most, cuts=(), kind=jnp.bfloat16):
    drawn = jax.random.normal(key, extent, jnp.float32) * scale
    if len(cuts) > 0:
        drawn = block_scale(key, extent, cuts, -0.22, 0.18) * drawn
    return jnp.clip(drawn, min=-most, max=most).astype(kind)


def setup_inputs(seed: int = 0) -> dict:
    streams_of = jax.random.split(jax.random.key(seed), 9)
    tokens = gaussian(streams_of[0], (TOKENS, D), 1.0, 6.0, ((0, 128),))
    expert_ids_keys = jax.random.split(jax.random.fold_in(streams_of[1], 1), TOKENS // TOK_DEV)
    expert_ids_turns = jax.random.permutation(jax.random.fold_in(streams_of[1], 3), TOKENS // TOK_DEV)
    expert_ids = jax.vmap(lambda own, number: routed_block(jax.random.fold_in(streams_of[1], 2), own, number, TOK_DEV, EXPERTS, TOP, MOST, 2))(expert_ids_keys, expert_ids_turns).reshape((TOKENS, TOP))
    gate_probs = jnp.clip(jnp.exp(math.log(0.6) - 2.4849067 * jax.random.uniform(streams_of[2], (TOKENS, TOP), jnp.float32) ** block_scale(streams_of[2], (TOKENS, TOP), ((0, 128),), -0.2, 0.2)), 0.05, 0.6)
    shed_blocks = draw_shed_blocks(jax.random.fold_in(streams_of[8], 71), 0)
    partner = draw_partner(jax.random.fold_in(streams_of[8], 71), 0)
    gate_weight = gaussian(streams_of[5], (EXPERTS, D, FF), D ** -0.5, 0.109375, ((0, 32), (2, 4)))
    up_weight = gaussian(streams_of[6], (EXPERTS, D, FF), D ** -0.5, 0.109375, ((0, 32), (2, 4)))
    down_weight = gaussian(streams_of[7], (EXPERTS, FF, D), FF ** -0.5, 0.109375, ((0, 32), (1, 4)))
    return {"tokens": tokens, "expert_ids": expert_ids, "gate_probs": gate_probs, "shed_blocks": shed_blocks, "partner": partner, "gate_weight": gate_weight, "up_weight": up_weight, "down_weight": down_weight}


SWISH_SCALE = 1.702


def activate(rows, gate_w, up_w):
    gate_part = jnp.dot(rows, gate_w, preferred_element_type=jnp.float32)
    up_part = jnp.dot(rows, up_w, preferred_element_type=jnp.float32)
    return (gate_part * jax.nn.sigmoid(SWISH_SCALE * gate_part) * (up_part + 1.0)).astype(jnp.bfloat16)


def reference(tokens, expert_ids, gate_probs, shed_blocks, partner, gate_weight, up_weight, down_weight):
    capacity = TOK_DEV * TOP * N_ATTN
    block_size = capacity // 8
    flat_ids = expert_ids.reshape(-1).astype(jnp.int32)
    onehot = (flat_ids[:, None] == jnp.arange(EXPERTS, dtype=jnp.int32)[None, :]).astype(jnp.int32)
    global_rank = jnp.sum((jnp.cumsum(onehot, axis=0) - onehot) * onehot, axis=1).astype(jnp.int32)
    limit = (capacity - block_size * shed_blocks[partner]).astype(jnp.int32)
    own_limit = limit[flat_ids]
    own_partner = partner[flat_ids].astype(jnp.int32)
    native = global_rank < own_limit
    borrowed = jnp.logical_and(jnp.logical_not(native), global_rank < own_limit + block_size * shed_blocks[flat_ids])
    target = jnp.where(native, flat_ids, jnp.where(borrowed, own_partner, -1)).astype(jnp.int32)
    slot_index = jnp.where(native, global_rank, limit[own_partner] + global_rank - own_limit).astype(jnp.int32)
    usable = target >= 0
    flat_index = jnp.where(usable, target * capacity + slot_index, EXPERTS * capacity).astype(jnp.int32)
    token_rows = jnp.repeat(tokens, TOP, axis=0)
    slot_rows = jnp.zeros((EXPERTS * capacity, D), jnp.bfloat16).at[flat_index].set(token_rows, mode="drop")
    slot_rows = slot_rows.reshape(EXPERTS, capacity, D)
    slot_place = jnp.arange(capacity, dtype=jnp.int32)

    def expert_layer(operands):
        rows, gate_w, up_w, down_w, other, bound = operands
        hidden_own = activate(rows, gate_w, up_w)
        hidden_other = activate(rows, gate_weight[other], up_weight[other])
        out_own = jnp.dot(hidden_own, down_w, preferred_element_type=jnp.float32)
        out_other = jnp.dot(hidden_other, down_weight[other], preferred_element_type=jnp.float32)
        keep = (slot_place < bound)[:, None]
        return jnp.where(keep, out_own, out_other).astype(jnp.bfloat16)

    expert_out = lax.map(expert_layer, (slot_rows, gate_weight, up_weight, down_weight, partner.astype(jnp.int32), limit))
    picked = expert_out.reshape(EXPERTS * capacity, D)[jnp.minimum(flat_index, EXPERTS * capacity - 1)]
    weights = jnp.where(usable, gate_probs.reshape(-1), 0.0).astype(jnp.float32)
    mixed = picked.astype(jnp.float32) * weights[:, None]
    return mixed.reshape(TOKENS, TOP, D).sum(axis=1).astype(jnp.bfloat16)
```

```python
import jax
import jax.numpy as jnp
from jax import lax
from jax.experimental import pallas as pl
from jax.experimental.pallas import tpu as pltpu
from jax.sharding import Mesh
from jax.sharding import PartitionSpec as P

SHED_MOST = 4
ATTN_EXPERT = ("attn", "expert_0", "expert_1", "expert_2")
EXPERT = ("expert_0", "expert_1", "expert_2")
SWISH_SCALE = 1.702
BF = jnp.bfloat16
F32 = jnp.float32
META = 16


def iota(shape, dim):
    return lax.broadcasted_iota(jnp.int32, shape, dim)


def pick_kernel(tok, groups, rows_out, width, top, x_ref, par_ref, g_ref, rank_ref, prob_ref):
    span = groups * tok
    blocks = x_ref.shape[0] // span
    total = x_ref.shape[0]
    me, bound = par_ref[0], par_ref[1]
    start = width // 128 * 128
    tail = x_ref[:, start:]
    lanes = tail.shape[1]
    choose = (iota((META, lanes), 1) == iota((META, lanes), 0) + (width - start)).astype(BF)
    meta = lax.dot_general(choose, tail, (((1,), (1,)), ((), ())), preferred_element_type=F32)
    hit = meta[0:top] == me.astype(F32)
    prob = meta[top : 2 * top] + meta[2 * top : 3 * top] + meta[3 * top : 4 * top]
    prob = jnp.sum(jnp.where(hit, prob, 0.0), axis=0, keepdims=True)
    named = jnp.sum(jnp.where(hit, 1.0, 0.0), axis=0, keepdims=True)
    named = jnp.concatenate([named[:, b * span : (b + 1) * span] for b in range(blocks)], axis=0)
    prob = jnp.concatenate([prob[:, b * span : (b + 1) * span] for b in range(blocks)], axis=0)
    r, c = iota((span, span), 0), iota((span, span), 1)
    same = (r // tok) == (c // tok)
    inside = jnp.logical_and(same, r < c).astype(BF)
    less = ((r // tok) < (c // tok)).astype(BF)
    m = named.astype(BF)
    dot = lambda a, b: jnp.dot(a, b, preferred_element_type=F32)
    rb, cb = iota((blocks, blocks), 0), iota((blocks, blocks), 1)
    rank = dot(m, inside)
    rank += dot((cb < rb).astype(BF), dot(m, same.astype(BF)).astype(BF))
    rank += dot(jnp.ones((blocks, blocks), BF), dot(m, less).astype(BF))
    keep = jnp.logical_and(named > 0.5, rank < bound.astype(F32))
    slot = jnp.where(keep, rank, -1.0)
    rank_ref[...] = slot.T
    prob_ref[...] = prob.T
    place = iota((rows_out, span), 0).astype(F32)
    per = 8
    for step in range(blocks // per):
        hot = jnp.concatenate(
            [
                jnp.where(slot[b : b + 1] == place, 1.0, 0.0).astype(BF)
                for b in range(step * per, (step + 1) * per)
            ],
            axis=1,
        )
        part = dot(hot, x_ref[step * per * span : (step + 1) * per * span, :width])
        if step == 0:
            acc = part
        else:
            acc += part
    g_ref[...] = acc.astype(BF)


def ffn_kernel(x_ref, wg_ref, wu_ref, wd_ref, o_ref):
    parts, _, width = x_ref.shape
    gate = up = None
    for b in range(parts):
        x = x_ref[b]
        g = jnp.dot(x, wg_ref[b * width : (b + 1) * width, :], preferred_element_type=F32)
        u = jnp.dot(x, wu_ref[b * width : (b + 1) * width, :], preferred_element_type=F32)
        gate, up = (g, u) if b == 0 else (gate + g, up + u)
    hidden = (gate * jax.nn.sigmoid(SWISH_SCALE * gate) * (up + 1.0)).astype(BF)
    for b in range(parts):
        o_ref[b] = jnp.dot(hidden, wd_ref[b], preferred_element_type=F32).astype(BF)


def place_kernel(y_ref, rank_ref, prob_ref, z_ref):
    span, blocks = rank_ref.shape
    rows = y_ref.shape[0]
    place = iota((span, rows), 1).astype(F32)
    lane = iota((span, blocks), 1)

    def step(b, carry):
        mine = lane == b
        slot = jnp.sum(jnp.where(mine, rank_ref[...], 0.0), axis=1, keepdims=True)
        prob = jnp.sum(jnp.where(mine, prob_ref[...], 0.0), axis=1, keepdims=True)
        hot = jnp.where(slot == place, 1.0, 0.0).astype(BF)
        rows_b = jnp.dot(hot, y_ref[...], preferred_element_type=F32) * prob
        z_ref[pl.ds(pl.multiple_of(b * span, span), span), :] = rows_b.astype(BF)
        return carry

    lax.fori_loop(0, blocks, step, 0)


VMEM = pl.BlockSpec(memory_space=pltpu.VMEM)
SMEM = pl.BlockSpec(memory_space=pltpu.SMEM)


def on_device(
    tokens, expert_ids, gate_probs, shed_blocks, partner, gate_weight, up_weight, down_weight
):
    tok, model = tokens.shape
    top = expert_ids.shape[1]
    experts = shed_blocks.shape[0]
    groups = lax.axis_size("attn")
    width = model // groups
    capacity = tok * top * groups
    block = capacity // 8
    slots = capacity + block * SHED_MOST
    span = groups * tok
    total = span * experts
    me = lax.axis_index(EXPERT)
    mine = shed_blocks[me]
    bound = capacity - block * shed_blocks[partner[me]] + block * mine
    par = jnp.stack([me, bound]).astype(jnp.int32)
    high = lax.reduce_precision(gate_probs, 8, 7)
    rest = gate_probs - high
    middle = lax.reduce_precision(rest, 8, 7)
    meta = jnp.concatenate([expert_ids.astype(F32), high, middle, rest - middle], axis=1).astype(BF)
    columns = jnp.stack(
        [
            jnp.concatenate([tokens[:, b * width : (b + 1) * width], meta], axis=1)
            for b in range(groups)
        ]
    )
    mixed = lax.all_to_all(columns, "attn", 0, 0, tiled=True).reshape(span, width + META)
    everyone = lax.all_gather(mixed, EXPERT, tiled=True)

    picked, rank, prob = pl.pallas_call(
        lambda *refs: pick_kernel(tok, groups, slots, width, top, *refs),
        out_shape=(
            jax.ShapeDtypeStruct((slots, width), BF),
            jax.ShapeDtypeStruct((span, experts), F32),
            jax.ShapeDtypeStruct((span, experts), F32),
        ),
        in_specs=[VMEM, SMEM],
        out_specs=(VMEM, VMEM, VMEM),
        cost_estimate=pl.CostEstimate(
            flops=2 * slots * total * width, bytes_accessed=2 * total * width, transcendentals=0
        ),
        name="pick",
    )(everyone, par)

    rows = lax.all_gather(picked, "attn", tiled=True).reshape(groups, slots, width)
    down = down_weight[0].reshape(-1, groups, width).transpose(1, 0, 2)
    units = gate_weight.shape[2]
    tile = 256
    partial = pl.pallas_call(
        ffn_kernel,
        grid=(slots // tile,),
        out_shape=jax.ShapeDtypeStruct((groups, slots, width), BF),
        in_specs=[
            pl.BlockSpec((groups, tile, width), lambda i: (0, i, 0)),
            pl.BlockSpec((model, units), lambda i: (0, 0)),
            pl.BlockSpec((model, units), lambda i: (0, 0)),
            pl.BlockSpec((groups, units, width), lambda i: (0, 0, 0)),
        ],
        out_specs=pl.BlockSpec((groups, tile, width), lambda i: (0, i, 0)),
        cost_estimate=pl.CostEstimate(
            flops=6 * slots * model * units, bytes_accessed=6 * model * units, transcendentals=0
        ),
        name="ffn",
    )(rows, gate_weight[0], up_weight[0], down)
    summed = lax.psum_scatter(
        partial.reshape(groups * slots, width), "attn", scatter_dimension=0, tiled=True
    )
    spread = pl.pallas_call(
        place_kernel,
        out_shape=jax.ShapeDtypeStruct((total, width), BF),
        in_specs=[VMEM, VMEM, VMEM],
        out_specs=VMEM,
        cost_estimate=pl.CostEstimate(
            flops=2 * slots * total * width, bytes_accessed=2 * total * width, transcendentals=0
        ),
        name="place",
    )(summed, rank, prob)
    home = lax.psum_scatter(spread, EXPERT, scatter_dimension=0, tiled=True)
    back = lax.all_to_all(home.reshape(groups, tok, width), "attn", 0, 0, tiled=True)
    return back.transpose(1, 0, 2).reshape(tok, model)


def solution(mesh):
    split = Mesh(
        mesh.devices.reshape(mesh.shape["attn"], 4, 4, 2),
        ("attn", "expert_0", "expert_1", "expert_2"),
    )
    return jax.shard_map(
        on_device,
        mesh=split,
        in_specs=(
            P(ATTN_EXPERT, None),
            P(ATTN_EXPERT, None),
            P(ATTN_EXPERT, None),
            P(),
            P(),
            P(EXPERT, None, "attn"),
            P(EXPERT, None, "attn"),
            P(EXPERT, "attn", None),
        ),
        out_specs=P(ATTN_EXPERT, None),
        check_vma=False,
    )
```

```python
import jax
import jax.numpy as jnp
from jax import lax
from jax.experimental import pallas as pl
from jax.experimental.pallas import tpu as pltpu
from jax.sharding import Mesh
from jax.sharding import PartitionSpec as P

SHED_MOST = 4
ATTN_EXPERT = ("attn", "expert_0", "expert_1", "expert_2")
EXPERT = ("expert_0", "expert_1", "expert_2")
SWISH_SCALE = 1.702
BF = jnp.bfloat16
F32 = jnp.float32

def iota(shape, dim):
    return lax.broadcasted_iota(jnp.int32, shape, dim)


def dot(a, b, dims=((1,), (0,))):
    return lax.dot_general(a, b, (dims, ((), ())), preferred_element_type=F32)


def send_kernel(tok, most, width, top, experts, x_ref, s_ref, r_ref):
    span = x_ref.shape[0]
    per = span // tok * most
    x = x_ref[...]
    ids = x[:, width : width + top].astype(F32)
    lane = iota((span, experts), 1).astype(F32)
    named = [ids[:, k : k + 1] == lane for k in range(top)]
    hits = jnp.where(named[0], 1.0, 0.0)
    for k in range(1, top):
        hits += jnp.where(named[k], 1.0, 0.0)
    r, c = iota((span, span), 0), iota((span, span), 1)
    before = jnp.logical_and(r // tok == c // tok, c < r).astype(BF)
    order = dot(before, hits.astype(BF))
    group = (iota((span, 1), 0) // tok * most).astype(F32)
    place = iota((span, experts * per), 1).astype(F32)
    hot = None
    for k in range(top):
        seat = jnp.sum(jnp.where(named[k], order, 0.0), axis=1, keepdims=True)
        seat = seat + ids[:, k : k + 1] * per + group
        r_ref[:, k : k + 1] = seat
        here = jnp.where(seat == place, 1.0, 0.0)
        hot = here if k == 0 else hot + here
    s_ref[...] = dot(hot.astype(BF), x, ((0,), (0,))).astype(BF)


def pick_kernel(most, width, flag, groups, x_ref, par_ref, g_ref, slot_ref):
    came, slots = x_ref.shape[0], g_ref.shape[1]
    per = groups * most
    blocks = came // per
    bound = par_ref[0].astype(F32)
    start = width // 128 * 128
    tail = x_ref[:, start:]
    lanes = tail.shape[1]
    choose = (iota((8, lanes), 1) == flag - start).astype(BF)
    flags = dot(choose, tail, ((1,), (1,)))[0:1]
    row = iota((1, came), 1)
    group, order = row % per // most, (row % most).astype(F32)
    owner = iota((blocks, came), 0) == iota((blocks, came), 1) // per
    split = jnp.where(owner, flags, 0.0).astype(BF)
    member = iota((came, 128), 0) % per // most == iota((came, 128), 1)
    counts = dot(split, member.astype(BF)).astype(BF)
    rb, cb = iota((blocks, blocks), 0), iota((blocks, blocks), 1)
    rl, cl = iota((128, 128), 0), iota((128, 128), 1)
    lower = dot(counts, (rl < cl).astype(BF)).astype(BF)
    offset = dot((cb < rb).astype(BF), counts) + dot(jnp.ones((blocks, blocks), BF), lower)
    spread = jnp.zeros((blocks, came), F32)
    for a in range(groups):
        spread += jnp.where(group == a, offset[:, a : a + 1], 0.0)
    base = jnp.sum(jnp.where(owner, spread, 0.0), axis=0, keepdims=True)
    rank = base + order
    slot = jnp.where(jnp.logical_and(flags > 0.5, rank < bound), rank, -1.0)
    slot_ref[...] = jnp.broadcast_to(slot, (8, came)).T
    hot = jnp.where(slot == iota((slots, came), 0).astype(F32), 1.0, 0.0).astype(BF)
    g_ref[...] = dot(hot, x_ref[:, :width]).astype(BF).T


def ffn_kernel(x_ref, wg_ref, wu_ref, wd_ref, o_ref):
    gate = dot(wg_ref[...], x_ref[...])
    up = dot(wu_ref[...], x_ref[...])
    hidden = (gate * jax.nn.sigmoid(SWISH_SCALE * gate) * (up + 1.0)).astype(BF)
    o_ref[...] = dot(wd_ref[...], hidden).astype(BF)


def place_kernel(y_ref, slot_ref, z_ref):
    slots = y_ref.shape[1]
    came = z_ref.shape[0]
    hot = jnp.where(slot_ref[:, 0:1] == iota((came, slots), 1).astype(F32), 1.0, 0.0)
    z_ref[...] = dot(hot.astype(BF), y_ref[...], ((1,), (1,))).astype(BF)


def mix_kernel(width, top, b_ref, r_ref, x_ref, o_ref):
    span = x_ref.shape[0]
    place = iota((span, b_ref.shape[0]), 1).astype(F32)
    here = [r_ref[:, k : k + 1] == place for k in range(top)]
    total = None
    for part in range(3):
        first = width + (1 + part) * top
        weight = jnp.zeros(place.shape, F32)
        for k in range(top):
            weight += jnp.where(here[k], x_ref[:, first + k : first + k + 1].astype(F32), 0.0)
        piece = dot(weight.astype(BF), b_ref[...])
        total = piece if part == 0 else total + piece
    o_ref[...] = total.astype(BF)


VMEM = pl.BlockSpec(memory_space=pltpu.VMEM)
SMEM = pl.BlockSpec(memory_space=pltpu.SMEM)


def cost(flops, moved):
    return pl.CostEstimate(flops=flops, bytes_accessed=moved, transcendentals=0)


def exchange(blocks):
    return lax.all_to_all(blocks, EXPERT, split_axis=0, concat_axis=0, tiled=True)


def on_device(
    tokens, expert_ids, gate_probs, shed_blocks, partner, gate_weight, up_weight, down_weight
):
    tok, model = tokens.shape
    top = expert_ids.shape[1]
    experts = shed_blocks.shape[0]
    groups = lax.axis_size("attn")
    width = model // groups
    capacity = tok * top * groups
    block = capacity // 8
    slots = capacity + block * SHED_MOST
    span = groups * tok
    most = min(tok, 3 * tok * top // experts)
    me = lax.axis_index(EXPERT)
    bound = capacity - block * shed_blocks[partner[me]] + block * shed_blocks[me]
    par = bound.reshape(1).astype(jnp.int32)
    high = lax.reduce_precision(gate_probs, 8, 7)
    rest = gate_probs - high
    middle = lax.reduce_precision(rest, 8, 7)
    meta = [expert_ids.astype(F32), high, middle, rest - middle, jnp.ones((tok, 1), F32)]
    flag = width + 4 * top
    meta = jnp.concatenate(meta, axis=1).astype(BF)
    columns = jnp.stack(
        [
            jnp.concatenate([tokens[:, b * width : (b + 1) * width], meta], axis=1)
            for b in range(groups)
        ]
    )
    wide = flag + 1
    mixed = lax.all_to_all(columns, "attn", 0, 0, tiled=True).reshape(span, wide)
    per = groups * most
    came = experts * per

    outgoing, seats = pl.pallas_call(
        lambda *refs: send_kernel(tok, most, width, top, experts, *refs),
        out_shape=(
            jax.ShapeDtypeStruct((came, wide), BF),
            jax.ShapeDtypeStruct((span, top), F32),
        ),
        in_specs=[VMEM],
        out_specs=(VMEM, VMEM),
        cost_estimate=cost(2 * span * came * width, 2 * came * width),
        name="send",
    )(mixed)
    arrived = exchange(outgoing.reshape(experts, per, wide)).reshape(came, wide)

    picked, slot = pl.pallas_call(
        lambda *refs: pick_kernel(most, width, flag, groups, *refs),
        out_shape=(
            jax.ShapeDtypeStruct((width, slots), BF),
            jax.ShapeDtypeStruct((came, 8), F32),
        ),
        in_specs=[VMEM, SMEM],
        out_specs=(VMEM, VMEM),
        cost_estimate=cost(2 * slots * came * width, 2 * came * width),
        name="pick",
    )(arrived, par)

    rows = lax.all_gather(picked, "attn", tiled=True)
    units = gate_weight.shape[2]
    tile = 256
    partial = pl.pallas_call(
        ffn_kernel,
        grid=(slots // tile,),
        out_shape=jax.ShapeDtypeStruct((model, slots), BF),
        in_specs=[
            pl.BlockSpec((model, tile), lambda i: (0, i)),
            pl.BlockSpec((units, model), lambda i: (0, 0)),
            pl.BlockSpec((units, model), lambda i: (0, 0)),
            pl.BlockSpec((model, units), lambda i: (0, 0)),
        ],
        out_specs=pl.BlockSpec((model, tile), lambda i: (0, i)),
        cost_estimate=cost(6 * slots * model * units, 6 * model * units),
        name="ffn",
    )(rows, gate_weight[0].T, up_weight[0].T, down_weight[0].T)
    summed = lax.psum_scatter(partial, "attn", scatter_dimension=0, tiled=True)
    answers = pl.pallas_call(
        place_kernel,
        out_shape=jax.ShapeDtypeStruct((came, width), BF),
        in_specs=[VMEM, VMEM],
        out_specs=VMEM,
        cost_estimate=cost(2 * slots * came * width, 2 * came * width),
        name="place",
    )(summed, slot)
    returned = exchange(answers.reshape(experts, per, width)).reshape(came, width)
    home = pl.pallas_call(
        lambda *refs: mix_kernel(width, top, *refs),
        out_shape=jax.ShapeDtypeStruct((span, width), BF),
        in_specs=[VMEM, VMEM, VMEM],
        out_specs=VMEM,
        cost_estimate=cost(6 * span * came * width, 2 * came * width),
        name="mix",
    )(returned, seats, mixed)
    back = lax.all_to_all(home.reshape(groups, tok, width), "attn", 0, 0, tiled=True)
    return back.transpose(1, 0, 2).reshape(tok, model)


def solution(mesh):
    split = Mesh(
        mesh.devices.reshape(mesh.shape["attn"], 4, 4, 2),
        ("attn", "expert_0", "expert_1", "expert_2"),
    )
    return jax.shard_map(
        on_device,
        mesh=split,
        in_specs=(
            P(ATTN_EXPERT, None),
            P(ATTN_EXPERT, None),
            P(ATTN_EXPERT, None),
            P(),
            P(),
            P(EXPERT, None, "attn"),
            P(EXPERT, None, "attn"),
            P(EXPERT, "attn", None),
        ),
        out_specs=P(ATTN_EXPERT, None),
        check_vma=False,
    )
```

```python
import jax
import jax.numpy as jnp
from jax import lax
from jax.experimental import pallas as pl
from jax.experimental.pallas import tpu as pltpu
from jax.sharding import Mesh
from jax.sharding import PartitionSpec as P

SHED_MOST = 4
ATTN_EXPERT = ("attn", "expert_0", "expert_1", "expert_2")
EXPERT = ("expert_0", "expert_1", "expert_2")
SWISH_SCALE = 1.702
BF = jnp.bfloat16
F32 = jnp.float32

def iota(shape, dim):
    return lax.broadcasted_iota(jnp.int32, shape, dim)


def dot(a, b, dims=((1,), (0,))):
    return lax.dot_general(a, b, (dims, ((), ())), preferred_element_type=F32)


def send_kernel(tok, most, width, top, experts, x_ref, s_ref, r_ref):
    span = x_ref.shape[0]
    per = span // tok * most
    x = x_ref[...]
    ids = x[:, width : width + top].astype(F32)
    lane = iota((span, experts), 1).astype(F32)
    named = [ids[:, k : k + 1] == lane for k in range(top)]
    hits = jnp.where(named[0], 1.0, 0.0)
    for k in range(1, top):
        hits += jnp.where(named[k], 1.0, 0.0)
    r, c = iota((span, span), 0), iota((span, span), 1)
    before = jnp.logical_and(r // tok == c // tok, c < r).astype(BF)
    order = dot(before, hits.astype(BF))
    group = (iota((span, 1), 0) // tok * most).astype(F32)
    place = iota((span, experts * per), 1).astype(F32)
    hot = None
    for k in range(top):
        seat = jnp.sum(jnp.where(named[k], order, 0.0), axis=1, keepdims=True)
        seat = seat + ids[:, k : k + 1] * per + group
        r_ref[:, k : k + 1] = seat
        here = jnp.where(seat == place, 1.0, 0.0)
        hot = here if k == 0 else hot + here
    s_ref[...] = dot(hot.astype(BF), x, ((0,), (0,))).astype(BF)


def pick_kernel(most, width, flag, groups, x_ref, par_ref, gh_ref, gl_ref, slot_ref):
    came, slots = x_ref.shape[0], gh_ref.shape[1]
    cut = gh_ref.shape[0]
    per = groups * most
    blocks = came // per
    bound = par_ref[0].astype(F32)
    start = width // 128 * 128
    tail = x_ref[:, start:]
    lanes = tail.shape[1]
    choose = (iota((8, lanes), 1) == flag - start).astype(BF)
    flags = dot(choose, tail, ((1,), (1,)))[0:1]
    row = iota((1, came), 1)
    group, order = row % per // most, (row % most).astype(F32)
    owner = iota((blocks, came), 0) == iota((blocks, came), 1) // per
    split = jnp.where(owner, flags, 0.0).astype(BF)
    member = iota((came, 128), 0) % per // most == iota((came, 128), 1)
    counts = dot(split, member.astype(BF)).astype(BF)
    rb, cb = iota((blocks, blocks), 0), iota((blocks, blocks), 1)
    rl, cl = iota((128, 128), 0), iota((128, 128), 1)
    lower = dot(counts, (rl < cl).astype(BF)).astype(BF)
    offset = dot((cb < rb).astype(BF), counts) + dot(jnp.ones((blocks, blocks), BF), lower)
    spread = jnp.zeros((blocks, came), F32)
    for a in range(groups):
        spread += jnp.where(group == a, offset[:, a : a + 1], 0.0)
    base = jnp.sum(jnp.where(owner, spread, 0.0), axis=0, keepdims=True)
    rank = base + order
    slot = jnp.where(jnp.logical_and(flags > 0.5, rank < bound), rank, -1.0)
    slot_ref[...] = jnp.broadcast_to(slot, (8, came)).T
    hot = jnp.where(slot == iota((slots, came), 0).astype(F32), 1.0, 0.0).astype(BF)
    got = dot(hot, x_ref[:, :width]).astype(BF).T
    gh_ref[...] = got[:cut]
    gl_ref[...] = got[cut:]


def whole(high, low):
    return jnp.concatenate([high[...], low[...]], axis=0)


def tiles(width, body):
    tile = 256 if width % 256 == 0 else width

    def step(i, carry):
        body(pl.ds(pl.multiple_of(i * tile, tile), tile))
        return carry

    lax.fori_loop(0, width // tile, step, 0)


def mid_kernel(par_ref, oh, ol, lh, ll, rh, rl, wg_ref, wu_ref, g_ref, u_ref):
    def body(at):
        gate = up = None
        for n, (high, low) in enumerate(((oh, ol), (lh, ll), (rh, rl))):
            x = jnp.concatenate([high[:, at], low[:, at]], axis=0)
            g, u = dot(wg_ref[par_ref[n]], x), dot(wu_ref[par_ref[n]], x)
            gate, up = (g, u) if n == 0 else (gate + g, up + u)
        g_ref[:, at] = gate
        u_ref[:, at] = up

    tiles(g_ref.shape[1], body)


def far_kernel(par_ref, g_ref, u_ref, fh, fl, wg_ref, wu_ref, wd_ref, h_ref, ch_ref, cl_ref):
    cut = ch_ref.shape[0]

    def body(at):
        x = jnp.concatenate([fh[:, at], fl[:, at]], axis=0)
        gate = g_ref[:, at] + dot(wg_ref[par_ref[3]], x)
        up = u_ref[:, at] + dot(wu_ref[par_ref[3]], x)
        hidden = (gate * jax.nn.sigmoid(SWISH_SCALE * gate) * (up + 1.0)).astype(BF)
        h_ref[:, at] = hidden
        share = dot(wd_ref[par_ref[3]], hidden).astype(BF)
        ch_ref[:, at] = share[:cut]
        cl_ref[:, at] = share[cut:]

    tiles(h_ref.shape[1], body)


def near_kernel(par_ref, h_ref, wd_ref, lh_ref, ll_ref, rh_ref, rl_ref, o_ref):
    cut = lh_ref.shape[0]

    def body(at):
        hidden = h_ref[:, at]
        left = dot(wd_ref[par_ref[1]], hidden)
        right = dot(wd_ref[par_ref[2]], hidden)
        lh_ref[:, at] = left[:cut]
        ll_ref[:, at] = left[cut:].astype(BF)
        rh_ref[:, at] = right[:cut].astype(BF)
        rl_ref[:, at] = right[cut:]
        o_ref[:, at] = dot(wd_ref[par_ref[0]], hidden)

    tiles(h_ref.shape[1], body)


def place_kernel(o_ref, lh, ll, rh, rl, slot_ref, z_ref):
    slots = o_ref.shape[1]
    came = z_ref.shape[0]
    total = o_ref[...] + whole(lh, ll).astype(F32) + whole(rh, rl).astype(F32)
    hot = jnp.where(slot_ref[:, 0:1] == iota((came, slots), 1).astype(F32), 1.0, 0.0)
    z_ref[...] = dot(hot.astype(BF), total.astype(BF), ((1,), (1,))).astype(BF)


def mix_kernel(width, top, b_ref, r_ref, x_ref, o_ref):
    span = x_ref.shape[0]
    place = iota((span, b_ref.shape[0]), 1).astype(F32)
    here = [r_ref[:, k : k + 1] == place for k in range(top)]
    total = None
    for part in range(3):
        first = width + (1 + part) * top
        weight = jnp.zeros(place.shape, F32)
        for k in range(top):
            weight += jnp.where(here[k], x_ref[:, first + k : first + k + 1].astype(F32), 0.0)
        piece = dot(weight.astype(BF), b_ref[...])
        total = piece if part == 0 else total + piece
    o_ref[...] = total.astype(BF)


VMEM = pl.BlockSpec(memory_space=pltpu.VMEM)
SMEM = pl.BlockSpec(memory_space=pltpu.SMEM)


def cost(flops, moved):
    return pl.CostEstimate(flops=flops, bytes_accessed=moved, transcendentals=0)


def exchange(blocks):
    return lax.all_to_all(blocks, EXPERT, split_axis=0, concat_axis=0, tiled=True)


def on_device(
    tokens, expert_ids, gate_probs, shed_blocks, partner, gate_weight, up_weight, down_weight
):
    tok, model = tokens.shape
    top = expert_ids.shape[1]
    experts = shed_blocks.shape[0]
    groups = lax.axis_size("attn")
    width = model // groups
    capacity = tok * top * groups
    block = capacity // 8
    slots = capacity + block * SHED_MOST
    span = groups * tok
    most = min(tok, 3 * tok * top // experts)
    me = lax.axis_index(EXPERT)
    bound = capacity - block * shed_blocks[partner[me]] + block * shed_blocks[me]
    par = bound.reshape(1).astype(jnp.int32)
    high = lax.reduce_precision(gate_probs, 8, 7)
    rest = gate_probs - high
    middle = lax.reduce_precision(rest, 8, 7)
    meta = [expert_ids.astype(F32), high, middle, rest - middle, jnp.ones((tok, 1), F32)]
    flag = width + 4 * top
    meta = jnp.concatenate(meta, axis=1).astype(BF)
    columns = jnp.stack(
        [
            jnp.concatenate([tokens[:, b * width : (b + 1) * width], meta], axis=1)
            for b in range(groups)
        ]
    )
    wide = flag + 1
    mixed = lax.all_to_all(columns, "attn", 0, 0, tiled=True).reshape(span, wide)
    per = groups * most
    came = experts * per

    outgoing, seats = pl.pallas_call(
        lambda *refs: send_kernel(tok, most, width, top, experts, *refs),
        out_shape=(
            jax.ShapeDtypeStruct((came, wide), BF),
            jax.ShapeDtypeStruct((span, top), F32),
        ),
        in_specs=[VMEM],
        out_specs=(VMEM, VMEM),
        cost_estimate=cost(2 * span * came * width, 2 * came * width),
        name="send",
    )(mixed)
    arrived = exchange(outgoing.reshape(experts, per, wide)).reshape(came, wide)

    cut = (width // 2 + 15) // 16 * 16
    shape = jax.ShapeDtypeStruct
    high, low = shape((cut, slots), BF), shape((width - cut, slots), BF)
    oh, ol, slot = pl.pallas_call(
        lambda *refs: pick_kernel(most, width, flag, groups, *refs),
        out_shape=(high, low, shape((came, 8), F32)),
        in_specs=[VMEM, SMEM],
        out_specs=(VMEM, VMEM, VMEM),
        cost_estimate=cost(2 * slots * came * width, 2 * came * width),
        name="pick",
    )(arrived, par)

    units = gate_weight.shape[2]
    at = lax.axis_index("attn")
    who = jnp.stack([at, (at - 1) % groups, (at + 1) % groups, (at + 2) % groups])
    who = who.astype(jnp.int32)
    to_right = [(i, (i + 1) % groups) for i in range(groups)]
    to_left = [(i, (i - 1) % groups) for i in range(groups)]
    right = lambda array: lax.ppermute(array, "attn", to_right)
    left = lambda array: lax.ppermute(array, "attn", to_left)
    wg = gate_weight[0].T.reshape(units, groups, width).transpose(1, 0, 2)
    wu = up_weight[0].T.reshape(units, groups, width).transpose(1, 0, 2)
    wd = down_weight[0].T.reshape(groups, width, units)

    ll = right(ol)
    rh = left(oh)
    lh = right(oh)
    rl = left(ol)
    fl = right(ll)
    fh = left(rh)
    big = shape((units, slots), F32)
    gate, up = pl.pallas_call(
        mid_kernel,
        out_shape=(big, big),
        in_specs=[SMEM] + [VMEM] * 8,
        out_specs=(VMEM, VMEM),
        cost_estimate=cost(12 * slots * width * units, 8 * model * units),
        name="mid",
    )(who, oh, ol, lh, ll, rh, rl, wg, wu)
    hidden, ch, cl = pl.pallas_call(
        far_kernel,
        out_shape=(shape((units, slots), BF), high, low),
        in_specs=[SMEM] + [VMEM] * 7,
        out_specs=(VMEM,) * 3,
        cost_estimate=cost(6 * slots * width * units, 8 * model * units),
        name="far",
    )(who, gate, up, fh, fl, wg, wu, wd)
    via_left, via_right = right(cl), left(ch)
    wide_high, wide_low = shape((cut, slots), F32), shape((width - cut, slots), F32)
    nlh, nll, nrh, nrl, own = pl.pallas_call(
        near_kernel,
        out_shape=(wide_high, low, high, wide_low, shape((width, slots), F32)),
        in_specs=[SMEM, VMEM, VMEM],
        out_specs=(VMEM,) * 5,
        cost_estimate=cost(6 * slots * width * units, 8 * model * units),
        name="near",
    )(who, hidden, wd)
    slh, srl = right(nrh), left(nll)
    sll = right((nrl + via_left.astype(F32)).astype(BF))
    srh = left((nlh + via_right.astype(F32)).astype(BF))
    answers = pl.pallas_call(
        place_kernel,
        out_shape=shape((came, width), BF),
        in_specs=[VMEM] * 6,
        out_specs=VMEM,
        cost_estimate=cost(2 * slots * came * width, 2 * came * width),
        name="place",
    )(own, slh, sll, srh, srl, slot)
    returned = exchange(answers.reshape(experts, per, width)).reshape(came, width)
    home = pl.pallas_call(
        lambda *refs: mix_kernel(width, top, *refs),
        out_shape=jax.ShapeDtypeStruct((span, width), BF),
        in_specs=[VMEM, VMEM, VMEM],
        out_specs=VMEM,
        cost_estimate=cost(6 * span * came * width, 2 * came * width),
        name="mix",
    )(returned, seats, mixed)
    back = lax.all_to_all(home.reshape(groups, tok, width), "attn", 0, 0, tiled=True)
    return back.transpose(1, 0, 2).reshape(tok, model)


def solution(mesh):
    split = Mesh(
        mesh.devices.reshape(mesh.shape["attn"], 4, 4, 2),
        ("attn", "expert_0", "expert_1", "expert_2"),
    )
    return jax.shard_map(
        on_device,
        mesh=split,
        in_specs=(
            P(ATTN_EXPERT, None),
            P(ATTN_EXPERT, None),
            P(ATTN_EXPERT, None),
            P(),
            P(),
            P(EXPERT, None, "attn"),
            P(EXPERT, None, "attn"),
            P(EXPERT, "attn", None),
        ),
        out_specs=P(ATTN_EXPERT, None),
        check_vma=False,
    )
```

```python
import jax
import jax.numpy as jnp
from jax import lax
from jax.experimental import pallas as pl
from jax.experimental.pallas import tpu as pltpu
from jax.sharding import Mesh
from jax.sharding import PartitionSpec as P

SHED_MOST = 4
ATTN_EXPERT = ("attn", "expert_0", "expert_1", "expert_2")
EXPERT = ("expert_0", "expert_1", "expert_2")
SWISH_SCALE = 1.702
BF = jnp.bfloat16
F32 = jnp.float32

def iota(shape, dim):
    return lax.broadcasted_iota(jnp.int32, shape, dim)


def dot(a, b, dims=((1,), (0,))):
    return lax.dot_general(a, b, (dims, ((), ())), preferred_element_type=F32)


def send_kernel(tok, most, width, top, experts, x_ref, s_ref, r_ref):
    span = x_ref.shape[0]
    per = span // tok * most
    x = x_ref[...]
    ids = x[:, width : width + top].astype(F32)
    lane = iota((span, experts), 1).astype(F32)
    named = [ids[:, k : k + 1] == lane for k in range(top)]
    hits = jnp.where(named[0], 1.0, 0.0)
    for k in range(1, top):
        hits += jnp.where(named[k], 1.0, 0.0)
    r, c = iota((span, span), 0), iota((span, span), 1)
    before = jnp.logical_and(r // tok == c // tok, c < r).astype(BF)
    order = dot(before, hits.astype(BF))
    group = (iota((span, 1), 0) // tok * most).astype(F32)
    place = iota((span, experts * per), 1).astype(F32)
    hot = None
    for k in range(top):
        seat = jnp.sum(jnp.where(named[k], order, 0.0), axis=1, keepdims=True)
        seat = seat + ids[:, k : k + 1] * per + group
        r_ref[:, k : k + 1] = seat
        here = jnp.where(seat == place, 1.0, 0.0)
        hot = here if k == 0 else hot + here
    s_ref[...] = dot(hot.astype(BF), x, ((0,), (0,))).astype(BF)


def pick_kernel(most, width, flag, groups, x_ref, par_ref, gh_ref, gl_ref, slot_ref):
    came, slots = x_ref.shape[0], gh_ref.shape[1]
    cut = gh_ref.shape[0]
    per = groups * most
    blocks = came // per
    bound = par_ref[0].astype(F32)
    start = width // 128 * 128
    tail = x_ref[:, start:]
    lanes = tail.shape[1]
    choose = (iota((8, lanes), 1) == flag - start).astype(BF)
    flags = dot(choose, tail, ((1,), (1,)))[0:1]
    row = iota((1, came), 1)
    group, order = row % per // most, (row % most).astype(F32)
    owner = iota((blocks, came), 0) == iota((blocks, came), 1) // per
    split = jnp.where(owner, flags, 0.0).astype(BF)
    member = iota((came, 128), 0) % per // most == iota((came, 128), 1)
    counts = dot(split, member.astype(BF)).astype(BF)
    rb, cb = iota((blocks, blocks), 0), iota((blocks, blocks), 1)
    rl, cl = iota((128, 128), 0), iota((128, 128), 1)
    lower = dot(counts, (rl < cl).astype(BF)).astype(BF)
    offset = dot((cb < rb).astype(BF), counts) + dot(jnp.ones((blocks, blocks), BF), lower)
    spread = jnp.zeros((blocks, came), F32)
    for a in range(groups):
        spread += jnp.where(group == a, offset[:, a : a + 1], 0.0)
    base = jnp.sum(jnp.where(owner, spread, 0.0), axis=0, keepdims=True)
    rank = base + order
    slot = jnp.where(jnp.logical_and(flags > 0.5, rank < bound), rank, -1.0)
    slot_ref[...] = jnp.broadcast_to(slot, (8, came)).T
    hot = jnp.where(slot == iota((slots, came), 0).astype(F32), 1.0, 0.0).astype(BF)
    got = dot(hot, x_ref[:, :width]).astype(BF).T
    gh_ref[...] = got[:cut]
    gl_ref[...] = got[cut:]


def whole(high, low):
    return jnp.concatenate([high[...], low[...]], axis=0)


def relay_kernel(seen_ref, g_ref, u_ref, d_ref, go_ref, uo_ref, do_ref):
    del seen_ref
    blocks, width = go_ref.shape[0], go_ref.shape[2]
    for b in range(blocks):
        at = slice(b * width, (b + 1) * width)
        go_ref[b] = g_ref[:, at]
        uo_ref[b] = u_ref[:, at]
        do_ref[b] = d_ref[:, at].T


def mid_kernel(par_ref, oh, ol, lh, ll, rh, rl, ga, gb, gc, ua, ub, uc, g_ref, u_ref):
    del par_ref
    gate = up = None
    for n, (x, g, u) in enumerate(
        ((whole(oh, ol), ga, ua), (whole(lh, ll), gb, ub), (whole(rh, rl), gc, uc))
    ):
        g, u = dot(g[0], x), dot(u[0], x)
        gate, up = (g, u) if n == 0 else (gate + g, up + u)
    g_ref[...] = gate
    u_ref[...] = up


def far_kernel(par_ref, g_ref, u_ref, fh, fl, wg_ref, wu_ref, wd_ref, h_ref, ch_ref, cl_ref):
    del par_ref
    cut = ch_ref.shape[0]
    x = whole(fh, fl)
    gate = g_ref[...] + dot(wg_ref[0], x)
    up = u_ref[...] + dot(wu_ref[0], x)
    hidden = (gate * jax.nn.sigmoid(SWISH_SCALE * gate) * (up + 1.0)).astype(BF)
    h_ref[...] = hidden
    share = dot(wd_ref[0], hidden).astype(BF)
    ch_ref[...] = share[:cut]
    cl_ref[...] = share[cut:]


def near_kernel(par_ref, h_ref, da, db, dc, lh_ref, ll_ref, rh_ref, rl_ref, o_ref):
    del par_ref
    cut = lh_ref.shape[0]
    hidden = h_ref[...]
    left = dot(db[0], hidden)
    right = dot(dc[0], hidden)
    lh_ref[...] = left[:cut]
    ll_ref[...] = left[cut:].astype(BF)
    rh_ref[...] = right[:cut].astype(BF)
    rl_ref[...] = right[cut:]
    o_ref[...] = dot(da[0], hidden)


def place_kernel(o_ref, lh, ll, rh, rl, slot_ref, z_ref):
    slots = o_ref.shape[1]
    came = z_ref.shape[0]
    total = o_ref[...] + whole(lh, ll).astype(F32) + whole(rh, rl).astype(F32)
    hot = jnp.where(slot_ref[:, 0:1] == iota((came, slots), 1).astype(F32), 1.0, 0.0)
    z_ref[...] = dot(hot.astype(BF), total.astype(BF), ((1,), (1,))).astype(BF)


def mix_kernel(width, top, b_ref, r_ref, x_ref, o_ref):
    span = x_ref.shape[0]
    place = iota((span, b_ref.shape[0]), 1).astype(F32)
    here = [r_ref[:, k : k + 1] == place for k in range(top)]
    total = None
    for part in range(3):
        first = width + (1 + part) * top
        weight = jnp.zeros(place.shape, F32)
        for k in range(top):
            weight += jnp.where(here[k], x_ref[:, first + k : first + k + 1].astype(F32), 0.0)
        piece = dot(weight.astype(BF), b_ref[...])
        total = piece if part == 0 else total + piece
    o_ref[...] = total.astype(BF)


VMEM = pl.BlockSpec(memory_space=pltpu.VMEM)
SMEM = pl.BlockSpec(memory_space=pltpu.SMEM)


def cost(flops, moved):
    return pl.CostEstimate(flops=flops, bytes_accessed=moved, transcendentals=0)


def exchange(blocks):
    return lax.all_to_all(blocks, EXPERT, split_axis=0, concat_axis=0, tiled=True)


def on_device(
    tokens, expert_ids, gate_probs, shed_blocks, partner, gate_weight, up_weight, down_weight
):
    tok, model = tokens.shape
    top = expert_ids.shape[1]
    experts = shed_blocks.shape[0]
    groups = lax.axis_size("attn")
    width = model // groups
    capacity = tok * top * groups
    block = capacity // 8
    slots = capacity + block * SHED_MOST
    span = groups * tok
    most = min(tok, 3 * tok * top // experts)
    me = lax.axis_index(EXPERT)
    bound = capacity - block * shed_blocks[partner[me]] + block * shed_blocks[me]
    par = bound.reshape(1).astype(jnp.int32)
    high = lax.reduce_precision(gate_probs, 8, 7)
    rest = gate_probs - high
    middle = lax.reduce_precision(rest, 8, 7)
    meta = [expert_ids.astype(F32), high, middle, rest - middle, jnp.ones((tok, 1), F32)]
    flag = width + 4 * top
    meta = jnp.concatenate(meta, axis=1).astype(BF)
    columns = jnp.stack(
        [
            jnp.concatenate([tokens[:, b * width : (b + 1) * width], meta], axis=1)
            for b in range(groups)
        ]
    )
    wide = flag + 1
    mixed = lax.all_to_all(columns, "attn", 0, 0, tiled=True).reshape(span, wide)
    per = groups * most
    came = experts * per

    outgoing, seats = pl.pallas_call(
        lambda *refs: send_kernel(tok, most, width, top, experts, *refs),
        out_shape=(
            jax.ShapeDtypeStruct((came, wide), BF),
            jax.ShapeDtypeStruct((span, top), F32),
        ),
        in_specs=[VMEM],
        out_specs=(VMEM, VMEM),
        cost_estimate=cost(2 * span * came * width, 2 * came * width),
        name="send",
    )(mixed)
    arrived = exchange(outgoing.reshape(experts, per, wide)).reshape(came, wide)

    cut = (width // 2 + 15) // 16 * 16
    shape = jax.ShapeDtypeStruct
    high, low = shape((cut, slots), BF), shape((width - cut, slots), BF)
    units = gate_weight.shape[2]
    relaid = shape((groups, units, width), BF)
    wg, wu, wd = pl.pallas_call(
        relay_kernel,
        out_shape=(relaid, relaid, shape((groups, width, units), BF)),
        in_specs=[pl.BlockSpec(memory_space=pl.ANY)] + [VMEM] * 3,
        out_specs=(VMEM,) * 3,
        cost_estimate=cost(12 * slots * width * units, 12 * model * units),
        name="relay",
    )(seats, gate_weight[0].T, up_weight[0].T, down_weight[0])
    arrived, wg, wu, wd = lax.optimization_barrier((arrived, wg, wu, wd))
    oh, ol, slot = pl.pallas_call(
        lambda *refs: pick_kernel(most, width, flag, groups, *refs),
        out_shape=(high, low, shape((came, 8), F32)),
        in_specs=[VMEM, SMEM],
        out_specs=(VMEM, VMEM, VMEM),
        cost_estimate=cost(2 * slots * came * width, 2 * came * width),
        name="pick",
    )(arrived, par)

    at = lax.axis_index("attn").astype(jnp.int32).reshape(1)
    to_right = [(i, (i + 1) % groups) for i in range(groups)]
    to_left = [(i, (i - 1) % groups) for i in range(groups)]
    right = lambda array: lax.ppermute(array, "attn", to_right)
    left = lambda array: lax.ppermute(array, "attn", to_left)
    ll = right(ol)
    rh = left(oh)
    lh = right(oh)
    rl = left(ol)
    fl = right(ll)
    fh = left(rh)
    big = shape((units, slots), F32)
    tile = 256
    lane = lambda rows: pl.BlockSpec((rows, tile), lambda i, p: (0, i))

    def weight(rows, columns, ahead):
        return pl.BlockSpec((1, rows, columns), lambda i, p: (lax.rem(p[0] + ahead, groups), 0, 0))

    def staged(kernel, name, ins, outs, out_shape, flops):
        return pl.pallas_call(
            kernel,
            grid_spec=pltpu.PrefetchScalarGridSpec(
                num_scalar_prefetch=1, grid=(slots // tile,), in_specs=ins, out_specs=outs
            ),
            out_shape=out_shape,
            cost_estimate=cost(flops, 8 * model * units),
            name=name,
        )

    before, after, across = groups - 1, 1, groups // 2
    halves = [lane(cut), lane(width - cut)]
    three = [weight(units, width, d) for d in (0, before, after)]
    gate, up = staged(
        mid_kernel,
        "mid",
        halves * 3 + three * 2,
        (lane(units), lane(units)),
        (big, big),
        12 * slots * width * units,
    )(at, oh, ol, lh, ll, rh, rl, wg, wg, wg, wu, wu, wu)
    opposite = weight(units, width, across)
    hidden, ch, cl = staged(
        far_kernel,
        "far",
        [lane(units), lane(units)] + halves + [opposite, opposite, weight(width, units, across)],
        (lane(units), *halves),
        (shape((units, slots), BF), high, low),
        6 * slots * width * units,
    )(at, gate, up, fh, fl, wg, wu, wd)
    via_left, via_right = right(cl), left(ch)
    wide_high, wide_low = shape((cut, slots), F32), shape((width - cut, slots), F32)
    nlh, nll, nrh, nrl, own = staged(
        near_kernel,
        "near",
        [lane(units)] + [weight(width, units, d) for d in (0, before, after)],
        (*halves, *halves, lane(width)),
        (wide_high, low, high, wide_low, shape((width, slots), F32)),
        6 * slots * width * units,
    )(at, hidden, wd, wd, wd)
    slh, srl = right(nrh), left(nll)
    sll = right((nrl + via_left.astype(F32)).astype(BF))
    srh = left((nlh + via_right.astype(F32)).astype(BF))
    answers = pl.pallas_call(
        place_kernel,
        out_shape=shape((came, width), BF),
        in_specs=[VMEM] * 6,
        out_specs=VMEM,
        cost_estimate=cost(2 * slots * came * width, 2 * came * width),
        name="place",
    )(own, slh, sll, srh, srl, slot)
    returned = exchange(answers.reshape(experts, per, width)).reshape(came, width)
    home = pl.pallas_call(
        lambda *refs: mix_kernel(width, top, *refs),
        out_shape=jax.ShapeDtypeStruct((span, width), BF),
        in_specs=[VMEM, VMEM, VMEM],
        out_specs=VMEM,
        cost_estimate=cost(6 * span * came * width, 2 * came * width),
        name="mix",
    )(returned, seats, mixed)
    back = lax.all_to_all(home.reshape(groups, tok, width), "attn", 0, 0, tiled=True)
    return back.transpose(1, 0, 2).reshape(tok, model)


def solution(mesh):
    split = Mesh(
        mesh.devices.reshape(mesh.shape["attn"], 4, 4, 2),
        ("attn", "expert_0", "expert_1", "expert_2"),
    )
    return jax.shard_map(
        on_device,
        mesh=split,
        in_specs=(
            P(ATTN_EXPERT, None),
            P(ATTN_EXPERT, None),
            P(ATTN_EXPERT, None),
            P(),
            P(),
            P(EXPERT, None, "attn"),
            P(EXPERT, None, "attn"),
            P(EXPERT, "attn", None),
        ),
        out_specs=P(ATTN_EXPERT, None),
        check_vma=False,
    )
```

```python
import jax
import jax.numpy as jnp
from jax import lax
from jax.experimental import pallas as pl
from jax.experimental.pallas import tpu as pltpu
from jax.sharding import Mesh
from jax.sharding import PartitionSpec as P

SHED_MOST = 4
ATTN_EXPERT = ("attn", "expert_0", "expert_1", "expert_2")
EXPERT = ("expert_0", "expert_1", "expert_2")
SWISH_SCALE = 1.702
BF = jnp.bfloat16
F32 = jnp.float32

def iota(shape, dim):
    return lax.broadcasted_iota(jnp.int32, shape, dim)


def dot(a, b, dims=((1,), (0,))):
    return lax.dot_general(a, b, (dims, ((), ())), preferred_element_type=F32)


def half(n):
    return (n // 2 + 15) // 16 * 16


def by_distance(at_ref, store_ref, outs):
    for r, out in enumerate(outs):
        out[...] = store_ref[lax.rem(at_ref[0] + r, len(outs))]


def from_distance(at_ref, store_ref, ins):
    for r, block in enumerate(ins):
        store_ref[lax.rem(at_ref[0] + r, len(ins))] = block[...]


def cut_kernel(lay, at_ref, x_ref, id_ref, p_ref, *refs):
    outs, store_ref = refs[:-1], refs[-1]
    prob = p_ref[...]
    high = prob.astype(BF).astype(F32)
    rest = prob - high
    middle = rest.astype(BF).astype(F32)
    meta = jnp.concatenate([id_ref[...].astype(F32), high, middle, rest - middle], axis=0)
    meta = meta.T.astype(BF)
    tok = x_ref.shape[0]
    store_ref[...] = jnp.zeros_like(store_ref)
    for b in range(len(outs)):
        first = b * lay.width
        store_ref[b, :, : lay.cut] = x_ref[:, first : first + lay.cut]
        store_ref[b, :, lay.cut : lay.cut + 1] = jnp.ones((tok, 1), BF)
        store_ref[b, :, lay.low : lay.meta] = x_ref[:, first + lay.cut : first + lay.width]
        store_ref[b, :, lay.meta :] = meta
    by_distance(at_ref, store_ref, outs)


def send_kernel(lay, at_ref, xa, xb, xc, xd, h_ref, l_ref, r_ref, m_ref, store_ref):
    from_distance(at_ref, store_ref, (xa, xb, xc, xd))
    tok = xa.shape[0]
    span = m_ref.shape[0]
    x = store_ref[...].reshape(span, store_ref.shape[2])
    m_ref[...] = x[:, lay.meta :]
    ids = x[:, lay.meta : lay.meta + lay.top].astype(F32)
    experts = h_ref.shape[0] // lay.per
    lane = iota((span, experts), 1).astype(F32)
    named = [ids[:, k : k + 1] == lane for k in range(lay.top)]
    hits = jnp.where(named[0], 1.0, 0.0)
    for k in range(1, lay.top):
        hits += jnp.where(named[k], 1.0, 0.0)
    r, c = iota((span, span), 0), iota((span, span), 1)
    before = jnp.logical_and(r // tok == c // tok, c < r).astype(BF)
    order = dot(before, hits.astype(BF))
    group = (iota((span, 1), 0) // tok * lay.most).astype(F32)
    place = iota((span, experts * lay.per), 1).astype(F32)
    hot = None
    for k in range(lay.top):
        seat = jnp.sum(jnp.where(named[k], order, 0.0), axis=1, keepdims=True)
        seat = seat + ids[:, k : k + 1] * lay.per + group
        r_ref[:, k : k + 1] = seat
        here = jnp.where(seat == place, 1.0, 0.0)
        hot = here if k == 0 else hot + here
    hot = hot.astype(BF)
    h_ref[...] = dot(hot, x[:, : lay.low], ((0,), (0,))).astype(BF)
    l_ref[...] = dot(hot, x[:, lay.low : lay.meta], ((0,), (0,))).astype(BF)


def gather_rows(slot, rows, out_ref):
    slots = out_ref.shape[1]
    hot = jnp.where(slot == iota((slots, slot.shape[1]), 0).astype(F32), 1.0, 0.0).astype(BF)
    out_ref[...] = dot(hot, rows).astype(BF).T


def pick_kernel(lay, groups, x_ref, par_ref, g_ref, row_ref, col_ref):
    came = x_ref.shape[0]
    blocks = came // lay.per
    bound = par_ref[0].astype(F32)
    start = lay.cut // 128 * 128
    tail = x_ref[:, start:]
    choose = (iota((8, tail.shape[1]), 1) == lay.cut - start).astype(BF)
    flags = dot(choose, tail, ((1,), (1,)))[0:1]
    row = iota((1, came), 1)
    group, order = row % lay.per // lay.most, (row % lay.most).astype(F32)
    owner = iota((blocks, came), 0) == iota((blocks, came), 1) // lay.per
    split = jnp.where(owner, flags, 0.0).astype(BF)
    member = iota((came, 128), 0) % lay.per // lay.most == iota((came, 128), 1)
    counts = dot(split, member.astype(BF)).astype(BF)
    rb, cb = iota((blocks, blocks), 0), iota((blocks, blocks), 1)
    rl, cl = iota((128, 128), 0), iota((128, 128), 1)
    lower = dot(counts, (rl < cl).astype(BF)).astype(BF)
    offset = dot((cb < rb).astype(BF), counts) + dot(jnp.ones((blocks, blocks), BF), lower)
    spread = jnp.zeros((blocks, came), F32)
    for a in range(groups):
        spread += jnp.where(group == a, offset[:, a : a + 1], 0.0)
    rank = jnp.sum(jnp.where(owner, spread, 0.0), axis=0, keepdims=True) + order
    slot = jnp.where(jnp.logical_and(flags > 0.5, rank < bound), rank, -1.0)
    every = jnp.broadcast_to(slot, (8, came))
    row_ref[...] = every
    col_ref[...] = every.T
    gather_rows(slot, x_ref[:, : lay.cut], g_ref)


def pick_low_kernel(x_ref, row_ref, g_ref):
    gather_rows(row_ref[0:1], x_ref[...], g_ref)


def whole(*parts):
    return jnp.concatenate([part[...] for part in parts], axis=0)


def relay_kernel(seen_ref, g_ref, u_ref, d_ref, go_ref, uo_ref, do_ref):
    del seen_ref
    blocks, width = go_ref.shape[0], go_ref.shape[2]
    for b in range(blocks):
        at = slice(b * width, (b + 1) * width)
        go_ref[b] = g_ref[:, at]
        uo_ref[b] = u_ref[:, at]
        do_ref[b] = d_ref[:, at].T


def mid_kernel(at_ref, oh, ol, lh, ll, rh, rl, ga, gb, gc, ua, ub, uc, g_ref, u_ref):
    del at_ref
    gate = up = None
    for n, (x, g, u) in enumerate(
        ((whole(oh, ol), ga, ua), (whole(lh, ll), gb, ub), (whole(rh, rl), gc, uc))
    ):
        g, u = dot(g[0], x), dot(u[0], x)
        gate, up = (g, u) if n == 0 else (gate + g, up + u)
    g_ref[...] = gate
    u_ref[...] = up


def share_out(values, refs):
    first = 0
    for ref in refs:
        ref[...] = values[first : first + ref.shape[0]].astype(ref.dtype)
        first += ref.shape[0]


def far_kernel(at_ref, g_ref, u_ref, fa, fb, fc, fd, wg_ref, wu_ref, wd_ref, h_ref, *outs):
    del at_ref
    x = whole(fa, fb, fc, fd)
    gate = g_ref[...] + dot(wg_ref[0], x)
    up = u_ref[...] + dot(wu_ref[0], x)
    hidden = (gate * jax.nn.sigmoid(SWISH_SCALE * gate) * (up + 1.0)).astype(BF)
    h_ref[...] = hidden
    share_out(dot(wd_ref[0], hidden), outs)


def near_kernel(at_ref, h_ref, da, db, dc, *outs):
    del at_ref
    hidden = h_ref[...]
    share_out(dot(db[0], hidden), outs[0:4])
    share_out(dot(dc[0], hidden), outs[4:8])
    share_out(dot(da[0], hidden), outs[8:10])


def place_kernel(o_ref, la, lb, ra, rb, slot_ref, z_ref):
    slots = o_ref.shape[1]
    came = z_ref.shape[0]
    total = o_ref[...] + whole(la, lb).astype(F32) + whole(ra, rb).astype(F32)
    hot = jnp.where(slot_ref[:, 0:1] == iota((came, slots), 1).astype(F32), 1.0, 0.0)
    z_ref[...] = dot(hot.astype(BF), total.astype(BF), ((1,), (1,))).astype(BF)


def mix_kernel(lay, at_ref, h_ref, l_ref, r_ref, m_ref, *refs):
    outs, store_ref = refs[:-1], refs[-1]
    span, tok = m_ref.shape[0], outs[0].shape[0]
    place = iota((span, h_ref.shape[0]), 1).astype(F32)
    here = [r_ref[:, k : k + 1] == place for k in range(lay.top)]
    high = low = None
    for part in range(3):
        first = (1 + part) * lay.top
        weight = jnp.zeros(place.shape, F32)
        for k in range(lay.top):
            weight += jnp.where(here[k], m_ref[:, first + k : first + k + 1].astype(F32), 0.0)
        weight = weight.astype(BF)
        h, l = dot(weight, h_ref[...]), dot(weight, l_ref[...])
        high, low = (h, l) if part == 0 else (high + h, low + l)
    for g in range(len(outs)):
        at = slice(g * tok, (g + 1) * tok)
        store_ref[g, :, : lay.cut] = high[at].astype(BF)
        store_ref[g, :, lay.low : lay.meta] = low[at].astype(BF)
    by_distance(at_ref, store_ref, outs)


def join_kernel(lay, at_ref, *refs):
    ins, out_ref, store_ref = refs[:-2], refs[-2], refs[-1]
    from_distance(at_ref, store_ref, ins)
    for b in range(len(ins)):
        first = b * lay.width
        out_ref[:, first : first + lay.cut] = store_ref[b, :, : lay.cut]
        out_ref[:, first + lay.cut : first + lay.width] = store_ref[b, :, lay.low : lay.meta]


VMEM = pl.BlockSpec(memory_space=pltpu.VMEM)
SMEM = pl.BlockSpec(memory_space=pltpu.SMEM)
ANY = pl.BlockSpec(memory_space=pl.ANY)
shape = jax.ShapeDtypeStruct


class Layout:
    def __init__(self, width, top, most, groups):
        self.width, self.top, self.most, self.per = width, top, most, groups * most
        self.cut = half(width)
        self.low = (self.cut + 1 + 127) // 128 * 128
        self.meta = self.low + width - self.cut
        self.lanes = self.meta + 4 * top


def cost(flops, moved):
    return pl.CostEstimate(flops=flops, bytes_accessed=moved, transcendentals=0)


def run(kernel, name, ins, outs, work, scratch=()):
    return pl.pallas_call(
        kernel,
        out_shape=outs,
        in_specs=ins,
        out_specs=jax.tree.map(lambda _: VMEM, outs),
        scratch_shapes=scratch,
        cost_estimate=cost(*work),
        name=name,
    )


def on_device(
    tokens, expert_ids, gate_probs, shed_blocks, partner, gate_weight, up_weight, down_weight
):
    tok, model = tokens.shape
    top = expert_ids.shape[1]
    experts = shed_blocks.shape[0]
    groups = lax.axis_size("attn")
    width = model // groups
    capacity = tok * top * groups
    block = capacity // 8
    slots = capacity + block * SHED_MOST
    span = groups * tok
    units = gate_weight.shape[2]
    lay = Layout(width, top, min(tok, 3 * tok * top // experts), groups)
    cut, rest = lay.cut, width - lay.cut
    came = experts * lay.per
    me = lax.axis_index(EXPERT)
    bound = capacity - block * shed_blocks[partner[me]] + block * shed_blocks[me]
    par = bound.reshape(1).astype(jnp.int32)
    at = lax.axis_index("attn").astype(jnp.int32).reshape(1)

    def shifted(distance):
        pairs = [(i, (i + distance) % groups) for i in range(groups)]
        return lambda array: lax.ppermute(array, "attn", pairs)

    right, left = shifted(1), shifted(groups - 1)

    def swap(blocks):
        moved = [blocks[0]] + [shifted(r)(blocks[r]) for r in range(1, groups)]
        return [moved[(groups - r) % groups] for r in range(groups)]

    def exchange(rows):
        blocks = rows.reshape(experts, lay.per, rows.shape[1])
        moved = lax.all_to_all(blocks, EXPERT, split_axis=0, concat_axis=0, tiled=True)
        return moved.reshape(rows.shape)

    piece = shape((tok, lay.lanes), BF)
    blocks = run(
        lambda *refs: cut_kernel(lay, *refs),
        "cut",
        [SMEM, VMEM, VMEM, VMEM],
        (piece,) * groups,
        (tok * model, 4 * tok * model),
        [pltpu.VMEM((groups, tok, lay.lanes), BF)],
    )(at, tokens, expert_ids.T, gate_probs.T)
    out_high, out_low, seats, meta = run(
        lambda *refs: send_kernel(lay, *refs),
        "send",
        [SMEM] + [VMEM] * 4,
        (
            shape((came, lay.low), BF),
            shape((came, rest), BF),
            shape((span, top), F32),
            shape((span, 4 * top), BF),
        ),
        (2 * span * came * width, 2 * came * width),
        [pltpu.VMEM((groups, tok, lay.lanes), BF)],
    )(at, *swap(blocks))
    came_high = exchange(out_high)
    came_low = exchange(out_low)
    relaid = shape((groups, units, width), BF)
    wg, wu, wd = run(
        relay_kernel,
        "relay",
        [ANY] + [VMEM] * 3,
        (relaid, relaid, shape((groups, width, units), BF)),
        (12 * slots * width * units, 12 * model * units),
    )(seats, gate_weight[0].T, up_weight[0].T, down_weight[0])
    came_high, wg, wu, wd = lax.optimization_barrier((came_high, wg, wu, wd))

    gather_work = (slots * came * width, came * width)
    oh, slot_row, slot_col = run(
        lambda *refs: pick_kernel(lay, groups, *refs),
        "pick",
        [VMEM, SMEM],
        (shape((cut, slots), BF), shape((8, came), F32), shape((came, 8), F32)),
        gather_work,
    )(came_high, par)

    def ring(part):
        point = half(part.shape[0])
        below, above = right(part), left(part)
        return below, above, left(above[:point]), right(below[point:])

    lh, rh, fha, fhb = ring(oh)
    ol = run(pick_low_kernel, "pick_low", [VMEM] * 2, shape((rest, slots), BF), gather_work)(
        came_low, slot_row
    )
    ll, rl, fla, flb = ring(ol)

    tile = 256
    lane = lambda rows: pl.BlockSpec((rows, tile), lambda i, p: (0, i))

    def weight(rows, columns, ahead):
        return pl.BlockSpec((1, rows, columns), lambda i, p: (lax.rem(p[0] + ahead, groups), 0, 0))

    def staged(kernel, name, ins, outs, flops):
        return pl.pallas_call(
            kernel,
            grid_spec=pltpu.PrefetchScalarGridSpec(
                num_scalar_prefetch=1,
                grid=(slots // tile,),
                in_specs=ins,
                out_specs=tuple(lane(out.shape[0]) for out in outs),
            ),
            out_shape=outs,
            cost_estimate=cost(flops, 8 * model * units),
            name=name,
        )

    before, after, across = groups - 1, 1, groups // 2
    heights = [half(cut), cut - half(cut), half(rest), rest - half(rest)]
    rows = lambda n, kind: shape((n, slots), kind)
    gate, up = staged(
        mid_kernel,
        "mid",
        [lane(cut), lane(rest)] * 3 + [weight(units, width, d) for d in (0, before, after)] * 2,
        (rows(units, F32), rows(units, F32)),
        12 * slots * width * units,
    )(at, oh, ol, lh, ll, rh, rl, wg, wg, wg, wu, wu, wu)
    opposite = weight(units, width, across)
    hidden, ha, hb, la, lb = staged(
        far_kernel,
        "far",
        [lane(units)] * 2
        + [lane(n) for n in heights]
        + [opposite, opposite, weight(width, units, across)],
        (rows(units, BF), *(rows(n, BF) for n in heights)),
        6 * slots * width * units,
    )(at, gate, up, fha, fhb, fla, flb, wg, wu, wd)
    near = staged(
        near_kernel,
        "near",
        [lane(units)] + [weight(width, units, d) for d in (0, before, after)],
        (
            *(rows(n, kind) for n, kind in zip(heights, (F32, BF, F32, BF))),
            *(rows(n, kind) for n, kind in zip(heights, (BF, F32, BF, F32))),
            rows(cut, F32),
            rows(rest, F32),
        ),
        6 * slots * width * units,
    )(at, hidden, wd, wd, wd)

    def ring_sum(name, far_a, far_b, left_a, left_b, right_a, right_b, own):
        to_right, to_left = right(far_b), left(far_a)
        ra, lb = right(right_a), left(left_b)
        rb = right((right_b + to_right.astype(F32)).astype(BF))
        la = left((left_a + to_left.astype(F32)).astype(BF))
        return run(
            place_kernel, name, [VMEM] * 6, shape((came, own.shape[0]), BF), gather_work
        )(own, ra, rb, la, lb, slot_col)

    back_high = exchange(ring_sum("place", ha, hb, *near[0:2], *near[4:6], near[8]))
    la, lb, low_own = lax.optimization_barrier((la, lb, near[9]))
    back_low = exchange(ring_sum("place_low", la, lb, *near[2:4], *near[6:8], low_own))
    home = run(
        lambda *refs: mix_kernel(lay, *refs),
        "mix",
        [SMEM] + [VMEM] * 4,
        (shape((tok, lay.meta), BF),) * groups,
        (6 * span * came * width, 2 * came * width),
        [pltpu.VMEM((groups, tok, lay.meta), BF)],
    )(at, back_high, back_low, seats, meta)
    return run(
        lambda *refs: join_kernel(lay, *refs),
        "join",
        [SMEM] + [VMEM] * groups,
        shape((tok, model), BF),
        (tok * model, 4 * tok * model),
        [pltpu.VMEM((groups, tok, lay.meta), BF)],
    )(at, *swap(home))


def solution(mesh):
    split = Mesh(
        mesh.devices.reshape(mesh.shape["attn"], 4, 4, 2),
        ("attn", "expert_0", "expert_1", "expert_2"),
    )
    return jax.shard_map(
        on_device,
        mesh=split,
        in_specs=(
            P(ATTN_EXPERT, None),
            P(ATTN_EXPERT, None),
            P(ATTN_EXPERT, None),
            P(),
            P(),
            P(EXPERT, None, "attn"),
            P(EXPERT, None, "attn"),
            P(EXPERT, "attn", None),
        ),
        out_specs=P(ATTN_EXPERT, None),
        check_vma=False,
    )
```

```python
import jax
import jax.numpy as jnp
from jax import lax
from jax.experimental import pallas as pl
from jax.experimental.pallas import tpu as pltpu
from jax.sharding import Mesh
from jax.sharding import PartitionSpec as P

SHED_MOST = 4
ATTN_EXPERT = ("attn", "expert_0", "expert_1", "expert_2")
EXPERT = ("expert_0", "expert_1", "expert_2")
SWISH_SCALE = 1.702
BF = jnp.bfloat16
F32 = jnp.float32

def iota(shape, dim):
    return lax.broadcasted_iota(jnp.int32, shape, dim)


def dot(a, b, dims=((1,), (0,))):
    return lax.dot_general(a, b, (dims, ((), ())), preferred_element_type=F32)


def half(n):
    return (n // 2 + 15) // 16 * 16


def by_distance(at_ref, store_ref, outs):
    for r, out in enumerate(outs):
        out[...] = store_ref[lax.rem(at_ref[0] + r, len(outs))]


def from_distance(at_ref, store_ref, ins):
    for r, block in enumerate(ins):
        store_ref[lax.rem(at_ref[0] + r, len(ins))] = block[...]


def cut_kernel(lay, at_ref, x_ref, id_ref, p_ref, *refs):
    outs, store_ref = refs[:-1], refs[-1]
    prob = p_ref[...]
    high = prob.astype(BF).astype(F32)
    rest = prob - high
    middle = rest.astype(BF).astype(F32)
    meta = jnp.concatenate([id_ref[...].astype(F32), high, middle, rest - middle], axis=0)
    meta = meta.T.astype(BF)
    tok = x_ref.shape[0]
    for b in range(len(outs)):
        first = b * lay.width
        store_ref[b, :, : lay.width] = x_ref[:, first : first + lay.width]
        store_ref[b, :, lay.width : lay.meta] = jnp.ones((tok, 1), BF)
        store_ref[b, :, lay.meta :] = meta
    by_distance(at_ref, store_ref, outs)


def send_kernel(lay, at_ref, xa, xb, xc, xd, s_ref, r_ref, m_ref, store_ref):
    from_distance(at_ref, store_ref, (xa, xb, xc, xd))
    tok = xa.shape[0]
    span = m_ref.shape[0]
    x = store_ref[...].reshape(span, store_ref.shape[2])
    m_ref[...] = x[:, lay.meta :]
    ids = x[:, lay.meta : lay.meta + lay.top].astype(F32)
    experts = s_ref.shape[0] // lay.per
    lane = iota((span, experts), 1).astype(F32)
    named = [ids[:, k : k + 1] == lane for k in range(lay.top)]
    hits = jnp.where(named[0], 1.0, 0.0)
    for k in range(1, lay.top):
        hits += jnp.where(named[k], 1.0, 0.0)
    r, c = iota((span, span), 0), iota((span, span), 1)
    before = jnp.logical_and(r // tok == c // tok, c < r).astype(BF)
    order = dot(before, hits.astype(BF))
    group = (iota((span, 1), 0) // tok * lay.most).astype(F32)
    place = iota((span, experts * lay.per), 1).astype(F32)
    hot = None
    for k in range(lay.top):
        seat = jnp.sum(jnp.where(named[k], order, 0.0), axis=1, keepdims=True)
        seat = seat + ids[:, k : k + 1] * lay.per + group
        r_ref[:, k : k + 1] = seat
        here = jnp.where(seat == place, 1.0, 0.0)
        hot = here if k == 0 else hot + here
    hot = hot.astype(BF)
    s_ref[...] = dot(hot, x[:, : lay.meta], ((0,), (0,))).astype(BF)


def pick_kernel(lay, groups, x_ref, par_ref, col_ref, *outs):
    came = x_ref.shape[0]
    blocks = came // lay.per
    bound = par_ref[0].astype(F32)
    start = lay.width // 128 * 128
    tail = x_ref[:, start:]
    choose = (iota((8, tail.shape[1]), 1) == lay.width - start).astype(BF)
    flags = dot(choose, tail, ((1,), (1,)))[0:1]
    row = iota((1, came), 1)
    group, order = row % lay.per // lay.most, (row % lay.most).astype(F32)
    owner = iota((blocks, came), 0) == iota((blocks, came), 1) // lay.per
    split = jnp.where(owner, flags, 0.0).astype(BF)
    member = iota((came, 128), 0) % lay.per // lay.most == iota((came, 128), 1)
    counts = dot(split, member.astype(BF)).astype(BF)
    rb, cb = iota((blocks, blocks), 0), iota((blocks, blocks), 1)
    rl, cl = iota((128, 128), 0), iota((128, 128), 1)
    lower = dot(counts, (rl < cl).astype(BF)).astype(BF)
    offset = dot((cb < rb).astype(BF), counts) + dot(jnp.ones((blocks, blocks), BF), lower)
    spread = jnp.zeros((blocks, came), F32)
    for a in range(groups):
        spread += jnp.where(group == a, offset[:, a : a + 1], 0.0)
    rank = jnp.sum(jnp.where(owner, spread, 0.0), axis=0, keepdims=True) + order
    slot = jnp.where(jnp.logical_and(flags > 0.5, rank < bound), rank, -1.0)
    col_ref[...] = jnp.broadcast_to(slot, (8, came)).T
    first = 0
    for high, low in zip(outs[::2], outs[1::2]):
        slots = high.shape[1]
        place = (iota((slots, came), 0) + first).astype(F32)
        hot = jnp.where(slot == place, 1.0, 0.0).astype(BF)
        share_out(dot(hot, x_ref[:, : lay.width]).astype(BF).T, (high, low))
        first += slots


def whole(*parts):
    return jnp.concatenate([part[...] for part in parts], axis=0)


def relay_kernel(seen_ref, g_ref, u_ref, d_ref, go_ref, uo_ref, do_ref):
    del seen_ref
    blocks, width = go_ref.shape[0], go_ref.shape[2]
    for b in range(blocks):
        at = slice(b * width, (b + 1) * width)
        go_ref[b] = g_ref[:, at]
        uo_ref[b] = u_ref[:, at]
        do_ref[b] = d_ref[:, at].T


def mid_kernel(at_ref, oh, ol, lh, ll, rh, rl, ga, gb, gc, ua, ub, uc, g_ref, u_ref):
    del at_ref
    gate = up = None
    for n, (x, g, u) in enumerate(
        ((whole(oh, ol), ga, ua), (whole(lh, ll), gb, ub), (whole(rh, rl), gc, uc))
    ):
        g, u = dot(g[0], x), dot(u[0], x)
        gate, up = (g, u) if n == 0 else (gate + g, up + u)
    g_ref[...] = gate
    u_ref[...] = up


def share_out(values, refs):
    first = 0
    for ref in refs:
        ref[...] = values[first : first + ref.shape[0]].astype(ref.dtype)
        first += ref.shape[0]


def far_kernel(at_ref, g_ref, u_ref, fh, fl, wg_ref, wu_ref, wd_ref, h_ref, *outs):
    del at_ref
    x = whole(fh, fl)
    gate = g_ref[...] + dot(wg_ref[0], x)
    up = u_ref[...] + dot(wu_ref[0], x)
    hidden = (gate * jax.nn.sigmoid(SWISH_SCALE * gate) * (up + 1.0)).astype(BF)
    h_ref[...] = hidden
    share_out(dot(wd_ref[0], hidden), outs)


def near_kernel(at_ref, h_ref, da, db, dc, *outs):
    del at_ref
    hidden = h_ref[...]
    share_out(dot(db[0], hidden), outs[0:2])
    share_out(dot(dc[0], hidden), outs[2:4])
    share_out(dot(da[0], hidden), outs[4:5])


def place_kernel(slot_ref, *refs):
    ins, z_ref = refs[:-1], refs[-1]
    came = z_ref.shape[0]
    columns = []
    for own, lh, ll, rh, rl in (ins[:5], ins[5:]):
        total = own[...] + whole(lh, ll).astype(F32) + whole(rh, rl).astype(F32)
        columns.append(total.astype(BF))
    y = jnp.concatenate(columns, axis=1)
    hot = jnp.where(slot_ref[:, 0:1] == iota((came, y.shape[1]), 1).astype(F32), 1.0, 0.0)
    z_ref[...] = dot(hot.astype(BF), y, ((1,), (1,))).astype(BF)


def mix_kernel(lay, at_ref, b_ref, r_ref, m_ref, *refs):
    outs, store_ref = refs[:-1], refs[-1]
    span, tok = m_ref.shape[0], outs[0].shape[0]
    place = iota((span, b_ref.shape[0]), 1).astype(F32)
    here = [r_ref[:, k : k + 1] == place for k in range(lay.top)]
    total = None
    for part in range(3):
        first = (1 + part) * lay.top
        weight = jnp.zeros(place.shape, F32)
        for k in range(lay.top):
            weight += jnp.where(here[k], m_ref[:, first + k : first + k + 1].astype(F32), 0.0)
        piece = dot(weight.astype(BF), b_ref[...])
        total = piece if part == 0 else total + piece
    for g in range(len(outs)):
        store_ref[g] = total[g * tok : (g + 1) * tok].astype(BF)
    by_distance(at_ref, store_ref, outs)


def join_kernel(lay, at_ref, *refs):
    ins, out_ref, store_ref = refs[:-2], refs[-2], refs[-1]
    from_distance(at_ref, store_ref, ins)
    for b in range(len(ins)):
        out_ref[:, b * lay.width : (b + 1) * lay.width] = store_ref[b]


VMEM = pl.BlockSpec(memory_space=pltpu.VMEM)
SMEM = pl.BlockSpec(memory_space=pltpu.SMEM)
ANY = pl.BlockSpec(memory_space=pl.ANY)
shape = jax.ShapeDtypeStruct


class Layout:
    def __init__(self, width, top, most, groups):
        self.width, self.top, self.most, self.per = width, top, most, groups * most
        self.meta = width + 1
        self.lanes = self.meta + 4 * top


def cost(flops, moved):
    return pl.CostEstimate(flops=flops, bytes_accessed=moved, transcendentals=0)


def grant(mebibytes):
    return pltpu.CompilerParams(vmem_limit_bytes=mebibytes << 20)


def run(kernel, name, ins, outs, work, scratch=(), mebibytes=24):
    return pl.pallas_call(
        kernel,
        out_shape=outs,
        in_specs=ins,
        out_specs=jax.tree.map(lambda _: VMEM, outs),
        scratch_shapes=scratch,
        cost_estimate=cost(*work),
        compiler_params=grant(mebibytes),
        name=name,
    )


def on_device(
    tokens, expert_ids, gate_probs, shed_blocks, partner, gate_weight, up_weight, down_weight
):
    tok, model = tokens.shape
    top = expert_ids.shape[1]
    experts = shed_blocks.shape[0]
    groups = lax.axis_size("attn")
    width = model // groups
    capacity = tok * top * groups
    block = capacity // 8
    slots = capacity + block * SHED_MOST
    span = groups * tok
    units = gate_weight.shape[2]
    lay = Layout(width, top, min(tok, 3 * tok * top // experts), groups)
    cut = half(width)
    rest = width - cut
    came = experts * lay.per
    me = lax.axis_index(EXPERT)
    bound = capacity - block * shed_blocks[partner[me]] + block * shed_blocks[me]
    par = bound.reshape(1).astype(jnp.int32)
    at = lax.axis_index("attn").astype(jnp.int32).reshape(1)

    def shifted(distance):
        pairs = [(i, (i + distance) % groups) for i in range(groups)]
        return lambda array: lax.ppermute(array, "attn", pairs)

    right, left = shifted(1), shifted(groups - 1)

    def swap(blocks):
        moved = [blocks[0]] + [shifted(r)(blocks[r]) for r in range(1, groups)]
        return [moved[(groups - r) % groups] for r in range(groups)]

    def exchange(rows):
        blocks = rows.reshape(experts, lay.per, rows.shape[1])
        moved = lax.all_to_all(blocks, EXPERT, split_axis=0, concat_axis=0, tiled=True)
        return moved.reshape(rows.shape)

    piece = shape((tok, lay.lanes), BF)
    blocks = run(
        lambda *refs: cut_kernel(lay, *refs),
        "cut",
        [SMEM, VMEM, VMEM, VMEM],
        (piece,) * groups,
        (tok * model, 4 * tok * model),
        [pltpu.VMEM((groups, tok, lay.lanes), BF)],
    )(at, tokens, expert_ids.T, gate_probs.T)
    outgoing, seats, meta = run(
        lambda *refs: send_kernel(lay, *refs),
        "send",
        [SMEM] + [VMEM] * 4,
        (
            shape((came, lay.meta), BF),
            shape((span, top), F32),
            shape((span, 4 * top), BF),
        ),
        (2 * span * came * width, 2 * came * width),
        [pltpu.VMEM((groups, tok, lay.lanes), BF)],
    )(at, *swap(blocks))
    arrived = exchange(outgoing)
    relaid = shape((groups, units, width), BF)
    wg, wu, wd = run(
        relay_kernel,
        "relay",
        [ANY] + [VMEM] * 3,
        (relaid, relaid, shape((groups, width, units), BF)),
        (12 * slots * width * units, 12 * model * units),
        mebibytes=40,
    )(seats, gate_weight[0].T, up_weight[0].T, down_weight[0])
    arrived, wg, wu, wd = lax.optimization_barrier((arrived, wg, wu, wd))

    tile = 256
    parts = (2 * tile, slots - 2 * tile)
    gather_work = (2 * slots * came * width, 2 * came * width)
    slot, *own = run(
        lambda *refs: pick_kernel(lay, groups, *refs),
        "pick",
        [VMEM, SMEM],
        (shape((came, 8), F32), *(shape((n, p), BF) for p in parts for n in (cut, rest))),
        gather_work,
    )(arrived, par)
    lane = lambda rows: pl.BlockSpec((rows, tile), lambda i, p: (0, i))

    def weight(rows, columns, ahead):
        return pl.BlockSpec((1, rows, columns), lambda i, p: (lax.rem(p[0] + ahead, groups), 0, 0))

    def staged(kernel, name, ins, outs, flops, moved):
        return pl.pallas_call(
            kernel,
            grid_spec=pltpu.PrefetchScalarGridSpec(
                num_scalar_prefetch=1,
                grid=(outs[0].shape[1] // tile,),
                in_specs=ins,
                out_specs=tuple(lane(out.shape[0]) for out in outs),
            ),
            out_shape=outs,
            cost_estimate=cost(flops, moved),
            compiler_params=grant(32),
            name=name,
        )

    before, after, across = groups - 1, 1, groups // 2
    halves = [lane(cut), lane(rest)]
    opposite = weight(units, width, across)
    area = width * units

    def ring(name, part, oh, ol):
        rows = lambda n, kind: shape((n, part), kind)
        ll, rh = right(ol), left(oh)
        lh, rl = right(oh), left(ol)
        fl, fh = right(ll), left(rh)
        gate, up = staged(
            mid_kernel,
            "mid" + name,
            halves * 3 + [weight(units, width, d) for d in (0, before, after)] * 2,
            (rows(units, F32), rows(units, F32)),
            12 * part * area,
            12 * area,
        )(at, oh, ol, lh, ll, rh, rl, wg, wg, wg, wu, wu, wu)
        return staged(
            far_kernel,
            "far" + name,
            [lane(units)] * 2 + halves + [opposite, opposite, weight(width, units, across)],
            (rows(units, BF), rows(cut, BF), rows(rest, BF)),
            6 * part * area,
            6 * area,
        )(at, gate, up, fh, fl, wg, wu, wd)

    def ring_sum(name, part, hidden, far_high, far_low):
        rows = lambda n, kind: shape((n, part), kind)
        to_right, to_left = right(far_low), left(far_high)
        left_high, left_low, right_high, right_low, mine = staged(
            near_kernel,
            "near" + name,
            [lane(units)] + [weight(width, units, d) for d in (0, before, after)],
            (rows(cut, F32), rows(rest, BF), rows(cut, BF), rows(rest, F32), rows(width, F32)),
            6 * part * area,
            6 * area,
        )(at, hidden, wd, wd, wd)
        lh, rl = right(right_high), left(left_low)
        ll = right((right_low + to_right.astype(F32)).astype(BF))
        rh = left((left_high + to_left.astype(F32)).astype(BF))
        return mine, lh, ll, rh, rl

    first = ring("_a", parts[0], *own[:2])
    second = ring("_b", parts[1], *own[2:])
    sums = ring_sum("_a", parts[0], *first) + ring_sum("_b", parts[1], *second)
    answers = run(
        place_kernel, "place", [VMEM] * 11, shape((came, width), BF), gather_work
    )(slot, *sums)
    returned = exchange(answers)
    home = run(
        lambda *refs: mix_kernel(lay, *refs),
        "mix",
        [SMEM] + [VMEM] * 3,
        (shape((tok, width), BF),) * groups,
        (6 * span * came * width, 2 * came * width),
        [pltpu.VMEM((groups, tok, width), BF)],
    )(at, returned, seats, meta)
    return run(
        lambda *refs: join_kernel(lay, *refs),
        "join",
        [SMEM] + [VMEM] * groups,
        shape((tok, model), BF),
        (tok * model, 4 * tok * model),
        [pltpu.VMEM((groups, tok, width), BF)],
    )(at, *swap(home))


def solution(mesh):
    split = Mesh(
        mesh.devices.reshape(mesh.shape["attn"], 4, 4, 2),
        ("attn", "expert_0", "expert_1", "expert_2"),
    )
    return jax.shard_map(
        on_device,
        mesh=split,
        in_specs=(
            P(ATTN_EXPERT, None),
            P(ATTN_EXPERT, None),
            P(ATTN_EXPERT, None),
            P(),
            P(),
            P(EXPERT, None, "attn"),
            P(EXPERT, None, "attn"),
            P(EXPERT, "attn", None),
        ),
        out_specs=P(ATTN_EXPERT, None),
        check_vma=False,
    )
```

```python
import jax
import jax.numpy as jnp
from jax import lax
from jax.experimental import pallas as pl
from jax.experimental.pallas import tpu as pltpu
from jax.sharding import Mesh
from jax.sharding import PartitionSpec as P

SHED_MOST = 4
ATTN_EXPERT = ("attn", "expert_0", "expert_1", "expert_2")
EXPERT = ("expert_0", "expert_1", "expert_2")
SWISH_SCALE = 1.702
BF = jnp.bfloat16
F32 = jnp.float32

def iota(shape, dim):
    return lax.broadcasted_iota(jnp.int32, shape, dim)


def dot(a, b, dims=((1,), (0,))):
    return lax.dot_general(a, b, (dims, ((), ())), preferred_element_type=F32)


def half(n):
    return (n // 2 + 15) // 16 * 16


def hot(places, width, first=0):
    at = (iota((places.shape[0], width), 1) + first).astype(F32)
    return jnp.where(places == at, 1.0, 0.0)


def send_kernel(lay, x_ref, id_ref, s_ref):
    tok, experts, seats = x_ref.shape[0], lay.experts, lay.seats
    ids = id_ref[...].astype(F32)
    expert = iota((experts, tok), 0).astype(F32)
    hits = jnp.zeros((experts, tok), F32)
    for k in range(ids.shape[0]):
        hits += jnp.where(ids[k : k + 1] == expert, 1.0, 0.0)
    earlier = (iota((tok, tok), 0) < iota((tok, tok), 1)).astype(BF)
    order = dot(hits.astype(BF), earlier)
    order = jnp.where(hits > 0.5, order, -1.0).astype(BF)
    rows = experts * seats
    spread = (iota((rows, experts), 0) // seats == iota((rows, experts), 1)).astype(BF)
    order = dot(spread, order)
    seat = iota((rows, tok), 0) % seats
    over = (seats + seat // 2).astype(F32)
    full = jnp.where(order == seat.astype(F32), 1.0, 0.0).astype(BF)
    part = jnp.where(order == over, 1.0, 0.0)
    even = jnp.where(seat % 2 == 0, part, 0.0).astype(BF)
    odd = jnp.where(seat % 2 == 1, part, 0.0).astype(BF)
    one, none = jnp.ones((tok, 1), BF), lambda n: jnp.zeros((tok, n), BF)
    second = jnp.concatenate([none(lay.width + 1), one, none(lay.low - lay.width - 2)], axis=1)
    flags = dot(part.astype(BF), second)
    for b in range(x_ref.shape[1] // lay.width):
        first = b * lay.width
        x = x_ref[:, first : first + lay.width]
        at = slice(b * rows, (b + 1) * rows)
        wide = jnp.concatenate([x, one, none(lay.low - lay.width - 1)], axis=1)
        s_ref[at, : lay.low] = (dot(full, wide) + flags).astype(BF)
        tail = jnp.concatenate([x[:, lay.point :], none(lay.short)], axis=1)
        s_ref[at, lay.low :] = (dot(even, x[:, : lay.point]) + dot(odd, tail)).astype(BF)


def pick_kernel(lay, x_ref, par_ref, col_ref, *outs):
    came, seats = x_ref.shape[0], lay.seats
    sources = came // seats
    bound = par_ref[0].astype(F32)
    start = lay.width // 128 * 128
    tail = x_ref[:, start : lay.low]
    choose = (iota((8, tail.shape[1]), 1) == iota((8, tail.shape[1]), 0) + lay.width - start)
    flags = dot(choose.astype(BF), tail, ((1,), (1,)))
    full, part = flags[0:1], flags[1:2]
    seat = iota((1, came), 1) % seats
    even = seat % 2 == 0
    owner = iota((sources, came), 0) == iota((sources, came), 1) // seats
    each = full + jnp.where(even, part, 0.0)
    counts = jnp.sum(jnp.where(owner, each, 0.0), axis=1, keepdims=True)
    counts = jnp.broadcast_to(counts, (sources, 128)).astype(BF)
    earlier = (iota((sources, sources), 1) < iota((sources, sources), 0)).astype(BF)
    before = dot(earlier, counts)[:, 0:1]
    base = jnp.sum(jnp.where(owner, before, 0.0), axis=0, keepdims=True)
    rank = base + seat.astype(F32)
    over = base + (seats + seat // 2).astype(F32)
    rank = jnp.where(jnp.logical_and(full > 0.5, rank < bound), rank, -1.0)
    over = jnp.where(jnp.logical_and(part > 0.5, over < bound), over, -1.0)
    evens, odds = jnp.where(even, over, -1.0), jnp.where(even, -1.0, over)
    nothing = jnp.full((5, came), -1.0, F32)
    col_ref[...] = jnp.concatenate([rank, evens, odds, nothing], axis=0).T
    first = 0
    for high, low in zip(outs[::2], outs[1::2]):
        slots = high.shape[1]
        place = (iota((slots, came), 0) + first).astype(F32)
        match = lambda row: jnp.where(row == place, 1.0, 0.0).astype(BF)
        got = dot(match(rank), x_ref[:, : lay.width])
        rest = x_ref[:, lay.low :]
        left, right = dot(match(evens), rest), dot(match(odds), rest)
        extra = jnp.concatenate([left, right[:, : lay.width - lay.point]], axis=1)
        share_out((got + extra).astype(BF).T, (high, low))
        first += slots


def whole(*parts):
    return jnp.concatenate([part[...] for part in parts], axis=0)


def relay_kernel(seen_ref, g_ref, u_ref, d_ref, go_ref, uo_ref, do_ref):
    del seen_ref
    blocks, width = go_ref.shape[0], go_ref.shape[2]
    for b in range(blocks):
        at = slice(b * width, (b + 1) * width)
        go_ref[b] = g_ref[:, at]
        uo_ref[b] = u_ref[:, at]
        do_ref[b] = d_ref[:, at].T


def mid_kernel(at_ref, oh, ol, lh, ll, rh, rl, ga, gb, gc, ua, ub, uc, g_ref, u_ref):
    del at_ref
    gate = up = None
    for n, (x, g, u) in enumerate(
        ((whole(oh, ol), ga, ua), (whole(lh, ll), gb, ub), (whole(rh, rl), gc, uc))
    ):
        g, u = dot(g[0], x), dot(u[0], x)
        gate, up = (g, u) if n == 0 else (gate + g, up + u)
    g_ref[...] = gate
    u_ref[...] = up


def share_out(values, refs):
    first = 0
    for ref in refs:
        ref[...] = values[first : first + ref.shape[0]].astype(ref.dtype)
        first += ref.shape[0]


def far_kernel(at_ref, g_ref, u_ref, fh, fl, wg_ref, wu_ref, wd_ref, h_ref, *outs):
    del at_ref
    x = whole(fh, fl)
    gate = g_ref[...] + dot(wg_ref[0], x)
    up = u_ref[...] + dot(wu_ref[0], x)
    hidden = (gate * jax.nn.sigmoid(SWISH_SCALE * gate) * (up + 1.0)).astype(BF)
    h_ref[...] = hidden
    share_out(dot(wd_ref[0], hidden), outs)


def near_kernel(at_ref, h_ref, da, db, dc, *outs):
    del at_ref
    hidden = h_ref[...]
    share_out(dot(db[0], hidden), outs[0:2])
    share_out(dot(dc[0], hidden), outs[2:4])
    share_out(dot(da[0], hidden), outs[4:5])


def place_kernel(lay, slot_ref, *refs):
    ins, z_ref = refs[:-1], refs[-1]
    columns = []
    for own, lh, ll, rh, rl in (ins[:5], ins[5:]):
        total = own[...] + whole(lh, ll).astype(F32) + whole(rh, rl).astype(F32)
        columns.append(total.astype(BF))
    y = jnp.concatenate(columns, axis=1)
    slots, came = y.shape[1], z_ref.shape[0]
    at = lambda k: hot(slot_ref[:, k : k + 1], slots).astype(BF)
    none = lambda n: jnp.zeros((came, n), BF)
    rows = dot(at(0), y, ((1,), (1,))).astype(BF)
    z_ref[:, : lay.low] = jnp.concatenate([rows, none(lay.low - lay.width)], axis=1)
    left = dot(at(1), y[: lay.point], ((1,), (1,))).astype(BF)
    right = dot(at(2), y[lay.point :], ((1,), (1,))).astype(BF)
    z_ref[:, lay.low :] = left + jnp.concatenate([right, none(lay.short)], axis=1)


def mix_kernel(lay, b_ref, id_ref, p_ref, o_ref):
    tok, seats = o_ref.shape[0], lay.seats
    ids, prob = id_ref[...].astype(F32).T, p_ref[...].T
    top = ids.shape[1]
    lane = iota((tok, lay.experts), 1).astype(F32)
    named = [ids[:, k : k + 1] == lane for k in range(top)]
    hits = jnp.zeros((tok, lay.experts), F32)
    for k in range(top):
        hits += jnp.where(named[k], 1.0, 0.0)
    earlier = (iota((tok, tok), 1) < iota((tok, tok), 0)).astype(BF)
    order = dot(earlier, hits.astype(BF))
    rows = lay.experts * seats
    kinds = [jnp.zeros((tok, rows), F32) for _ in range(3)]
    for k in range(top):
        seat = jnp.sum(jnp.where(named[k], order, 0.0), axis=1, keepdims=True)
        base = ids[:, k : k + 1] * seats
        full = jnp.where(seat < seats, base + seat, -1.0)
        over = jnp.where(seat < seats, -1.0, base + 2.0 * (seat - seats))
        odd = jnp.where(seat < seats, -1.0, over + 1.0)
        for n, place in enumerate((full, over, odd)):
            kinds[n] += hot(place, rows) * prob[:, k : k + 1]
    weights = []
    for kind in kinds:
        high = kind.astype(BF)
        rest = kind - high.astype(F32)
        middle = rest.astype(BF)
        low = (rest - middle.astype(F32)).astype(BF)
        weights.append(jnp.concatenate([high, middle, low], axis=0))

    def weighted(n, block):
        three = dot(weights[n], block)
        return three[:tok] + three[tok : 2 * tok] + three[2 * tok :]

    for b in range(o_ref.shape[1] // lay.width):
        at = slice(b * rows, (b + 1) * rows)
        whole_rows = weighted(0, b_ref[at, : lay.width])
        rest = b_ref[at, lay.low :]
        left, right = weighted(1, rest), weighted(2, rest)
        extra = jnp.concatenate([left, right[:, : lay.width - lay.point]], axis=1)
        o_ref[:, b * lay.width : (b + 1) * lay.width] = (whole_rows + extra).astype(BF)


VMEM = pl.BlockSpec(memory_space=pltpu.VMEM)
SMEM = pl.BlockSpec(memory_space=pltpu.SMEM)
ANY = pl.BlockSpec(memory_space=pl.ANY)
shape = jax.ShapeDtypeStruct


class Layout:
    def __init__(self, width, experts, most):
        self.width, self.experts = width, experts
        self.seats = 8
        self.low = (width + 2 + 127) // 128 * 128
        self.point = (width // 2 + 127) // 128 * 128
        self.short = 2 * self.point - width
        self.lanes = self.low + self.point
        assert self.seats <= most <= self.seats * 3 // 2


def cost(flops, moved):
    return pl.CostEstimate(flops=flops, bytes_accessed=moved, transcendentals=0)


def grant(mebibytes):
    return pltpu.CompilerParams(vmem_limit_bytes=mebibytes << 20)


def run(kernel, name, ins, outs, work, scratch=(), mebibytes=24):
    return pl.pallas_call(
        kernel,
        out_shape=outs,
        in_specs=ins,
        out_specs=jax.tree.map(lambda _: VMEM, outs),
        scratch_shapes=scratch,
        cost_estimate=cost(*work),
        compiler_params=grant(mebibytes),
        name=name,
    )


def on_device(
    tokens, expert_ids, gate_probs, shed_blocks, partner, gate_weight, up_weight, down_weight
):
    tok, model = tokens.shape
    top = expert_ids.shape[1]
    experts = shed_blocks.shape[0]
    groups = lax.axis_size("attn")
    width = model // groups
    capacity = tok * top * groups
    block = capacity // 8
    slots = capacity + block * SHED_MOST
    units = gate_weight.shape[2]
    lay = Layout(width, experts, min(tok, 3 * tok * top // experts))
    cut = half(width)
    rest = width - cut
    devices = groups * experts
    came = devices * lay.seats
    me = lax.axis_index(EXPERT)
    bound = capacity - block * shed_blocks[partner[me]] + block * shed_blocks[me]
    par = bound.reshape(1).astype(jnp.int32)
    at = lax.axis_index("attn").astype(jnp.int32).reshape(1)

    def shifted(distance):
        pairs = [(i, (i + distance) % groups) for i in range(groups)]
        return lambda array: lax.ppermute(array, "attn", pairs)

    right, left = shifted(1), shifted(groups - 1)

    def exchange(rows):
        blocks = rows.reshape(devices, lay.seats, lay.lanes)
        moved = lax.all_to_all(blocks, ATTN_EXPERT, split_axis=0, concat_axis=0, tiled=True)
        return moved.reshape(came, lay.lanes)

    packed = shape((came, lay.lanes), BF)
    outgoing = run(
        lambda *refs: send_kernel(lay, *refs),
        "send",
        [VMEM] * 2,
        packed,
        (2 * tok * came * width, 2 * came * width),
    )(tokens, expert_ids.T)
    arrived = exchange(outgoing)
    relaid = shape((groups, units, width), BF)
    wg, wu, wd = run(
        relay_kernel,
        "relay",
        [ANY] + [VMEM] * 3,
        (relaid, relaid, shape((groups, width, units), BF)),
        (12 * slots * width * units, 12 * model * units),
        mebibytes=40,
    )(outgoing, gate_weight[0].T, up_weight[0].T, down_weight[0])
    arrived, wg, wu, wd = lax.optimization_barrier((arrived, wg, wu, wd))

    tile = 256
    parts = (2 * tile, slots - 2 * tile)
    gather_work = (2 * slots * came * width, 2 * came * width)
    slot, *own = run(
        lambda *refs: pick_kernel(lay, *refs),
        "pick",
        [VMEM, SMEM],
        (shape((came, 8), F32), *(shape((n, p), BF) for p in parts for n in (cut, rest))),
        gather_work,
    )(arrived, par)
    lane = lambda rows: pl.BlockSpec((rows, tile), lambda i, p: (0, i))

    def weight(rows, columns, ahead):
        return pl.BlockSpec((1, rows, columns), lambda i, p: (lax.rem(p[0] + ahead, groups), 0, 0))

    def staged(kernel, name, ins, outs, flops, moved):
        return pl.pallas_call(
            kernel,
            grid_spec=pltpu.PrefetchScalarGridSpec(
                num_scalar_prefetch=1,
                grid=(outs[0].shape[1] // tile,),
                in_specs=ins,
                out_specs=tuple(lane(out.shape[0]) for out in outs),
            ),
            out_shape=outs,
            cost_estimate=cost(flops, moved),
            compiler_params=grant(32),
            name=name,
        )

    before, after, across = groups - 1, 1, groups // 2
    halves = [lane(cut), lane(rest)]
    opposite = weight(units, width, across)
    area = width * units

    def ring(name, part, oh, ol):
        rows = lambda n, kind: shape((n, part), kind)
        ll, rh = right(ol), left(oh)
        lh, rl = right(oh), left(ol)
        fl, fh = right(ll), left(rh)
        gate, up = staged(
            mid_kernel,
            "mid" + name,
            halves * 3 + [weight(units, width, d) for d in (0, before, after)] * 2,
            (rows(units, F32), rows(units, F32)),
            12 * part * area,
            12 * area,
        )(at, oh, ol, lh, ll, rh, rl, wg, wg, wg, wu, wu, wu)
        return staged(
            far_kernel,
            "far" + name,
            [lane(units)] * 2 + halves + [opposite, opposite, weight(width, units, across)],
            (rows(units, BF), rows(cut, BF), rows(rest, BF)),
            6 * part * area,
            6 * area,
        )(at, gate, up, fh, fl, wg, wu, wd)

    def ring_sum(name, part, hidden, far_high, far_low):
        rows = lambda n, kind: shape((n, part), kind)
        to_right, to_left = right(far_low), left(far_high)
        left_high, left_low, right_high, right_low, mine = staged(
            near_kernel,
            "near" + name,
            [lane(units)] + [weight(width, units, d) for d in (0, before, after)],
            (rows(cut, F32), rows(rest, BF), rows(cut, BF), rows(rest, F32), rows(width, F32)),
            6 * part * area,
            6 * area,
        )(at, hidden, wd, wd, wd)
        lh, rl = right(right_high), left(left_low)
        ll = right((right_low + to_right.astype(F32)).astype(BF))
        rh = left((left_high + to_left.astype(F32)).astype(BF))
        return mine, lh, ll, rh, rl

    first = ring("_a", parts[0], *own[:2])
    second = ring("_b", parts[1], *own[2:])
    sums = ring_sum("_a", parts[0], *first) + ring_sum("_b", parts[1], *second)
    answers = run(
        lambda *refs: place_kernel(lay, *refs), "place", [VMEM] * 11, packed, gather_work
    )(slot, *sums)
    return run(
        lambda *refs: mix_kernel(lay, *refs),
        "mix",
        [VMEM] * 3,
        shape((tok, model), BF),
        (6 * tok * came * width, 2 * came * width),
    )(exchange(answers), expert_ids.T, gate_probs.T)


def solution(mesh):
    split = Mesh(
        mesh.devices.reshape(mesh.shape["attn"], 4, 4, 2),
        ("attn", "expert_0", "expert_1", "expert_2"),
    )
    return jax.shard_map(
        on_device,
        mesh=split,
        in_specs=(
            P(ATTN_EXPERT, None),
            P(ATTN_EXPERT, None),
            P(ATTN_EXPERT, None),
            P(),
            P(),
            P(EXPERT, None, "attn"),
            P(EXPERT, None, "attn"),
            P(EXPERT, "attn", None),
        ),
        out_specs=P(ATTN_EXPERT, None),
        check_vma=False,
    )
```

```python
import jax
import jax.numpy as jnp
from jax import lax
from jax.experimental import pallas as pl
from jax.experimental.pallas import tpu as pltpu
from jax.sharding import Mesh
from jax.sharding import PartitionSpec as P

SHED_MOST = 4
ATTN_EXPERT = ("attn", "expert_0", "expert_1", "expert_2")
EXPERT = ("expert_0", "expert_1", "expert_2")
SWISH_SCALE = 1.702
BF = jnp.bfloat16
F32 = jnp.float32


def iota(shape, dim):
    return lax.broadcasted_iota(jnp.int32, shape, dim)


def dot(a, b, dims=((1,), (0,))):
    return lax.dot_general(a, b, (dims, ((), ())), preferred_element_type=F32)


def half(n):
    return (n // 2 + 15) // 16 * 16


def hot(places, width, first=0):
    at = (iota((places.shape[0], width), 1) + first).astype(F32)
    return jnp.where(places == at, 1.0, 0.0)


def send_kernel(lay, x_ref, id_ref, s_ref, seen_ref):
    tok, experts, seats = x_ref.shape[0], lay.experts, lay.seats
    seen_ref[...] = jnp.zeros_like(seen_ref)
    ids = id_ref[...].astype(F32)
    expert = iota((experts, tok), 0).astype(F32)
    hits = jnp.zeros((experts, tok), F32)
    for k in range(ids.shape[0]):
        hits += jnp.where(ids[k : k + 1] == expert, 1.0, 0.0)
    earlier = (iota((tok, tok), 0) < iota((tok, tok), 1)).astype(BF)
    order = dot(hits.astype(BF), earlier)
    order = jnp.where(hits > 0.5, order, -1.0).astype(BF)
    rows = experts * seats
    spread = (iota((rows, experts), 0) // seats == iota((rows, experts), 1)).astype(BF)
    order = dot(spread, order)
    seat = iota((rows, tok), 0) % seats
    over = (seats + seat // 2).astype(F32)
    full = jnp.where(order == seat.astype(F32), 1.0, 0.0).astype(BF)
    part = jnp.where(order == over, 1.0, 0.0)
    even = jnp.where(seat % 2 == 0, part, 0.0).astype(BF)
    odd = jnp.where(seat % 2 == 1, part, 0.0).astype(BF)
    one, none = jnp.ones((tok, 1), BF), lambda n: jnp.zeros((tok, n), BF)
    second = jnp.concatenate([none(lay.width + 1), one, none(lay.low - lay.width - 2)], axis=1)
    flags = dot(part.astype(BF), second)
    for b in range(x_ref.shape[1] // lay.width):
        first = b * lay.width
        x = x_ref[:, first : first + lay.width]
        at = slice(b * rows, (b + 1) * rows)
        wide = jnp.concatenate([x, one, none(lay.low - lay.width - 1)], axis=1)
        s_ref[at, : lay.low] = (dot(full, wide) + flags).astype(BF)
        tail = jnp.concatenate([x[:, lay.point :], none(lay.short)], axis=1)
        s_ref[at, lay.low :] = (dot(even, x[:, : lay.point]) + dot(odd, tail)).astype(BF)


def gather_slots(lay, rows, x_ref, first, outs):
    slots = outs[0].shape[1]
    place = (iota((slots, x_ref.shape[0]), 0) + first).astype(F32)
    match = lambda row: jnp.where(row == place, 1.0, 0.0).astype(BF)
    got = dot(match(rows[0]), x_ref[:, : lay.width])
    rest = x_ref[:, lay.low :]
    left, right = dot(match(rows[1]), rest), dot(match(rows[2]), rest)
    extra = jnp.concatenate([left, right[:, : lay.width - lay.point]], axis=1)
    share_out((got + extra).astype(BF).T, outs)


def pick_more_kernel(lay, first, x_ref, row_ref, *outs):
    gather_slots(lay, [row_ref[k : k + 1] for k in range(3)], x_ref, first, outs)


def pick_kernel(lay, x_ref, par_ref, row_ref, col_ref, *outs):
    came, seats = x_ref.shape[0], lay.seats
    sources = came // seats
    bound = par_ref[0].astype(F32)
    start = lay.width // 128 * 128
    tail = x_ref[:, start : lay.low]
    choose = (iota((8, tail.shape[1]), 1) == iota((8, tail.shape[1]), 0) + lay.width - start)
    flags = dot(choose.astype(BF), tail, ((1,), (1,)))
    full, part = flags[0:1], flags[1:2]
    seat = iota((1, came), 1) % seats
    even = seat % 2 == 0
    owner = iota((sources, came), 0) == iota((sources, came), 1) // seats
    each = full + jnp.where(even, part, 0.0)
    counts = jnp.sum(jnp.where(owner, each, 0.0), axis=1, keepdims=True)
    counts = jnp.broadcast_to(counts, (sources, 128)).astype(BF)
    earlier = (iota((sources, sources), 1) < iota((sources, sources), 0)).astype(BF)
    before = dot(earlier, counts)[:, 0:1]
    base = jnp.sum(jnp.where(owner, before, 0.0), axis=0, keepdims=True)
    rank = base + seat.astype(F32)
    over = base + (seats + seat // 2).astype(F32)
    rank = jnp.where(jnp.logical_and(full > 0.5, rank < bound), rank, -1.0)
    over = jnp.where(jnp.logical_and(part > 0.5, over < bound), over, -1.0)
    evens, odds = jnp.where(even, over, -1.0), jnp.where(even, -1.0, over)
    nothing = jnp.full((5, came), -1.0, F32)
    every = jnp.concatenate([rank, evens, odds, nothing], axis=0)
    row_ref[...] = every
    col_ref[...] = every.T
    gather_slots(lay, (rank, evens, odds), x_ref, 0, outs)


def whole(*parts):
    return jnp.concatenate([part[...] for part in parts], axis=0)


def relay_kernel(seen_ref, g_ref, u_ref, d_ref, go_ref, uo_ref, do_ref):
    del seen_ref
    blocks, width = go_ref.shape[0], go_ref.shape[2]
    for b in range(blocks):
        at = slice(b * width, (b + 1) * width)
        go_ref[b] = g_ref[:, at]
        uo_ref[b] = u_ref[:, at]
        do_ref[b] = d_ref[:, at].T


def mid_kernel(at_ref, oh, ol, lh, ll, rh, rl, ga, gb, gc, ua, ub, uc, g_ref, u_ref):
    del at_ref
    gate = up = None
    for n, (x, g, u) in enumerate(
        ((whole(oh, ol), ga, ua), (whole(lh, ll), gb, ub), (whole(rh, rl), gc, uc))
    ):
        g, u = dot(g[0], x), dot(u[0], x)
        gate, up = (g, u) if n == 0 else (gate + g, up + u)
    g_ref[...] = gate
    u_ref[...] = up


def share_out(values, refs):
    first = 0
    for ref in refs:
        ref[...] = values[first : first + ref.shape[0]].astype(ref.dtype)
        first += ref.shape[0]


def far_kernel(at_ref, g_ref, u_ref, fh, fl, wg_ref, wu_ref, wd_ref, h_ref, *outs):
    del at_ref
    x = whole(fh, fl)
    gate = g_ref[...] + dot(wg_ref[0], x)
    up = u_ref[...] + dot(wu_ref[0], x)
    hidden = (gate * jax.nn.sigmoid(SWISH_SCALE * gate) * (up + 1.0)).astype(BF)
    h_ref[...] = hidden
    share_out(dot(wd_ref[0], hidden), outs)


def near_kernel(at_ref, h_ref, da, db, dc, *outs):
    del at_ref
    hidden = h_ref[...]
    share_out(dot(db[0], hidden), outs[0:2])
    share_out(dot(dc[0], hidden), outs[2:4])
    share_out(dot(da[0], hidden), outs[4:5])


def place_kernel(lay, slot_ref, *refs):
    ins, z_ref = refs[:-1], refs[-1]
    columns = []
    for own, lh, ll, rh, rl in (ins[:5], ins[5:]):
        total = own[...] + whole(lh, ll).astype(F32) + whole(rh, rl).astype(F32)
        columns.append(total.astype(BF))
    y = jnp.concatenate(columns, axis=1)
    slots, came = y.shape[1], z_ref.shape[0]
    at = lambda k: hot(slot_ref[:, k : k + 1], slots).astype(BF)
    none = lambda n: jnp.zeros((came, n), BF)
    rows = dot(at(0), y, ((1,), (1,))).astype(BF)
    z_ref[:, : lay.low] = jnp.concatenate([rows, none(lay.low - lay.width)], axis=1)
    left = dot(at(1), y[: lay.point], ((1,), (1,))).astype(BF)
    right = dot(at(2), y[lay.point :], ((1,), (1,))).astype(BF)
    z_ref[:, lay.low :] = left + jnp.concatenate([right, none(lay.short)], axis=1)


def mix_kernel(lay, b_ref, id_ref, p_ref, o_ref):
    tok, seats = o_ref.shape[0], lay.seats
    ids, prob = id_ref[...].astype(F32).T, p_ref[...].T
    top = ids.shape[1]
    lane = iota((tok, lay.experts), 1).astype(F32)
    named = [ids[:, k : k + 1] == lane for k in range(top)]
    hits = jnp.zeros((tok, lay.experts), F32)
    for k in range(top):
        hits += jnp.where(named[k], 1.0, 0.0)
    earlier = (iota((tok, tok), 1) < iota((tok, tok), 0)).astype(BF)
    order = dot(earlier, hits.astype(BF))
    rows = lay.experts * seats
    kinds = [jnp.zeros((tok, rows), F32) for _ in range(3)]
    for k in range(top):
        seat = jnp.sum(jnp.where(named[k], order, 0.0), axis=1, keepdims=True)
        base = ids[:, k : k + 1] * seats
        full = jnp.where(seat < seats, base + seat, -1.0)
        over = jnp.where(seat < seats, -1.0, base + 2.0 * (seat - seats))
        odd = jnp.where(seat < seats, -1.0, over + 1.0)
        for n, place in enumerate((full, over, odd)):
            kinds[n] += hot(place, rows) * prob[:, k : k + 1]
    weights = []
    for kind in kinds:
        high = kind.astype(BF)
        rest = kind - high.astype(F32)
        middle = rest.astype(BF)
        low = (rest - middle.astype(F32)).astype(BF)
        weights.append(jnp.concatenate([high, middle, low], axis=0))

    def weighted(n, block):
        three = dot(weights[n], block)
        return three[:tok] + three[tok : 2 * tok] + three[2 * tok :]

    for b in range(o_ref.shape[1] // lay.width):
        at = slice(b * rows, (b + 1) * rows)
        whole_rows = weighted(0, b_ref[at, : lay.width])
        rest = b_ref[at, lay.low :]
        left, right = weighted(1, rest), weighted(2, rest)
        extra = jnp.concatenate([left, right[:, : lay.width - lay.point]], axis=1)
        o_ref[:, b * lay.width : (b + 1) * lay.width] = (whole_rows + extra).astype(BF)


VMEM = pl.BlockSpec(memory_space=pltpu.VMEM)
SMEM = pl.BlockSpec(memory_space=pltpu.SMEM)
ANY = pl.BlockSpec(memory_space=pl.ANY)
shape = jax.ShapeDtypeStruct


class Layout:
    def __init__(self, width, experts, most):
        self.width, self.experts = width, experts
        self.seats = 8
        self.low = (width + 2 + 127) // 128 * 128
        self.point = (width // 2 + 127) // 128 * 128
        self.short = 2 * self.point - width
        self.lanes = self.low + self.point
        assert self.seats <= most <= self.seats * 3 // 2


def cost(flops, moved):
    return pl.CostEstimate(flops=flops, bytes_accessed=moved, transcendentals=0)


def grant(mebibytes):
    return pltpu.CompilerParams(vmem_limit_bytes=mebibytes << 20)


def run(kernel, ins, outs, work, scratch=(), mebibytes=24):
    return pl.pallas_call(
        kernel,
        out_shape=outs,
        in_specs=ins,
        out_specs=jax.tree.map(lambda _: VMEM, outs),
        scratch_shapes=scratch,
        cost_estimate=cost(*work),
        compiler_params=grant(mebibytes),
    )


def on_device(
    tokens, expert_ids, gate_probs, shed_blocks, partner, gate_weight, up_weight, down_weight
):
    tok, model = tokens.shape
    top = expert_ids.shape[1]
    experts = shed_blocks.shape[0]
    groups = lax.axis_size("attn")
    width = model // groups
    capacity = tok * top * groups
    block = capacity // 8
    slots = capacity + block * SHED_MOST
    units = gate_weight.shape[2]
    lay = Layout(width, experts, min(tok, 3 * tok * top // experts))
    cut = half(width)
    rest = width - cut
    devices = groups * experts
    came = devices * lay.seats
    me = lax.axis_index(EXPERT)
    bound = capacity - block * shed_blocks[partner[me]] + block * shed_blocks[me]
    par = bound.reshape(1).astype(jnp.int32)
    at = lax.axis_index("attn").astype(jnp.int32).reshape(1)

    def shifted(distance):
        pairs = [(i, (i + distance) % groups) for i in range(groups)]
        return lambda array: lax.ppermute(array, "attn", pairs)

    right, left = shifted(1), shifted(groups - 1)

    def exchange(rows):
        blocks = rows.reshape(devices, lay.seats, lay.lanes)
        moved = lax.all_to_all(blocks, ATTN_EXPERT, split_axis=0, concat_axis=0, tiled=True)
        return moved.reshape(came, lay.lanes)

    packed = shape((came, lay.lanes), BF)
    outgoing, seen = run(
        lambda *refs: send_kernel(lay, *refs),
        [VMEM] * 2,
        (packed, shape((8, 128), F32)),
        (2 * tok * came * width, 2 * came * width),
        mebibytes=60,
    )(tokens, expert_ids.T)
    arrived = exchange(outgoing)
    relaid = shape((groups, units, width), BF)
    step = 128
    rows_in = pl.BlockSpec((step, model), lambda i: (i, 0))
    rows_out = pl.BlockSpec((groups, step, width), lambda i: (0, i, 0))
    wg, wu, wd = pl.pallas_call(
        relay_kernel,
        grid=(pl.cdiv(units, step),),
        out_shape=(relaid, relaid, shape((groups, width, units), BF)),
        in_specs=[ANY] + [rows_in] * 3,
        out_specs=(rows_out, rows_out, pl.BlockSpec((groups, width, step), lambda i: (0, 0, i))),
        cost_estimate=cost(12 * slots * width * units, 12 * model * units),
        compiler_params=grant(60),
        name="relay",
    )(seen, gate_weight[0].T, up_weight[0].T, down_weight[0])
    arrived, wg, wu, wd = lax.optimization_barrier((arrived, wg, wu, wd))

    tile = 256
    parts = (tile, slots - tile)
    gather_work = (2 * slots * came * width, 2 * came * width)
    pieces = [tuple(shape((n, p), BF) for n in (cut, rest)) for p in parts]
    places, slot, *own = run(
        lambda *refs: pick_kernel(lay, *refs),
        [VMEM, SMEM],
        (shape((8, came), F32), shape((came, 8), F32), *pieces[0]),
        gather_work,
    )(arrived, par)
    more = run(
        lambda *refs: pick_more_kernel(lay, parts[0], *refs), [VMEM] * 2, pieces[1], gather_work
    )(arrived, places)
    lane = lambda rows: pl.BlockSpec((rows, tile), lambda i, p: (0, i))

    def weight(rows, columns, ahead):
        return pl.BlockSpec((1, rows, columns), lambda i, p: (lax.rem(p[0] + ahead, groups), 0, 0))

    def staged(kernel, ins, outs, flops, moved):
        return pl.pallas_call(
            kernel,
            grid_spec=pltpu.PrefetchScalarGridSpec(
                num_scalar_prefetch=1,
                grid=(outs[0].shape[1] // tile,),
                in_specs=ins,
                out_specs=tuple(lane(out.shape[0]) for out in outs),
            ),
            out_shape=outs,
            cost_estimate=cost(flops, moved),
            compiler_params=grant(32),
        )

    before, after, across = groups - 1, 1, groups // 2
    halves = [lane(cut), lane(rest)]
    opposite = weight(units, width, across)
    area = width * units

    def ring(part, oh, ol):
        rows = lambda n, kind: shape((n, part), kind)
        ll, rh = right(ol), left(oh)
        lh, rl = right(oh), left(ol)
        fl, fh = right(ll), left(rh)
        gate, up = staged(
            mid_kernel,
            halves * 3 + [weight(units, width, d) for d in (0, before, after)] * 2,
            (rows(units, F32), rows(units, F32)),
            12 * part * area,
            12 * area,
        )(at, oh, ol, lh, ll, rh, rl, wg, wg, wg, wu, wu, wu)
        return gate, up, fh, fl

    def far(part, gate, up, fh, fl):
        rows = lambda n, kind: shape((n, part), kind)
        return staged(
            far_kernel,
            [lane(units)] * 2 + halves + [opposite, opposite, weight(width, units, across)],
            (rows(units, BF), rows(cut, BF), rows(rest, BF)),
            6 * part * area,
            6 * area,
        )(at, gate, up, fh, fl, wg, wu, wd)

    def near(part, hidden):
        rows = lambda n, kind: shape((n, part), kind)
        return staged(
            near_kernel,
            [lane(units)] + [weight(width, units, d) for d in (0, before, after)],
            (rows(cut, F32), rows(rest, BF), rows(cut, BF), rows(rest, F32), rows(width, F32)),
            6 * part * area,
            6 * area,
        )(at, hidden, wd, wd, wd)

    def add(mine, came):
        return (mine + came.astype(F32)).astype(BF)

    first = ring(parts[0], *own)
    second = ring(parts[1], *more)
    first, ready = lax.optimization_barrier((first, second[:2]))
    second = (*ready, *second[2:])
    hidden_a, high_a, low_a = far(parts[0], *first)
    to_right_a, to_left_a = right(low_a), left(high_a)
    lha, lla, rha, rla, own_a = near(parts[0], hidden_a)
    straight_a = right(rha), left(lla)
    hidden_b, high_b, low_b = far(parts[1], *second)
    to_right_b, to_left_b = right(low_b), left(high_b)
    sum_right, sum_left = add(rla, to_right_a), add(lha, to_left_a)
    added_a = right(sum_right), left(sum_left)
    sums_a = own_a, straight_a[0], *added_a, straight_a[1]
    lhb, llb, rhb, rlb, own_b = near(parts[1], hidden_b)
    straight_b = right(rhb), left(llb)
    sums_b = (
        own_b,
        straight_b[0],
        right(add(rlb, to_right_b)),
        left(add(lhb, to_left_b)),
        straight_b[1],
    )
    sums = sums_a + sums_b
    answers = run(
        lambda *refs: place_kernel(lay, *refs), [VMEM] * 11, packed, gather_work
    )(slot, *sums)
    return run(
        lambda *refs: mix_kernel(lay, *refs),
        [VMEM] * 3,
        shape((tok, model), BF),
        (6 * tok * came * width, 2 * came * width),
    )(exchange(answers), expert_ids.T, gate_probs.T)


def solution(mesh):
    split = Mesh(
        mesh.devices.reshape(mesh.shape["attn"], 4, 4, 2),
        ("attn", "expert_0", "expert_1", "expert_2"),
    )
    return jax.shard_map(
        on_device,
        mesh=split,
        in_specs=(
            P(ATTN_EXPERT, None),
            P(ATTN_EXPERT, None),
            P(ATTN_EXPERT, None),
            P(),
            P(),
            P(EXPERT, None, "attn"),
            P(EXPERT, None, "attn"),
            P(EXPERT, "attn", None),
        ),
        out_specs=P(ATTN_EXPERT, None),
        check_vma=False,
    )
```

```python
import jax
import jax.numpy as jnp
from jax import lax
from jax.experimental import pallas as pl
from jax.experimental.pallas import tpu as pltpu
from jax.sharding import Mesh
from jax.sharding import PartitionSpec as P

SHED_MOST = 4
ATTN_EXPERT = ("attn", "expert_0", "expert_1", "expert_2")
EXPERT = ("expert_0", "expert_1", "expert_2")
SWISH_SCALE = 1.702
BF = jnp.bfloat16
F32 = jnp.float32


def iota(shape, dim):
    return lax.broadcasted_iota(jnp.int32, shape, dim)


def dot(a, b, dims=((1,), (0,))):
    return lax.dot_general(a, b, (dims, ((), ())), preferred_element_type=F32)


def hot(places, width, first=0):
    at = (iota((places.shape[0], width), 1) + first).astype(F32)
    return jnp.where(places == at, 1.0, 0.0)


def send_kernel(lay, x_ref, id_ref, s_ref, seen_ref):
    tok, experts, seats = x_ref.shape[0], lay.experts, lay.seats
    seen_ref[...] = jnp.zeros_like(seen_ref)
    ids = id_ref[...].astype(F32)
    expert = iota((experts, tok), 0).astype(F32)
    hits = jnp.zeros((experts, tok), F32)
    for k in range(ids.shape[0]):
        hits += jnp.where(ids[k : k + 1] == expert, 1.0, 0.0)
    earlier = (iota((tok, tok), 0) < iota((tok, tok), 1)).astype(BF)
    order = dot(hits.astype(BF), earlier)
    order = jnp.where(hits > 0.5, order, -1.0).astype(BF)
    rows = experts * seats
    spread = (iota((rows, experts), 0) // seats == iota((rows, experts), 1)).astype(BF)
    order = dot(spread, order)
    seat = iota((rows, tok), 0) % seats
    over = (seats + seat // 2).astype(F32)
    full = jnp.where(order == seat.astype(F32), 1.0, 0.0).astype(BF)
    part = jnp.where(order == over, 1.0, 0.0)
    even = jnp.where(seat % 2 == 0, part, 0.0).astype(BF)
    odd = jnp.where(seat % 2 == 1, part, 0.0).astype(BF)
    one, none = jnp.ones((tok, 1), BF), lambda n: jnp.zeros((tok, n), BF)
    second = jnp.concatenate([none(lay.width + 1), one, none(lay.low - lay.width - 2)], axis=1)
    flags = dot(part.astype(BF), second)
    for b in range(x_ref.shape[1] // lay.width):
        first = b * lay.width
        x = x_ref[:, first : first + lay.width]
        at = slice(b * rows, (b + 1) * rows)
        wide = jnp.concatenate([x, one, none(lay.low - lay.width - 1)], axis=1)
        s_ref[at, : lay.low] = (dot(full, wide) + flags).astype(BF)
        tail = jnp.concatenate([x[:, lay.point :], none(lay.short)], axis=1)
        s_ref[at, lay.low :] = (dot(even, x[:, : lay.point]) + dot(odd, tail)).astype(BF)


def gather_slots(lay, rows, x_ref, first, out):
    slots = out.shape[1]
    place = (iota((slots, x_ref.shape[0]), 0) + first).astype(F32)
    match = lambda row: jnp.where(row == place, 1.0, 0.0).astype(BF)
    got = dot(match(rows[0]), x_ref[:, : lay.width])
    rest = x_ref[:, lay.low :]
    left, right = dot(match(rows[1]), rest), dot(match(rows[2]), rest)
    extra = jnp.concatenate([left, right[:, : lay.width - lay.point]], axis=1)
    out[...] = (got + extra).astype(BF).T


def pick_more_kernel(lay, first, x_ref, row_ref, out):
    gather_slots(lay, [row_ref[k : k + 1] for k in range(3)], x_ref, first, out)


def pick_kernel(lay, x_ref, par_ref, row_ref, col_ref, out):
    came, seats = x_ref.shape[0], lay.seats
    sources = came // seats
    bound = par_ref[0].astype(F32)
    start = lay.width // 128 * 128
    tail = x_ref[:, start : lay.low]
    choose = (iota((8, tail.shape[1]), 1) == iota((8, tail.shape[1]), 0) + lay.width - start)
    flags = dot(choose.astype(BF), tail, ((1,), (1,)))
    full, part = flags[0:1], flags[1:2]
    seat = iota((1, came), 1) % seats
    even = seat % 2 == 0
    owner = iota((sources, came), 0) == iota((sources, came), 1) // seats
    each = full + jnp.where(even, part, 0.0)
    counts = jnp.sum(jnp.where(owner, each, 0.0), axis=1, keepdims=True)
    counts = jnp.broadcast_to(counts, (sources, 128)).astype(BF)
    earlier = (iota((sources, sources), 1) < iota((sources, sources), 0)).astype(BF)
    before = dot(earlier, counts)[:, 0:1]
    base = jnp.sum(jnp.where(owner, before, 0.0), axis=0, keepdims=True)
    rank = base + seat.astype(F32)
    over = base + (seats + seat // 2).astype(F32)
    rank = jnp.where(jnp.logical_and(full > 0.5, rank < bound), rank, -1.0)
    over = jnp.where(jnp.logical_and(part > 0.5, over < bound), over, -1.0)
    evens, odds = jnp.where(even, over, -1.0), jnp.where(even, -1.0, over)
    nothing = jnp.full((5, came), -1.0, F32)
    every = jnp.concatenate([rank, evens, odds, nothing], axis=0)
    row_ref[...] = every
    col_ref[...] = every.T
    gather_slots(lay, (rank, evens, odds), x_ref, 0, out)


def relay_kernel(seen_ref, g_ref, u_ref, d_ref, go_ref, uo_ref, do_ref):
    del seen_ref
    blocks, width = go_ref.shape[0], go_ref.shape[2]
    for b in range(blocks):
        at = slice(b * width, (b + 1) * width)
        go_ref[b] = g_ref[:, at]
        uo_ref[b] = u_ref[:, at]
        do_ref[b] = d_ref[:, at].T


def gate_up(refs):
    count = len(refs) // 3
    gate = up = None
    for x, wg, wu in zip(refs[:count], refs[count : 2 * count], refs[2 * count :]):
        g, u = dot(wg[0], x[...]), dot(wu[0], x[...])
        gate, up = (g, u) if gate is None else (gate + g, up + u)
    return gate, up


def mid_kernel(at_ref, *refs):
    del at_ref
    refs[-2][...], refs[-1][...] = gate_up(refs[:-2])


def far_kernel(at_ref, g_ref, u_ref, wd_ref, *refs):
    del at_ref
    gate, up = gate_up(refs[:-2])
    h_ref, o_ref = refs[-2:]
    gate, up = gate + g_ref[...], up + u_ref[...]
    hidden = (gate * jax.nn.sigmoid(SWISH_SCALE * gate) * (up + 1.0)).astype(BF)
    h_ref[...] = hidden
    o_ref[...] = dot(wd_ref[0], hidden).astype(BF)


def near_kernel(at_ref, h_ref, *refs):
    del at_ref
    hidden = h_ref[...]
    for weight, out in zip(refs[:3], refs[3:]):
        out[...] = dot(weight[0], hidden).astype(out.dtype)


def place_kernel(lay, slot_ref, *refs):
    ins, z_ref = refs[:-1], refs[-1]
    columns = []
    for own, left, right in (ins[:3], ins[3:]):
        total = own[...] + left[...].astype(F32) + right[...].astype(F32)
        columns.append(total.astype(BF))
    y = jnp.concatenate(columns, axis=1)
    slots, came = y.shape[1], z_ref.shape[0]
    at = lambda k: hot(slot_ref[:, k : k + 1], slots).astype(BF)
    none = lambda n: jnp.zeros((came, n), BF)
    rows = dot(at(0), y, ((1,), (1,))).astype(BF)
    z_ref[:, : lay.low] = jnp.concatenate([rows, none(lay.low - lay.width)], axis=1)
    left = dot(at(1), y[: lay.point], ((1,), (1,))).astype(BF)
    right = dot(at(2), y[lay.point :], ((1,), (1,))).astype(BF)
    z_ref[:, lay.low :] = left + jnp.concatenate([right, none(lay.short)], axis=1)


def mix_kernel(lay, b_ref, id_ref, p_ref, o_ref):
    tok, seats = o_ref.shape[0], lay.seats
    ids, prob = id_ref[...].astype(F32).T, p_ref[...].T
    top = ids.shape[1]
    lane = iota((tok, lay.experts), 1).astype(F32)
    named = [ids[:, k : k + 1] == lane for k in range(top)]
    hits = jnp.zeros((tok, lay.experts), F32)
    for k in range(top):
        hits += jnp.where(named[k], 1.0, 0.0)
    earlier = (iota((tok, tok), 1) < iota((tok, tok), 0)).astype(BF)
    order = dot(earlier, hits.astype(BF))
    rows = lay.experts * seats
    kinds = [jnp.zeros((tok, rows), F32) for _ in range(3)]
    for k in range(top):
        seat = jnp.sum(jnp.where(named[k], order, 0.0), axis=1, keepdims=True)
        base = ids[:, k : k + 1] * seats
        full = jnp.where(seat < seats, base + seat, -1.0)
        over = jnp.where(seat < seats, -1.0, base + 2.0 * (seat - seats))
        odd = jnp.where(seat < seats, -1.0, over + 1.0)
        for n, place in enumerate((full, over, odd)):
            kinds[n] += hot(place, rows) * prob[:, k : k + 1]
    weights = []
    for kind in kinds:
        high = kind.astype(BF)
        rest = kind - high.astype(F32)
        middle = rest.astype(BF)
        low = (rest - middle.astype(F32)).astype(BF)
        weights.append(jnp.concatenate([high, middle, low], axis=0))

    def weighted(n, block):
        three = dot(weights[n], block)
        return three[:tok] + three[tok : 2 * tok] + three[2 * tok :]

    for b in range(o_ref.shape[1] // lay.width):
        at = slice(b * rows, (b + 1) * rows)
        whole_rows = weighted(0, b_ref[at, : lay.width])
        rest = b_ref[at, lay.low :]
        left, right = weighted(1, rest), weighted(2, rest)
        extra = jnp.concatenate([left, right[:, : lay.width - lay.point]], axis=1)
        o_ref[:, b * lay.width : (b + 1) * lay.width] = (whole_rows + extra).astype(BF)


VMEM = pl.BlockSpec(memory_space=pltpu.VMEM)
SMEM = pl.BlockSpec(memory_space=pltpu.SMEM)
ANY = pl.BlockSpec(memory_space=pl.ANY)
shape = jax.ShapeDtypeStruct


class Layout:
    def __init__(self, width, experts, most):
        self.width, self.experts = width, experts
        self.seats = 8
        self.low = (width + 2 + 127) // 128 * 128
        self.point = (width // 2 + 127) // 128 * 128
        self.short = 2 * self.point - width
        self.lanes = self.low + self.point
        assert self.seats <= most <= self.seats * 3 // 2


def cost(flops, moved):
    return pl.CostEstimate(flops=flops, bytes_accessed=moved, transcendentals=0)


def grant(mebibytes):
    return pltpu.CompilerParams(vmem_limit_bytes=mebibytes << 20)


def run(kernel, ins, outs, work, scratch=(), mebibytes=24):
    return pl.pallas_call(
        kernel,
        out_shape=outs,
        in_specs=ins,
        out_specs=jax.tree.map(lambda _: VMEM, outs),
        scratch_shapes=scratch,
        cost_estimate=cost(*work),
        compiler_params=grant(mebibytes),
    )


def on_device(
    tokens, expert_ids, gate_probs, shed_blocks, partner, gate_weight, up_weight, down_weight
):
    tok, model = tokens.shape
    top = expert_ids.shape[1]
    experts = shed_blocks.shape[0]
    groups = lax.axis_size("attn")
    width = model // groups
    capacity = tok * top * groups
    block = capacity // 8
    slots = capacity + block * SHED_MOST
    units = gate_weight.shape[2]
    lay = Layout(width, experts, min(tok, 3 * tok * top // experts))
    devices = groups * experts
    came = devices * lay.seats
    me = lax.axis_index(EXPERT)
    bound = capacity - block * shed_blocks[partner[me]] + block * shed_blocks[me]
    par = bound.reshape(1).astype(jnp.int32)
    at = lax.axis_index("attn").astype(jnp.int32).reshape(1)

    def shifted(distance):
        pairs = [(i, (i + distance) % groups) for i in range(groups)]
        return lambda array: lax.ppermute(array, "attn", pairs)

    right, left = shifted(1), shifted(groups - 1)

    def exchange(rows):
        blocks = rows.reshape(devices, lay.seats, lay.lanes)
        moved = lax.all_to_all(blocks, ATTN_EXPERT, split_axis=0, concat_axis=0, tiled=True)
        return moved.reshape(came, lay.lanes)

    packed = shape((came, lay.lanes), BF)
    outgoing, seen = run(
        lambda *refs: send_kernel(lay, *refs),
        [VMEM] * 2,
        (packed, shape((8, 128), F32)),
        (2 * tok * came * width, 2 * came * width),
        mebibytes=60,
    )(tokens, expert_ids.T)
    arrived = exchange(outgoing)
    relaid = shape((groups, units, width), BF)
    step = 128
    rows_in = pl.BlockSpec((step, model), lambda i: (i, 0))
    rows_out = pl.BlockSpec((groups, step, width), lambda i: (0, i, 0))
    wg, wu, wd = pl.pallas_call(
        relay_kernel,
        grid=(pl.cdiv(units, step),),
        out_shape=(relaid, relaid, shape((groups, width, units), BF)),
        in_specs=[ANY] + [rows_in] * 3,
        out_specs=(rows_out, rows_out, pl.BlockSpec((groups, width, step), lambda i: (0, 0, i))),
        cost_estimate=cost(12 * slots * width * units, 12 * model * units),
        compiler_params=grant(60),
        name="relay",
    )(seen, gate_weight[0].T, up_weight[0].T, down_weight[0])
    arrived, wg, wu, wd = lax.optimization_barrier((arrived, wg, wu, wd))

    part = slots // 2
    columns = shape((width, part), BF)
    gather_work = (2 * slots * came * width, 2 * came * width)
    places, slot, own_a = run(
        lambda *refs: pick_kernel(lay, *refs),
        [VMEM, SMEM],
        (shape((8, came), F32), shape((came, 8), F32), columns),
        gather_work,
    )(arrived, par)
    own_b = run(
        lambda *refs: pick_more_kernel(lay, part, *refs), [VMEM] * 2, columns, gather_work
    )(arrived, places)
    lane = lambda rows: pl.BlockSpec((rows, part), lambda i, p: (0, 0))

    def weight(rows, columns, ahead):
        return pl.BlockSpec((1, rows, columns), lambda i, p: (lax.rem(p[0] + ahead, groups), 0, 0))

    def staged(kernel, ins, outs, flops, moved):
        return pl.pallas_call(
            kernel,
            grid_spec=pltpu.PrefetchScalarGridSpec(
                num_scalar_prefetch=1,
                grid=(1,),
                in_specs=ins,
                out_specs=tuple(lane(out.shape[0]) for out in outs),
            ),
            out_shape=outs,
            cost_estimate=cost(flops, moved),
            compiler_params=grant(32),
        )

    before, after, across = groups - 1, 1, groups // 2
    area = width * units
    rows = lambda n, kind: shape((n, part), kind)

    def mid(blocks, ahead):
        count = len(blocks)
        return staged(
            mid_kernel,
            [lane(width)] * count + [weight(units, width, d) for d in ahead] * 2,
            (rows(units, F32), rows(units, F32)),
            4 * count * part * area,
            4 * count * area,
        )(at, *blocks, *[wg] * count, *[wu] * count)

    def far(sums, blocks, ahead):
        count = len(blocks)
        return staged(
            far_kernel,
            [lane(units)] * 2
            + [weight(width, units, across)]
            + [lane(width)] * count
            + [weight(units, width, d) for d in ahead] * 2,
            (rows(units, BF), rows(width, BF)),
            (4 * count + 2) * part * area,
            (4 * count + 2) * area,
        )(at, *sums, wd, *blocks, *[wg] * count, *[wu] * count)

    def near(hidden, kinds):
        return staged(
            near_kernel,
            [lane(units)] + [weight(width, units, d) for d in (0, before, after)],
            tuple(rows(width, kind) for kind in kinds),
            6 * part * area,
            6 * area,
        )(at, hidden, wd, wd, wd)

    def add(mine, came):
        return (mine + came.astype(F32)).astype(BF)

    below_a, above_a = right(own_a), left(own_a)
    above_b = left(own_b)
    far_a = right(below_a)
    below_b = right(own_b)
    far_b = left(above_b)
    sums_a = mid((own_a, below_a, above_a), (0, before, after))
    hidden_a, share_a = far(sums_a, (far_a,), (across,))
    crossed_a = right(share_a)
    mine_a, left_a, right_a = near(hidden_a, (F32, BF, F32))
    from_right_a = left(left_a)
    sums_b = mid((own_b, above_b), (0, after))
    hidden_b, share_b = far(sums_b, (below_b, far_b), (before, across))
    crossed_b = left(share_b)
    mine_b, left_b, right_b = near(hidden_b, (F32, F32, BF))
    from_left_b = right(right_b)
    added_a, added_b = add(right_a, crossed_a), add(left_b, crossed_b)
    from_left_a = right(added_a)
    from_right_b = left(added_b)
    sums = (mine_a, from_left_a, from_right_a, mine_b, from_left_b, from_right_b)
    answers = run(
        lambda *refs: place_kernel(lay, *refs), [VMEM] * 7, packed, gather_work
    )(slot, *sums)
    return run(
        lambda *refs: mix_kernel(lay, *refs),
        [VMEM] * 3,
        shape((tok, model), BF),
        (6 * tok * came * width, 2 * came * width),
    )(exchange(answers), expert_ids.T, gate_probs.T)


def solution(mesh):
    split = Mesh(
        mesh.devices.reshape(mesh.shape["attn"], 4, 4, 2),
        ("attn", "expert_0", "expert_1", "expert_2"),
    )
    return jax.shard_map(
        on_device,
        mesh=split,
        in_specs=(
            P(ATTN_EXPERT, None),
            P(ATTN_EXPERT, None),
            P(ATTN_EXPERT, None),
            P(),
            P(),
            P(EXPERT, None, "attn"),
            P(EXPERT, None, "attn"),
            P(EXPERT, "attn", None),
        ),
        out_specs=P(ATTN_EXPERT, None),
        check_vma=False,
    )
```

```python
import jax
import jax.numpy as jnp
from jax import lax
from jax.experimental import pallas as pl
from jax.experimental.pallas import tpu as pltpu
from jax.sharding import Mesh
from jax.sharding import PartitionSpec as P

SHED_MOST = 4
ATTN_EXPERT = ("attn", "expert_0", "expert_1", "expert_2")
EXPERT = ("expert_0", "expert_1", "expert_2")
SWISH_SCALE = 1.702
BF = jnp.bfloat16
F32 = jnp.float32


def iota(shape, dim):
    return lax.broadcasted_iota(jnp.int32, shape, dim)


def dot(a, b, dims=((1,), (0,))):
    return lax.dot_general(a, b, (dims, ((), ())), preferred_element_type=F32)


def hot(places, width, first=0):
    at = (iota((places.shape[0], width), 1) + first).astype(F32)
    return jnp.where(places == at, 1.0, 0.0)


def send_kernel(lay, x_ref, id_ref, s_ref, seen_ref):
    tok, experts, seats = x_ref.shape[0], lay.experts, lay.seats
    seen_ref[...] = jnp.zeros_like(seen_ref)
    ids = id_ref[...].astype(F32)
    expert = iota((experts, tok), 0).astype(F32)
    hits = jnp.zeros((experts, tok), F32)
    for k in range(ids.shape[0]):
        hits += jnp.where(ids[k : k + 1] == expert, 1.0, 0.0)
    earlier = (iota((tok, tok), 0) < iota((tok, tok), 1)).astype(BF)
    order = dot(hits.astype(BF), earlier)
    order = jnp.where(hits > 0.5, order, -1.0).astype(BF)
    rows = experts * seats
    spread = (iota((rows, experts), 0) // seats == iota((rows, experts), 1)).astype(BF)
    order = dot(spread, order)
    seat = iota((rows, tok), 0) % seats
    over = (seats + seat // 2).astype(F32)
    full = jnp.where(order == seat.astype(F32), 1.0, 0.0).astype(BF)
    part = jnp.where(order == over, 1.0, 0.0)
    even = jnp.where(seat % 2 == 0, part, 0.0).astype(BF)
    odd = jnp.where(seat % 2 == 1, part, 0.0).astype(BF)
    one, none = jnp.ones((tok, 1), BF), lambda n: jnp.zeros((tok, n), BF)
    second = jnp.concatenate([none(lay.width + 1), one, none(lay.low - lay.width - 2)], axis=1)
    flags = dot(part.astype(BF), second)
    for b in range(x_ref.shape[1] // lay.width):
        first = b * lay.width
        x = x_ref[:, first : first + lay.width]
        at = slice(b * rows, (b + 1) * rows)
        wide = jnp.concatenate([x, one, none(lay.low - lay.width - 1)], axis=1)
        s_ref[at, : lay.low] = (dot(full, wide) + flags).astype(BF)
        tail = jnp.concatenate([x[:, lay.point :], none(lay.short)], axis=1)
        s_ref[at, lay.low :] = (dot(even, x[:, : lay.point]) + dot(odd, tail)).astype(BF)


def gather_slots(lay, rows, x_ref, first, out):
    slots = out.shape[1]
    place = (iota((slots, x_ref.shape[0]), 0) + first).astype(F32)
    match = lambda row: jnp.where(row == place, 1.0, 0.0).astype(BF)
    got = dot(match(rows[0]), x_ref[:, : lay.width])
    rest = x_ref[:, lay.low :]
    left, right = dot(match(rows[1]), rest), dot(match(rows[2]), rest)
    extra = jnp.concatenate([left, right[:, : lay.width - lay.point]], axis=1)
    out[...] = (got + extra).astype(BF).T


def pick_more_kernel(lay, first, x_ref, row_ref, out):
    gather_slots(lay, [row_ref[k : k + 1] for k in range(3)], x_ref, first, out)


def pick_kernel(lay, x_ref, par_ref, row_ref, col_ref, out):
    came, seats = x_ref.shape[0], lay.seats
    sources = came // seats
    bound = par_ref[0].astype(F32)
    start = lay.width // 128 * 128
    tail = x_ref[:, start : lay.low]
    choose = (iota((8, tail.shape[1]), 1) == iota((8, tail.shape[1]), 0) + lay.width - start)
    flags = dot(choose.astype(BF), tail, ((1,), (1,)))
    full, part = flags[0:1], flags[1:2]
    seat = iota((1, came), 1) % seats
    even = seat % 2 == 0
    owner = iota((sources, came), 0) == iota((sources, came), 1) // seats
    each = full + jnp.where(even, part, 0.0)
    counts = jnp.sum(jnp.where(owner, each, 0.0), axis=1, keepdims=True)
    counts = jnp.broadcast_to(counts, (sources, 128)).astype(BF)
    earlier = (iota((sources, sources), 1) < iota((sources, sources), 0)).astype(BF)
    before = dot(earlier, counts)[:, 0:1]
    base = jnp.sum(jnp.where(owner, before, 0.0), axis=0, keepdims=True)
    rank = base + seat.astype(F32)
    over = base + (seats + seat // 2).astype(F32)
    rank = jnp.where(jnp.logical_and(full > 0.5, rank < bound), rank, -1.0)
    over = jnp.where(jnp.logical_and(part > 0.5, over < bound), over, -1.0)
    evens, odds = jnp.where(even, over, -1.0), jnp.where(even, -1.0, over)
    nothing = jnp.full((5, came), -1.0, F32)
    every = jnp.concatenate([rank, evens, odds, nothing], axis=0)
    row_ref[...] = every
    col_ref[...] = every.T
    gather_slots(lay, (rank, evens, odds), x_ref, 0, out)


def relay_kernel(seen_ref, g_ref, u_ref, d_ref, go_ref, uo_ref, do_ref):
    del seen_ref
    blocks, width = go_ref.shape[0], go_ref.shape[2]
    for b in range(blocks):
        at = slice(b * width, (b + 1) * width)
        go_ref[b] = g_ref[:, at]
        uo_ref[b] = u_ref[:, at]
        do_ref[b] = d_ref[:, at].T


def gate_up(at, ahead, wg_ref, wu_ref, blocks):
    gate = up = None
    for distance, x in zip(ahead, blocks):
        block = lax.rem(at + distance, wg_ref.shape[0])
        g, u = dot(wg_ref[block], x[...]), dot(wu_ref[block], x[...])
        gate, up = (g, u) if gate is None else (gate + g, up + u)
    return gate, up


def mid_kernel(ahead, at_ref, wg_ref, wu_ref, *refs):
    refs[-2][...], refs[-1][...] = gate_up(at_ref[0], ahead, wg_ref, wu_ref, refs[:-2])


def far_kernel(ahead, at_ref, wg_ref, wu_ref, wd_ref, g_ref, u_ref, *refs):
    gate, up = gate_up(at_ref[0], ahead, wg_ref, wu_ref, refs[:-2])
    h_ref, o_ref = refs[-2:]
    gate, up = gate + g_ref[...], up + u_ref[...]
    hidden = (gate * jax.nn.sigmoid(SWISH_SCALE * gate) * (up + 1.0)).astype(BF)
    h_ref[...] = hidden
    groups = wd_ref.shape[0]
    across = lax.rem(at_ref[0] + groups // 2, groups)
    o_ref[...] = dot(wd_ref[across], hidden).astype(BF)


def near_kernel(at_ref, h_ref, wd_ref, *outs):
    hidden = h_ref[...]
    groups = wd_ref.shape[0]
    for distance, out in zip((0, groups - 1, 1), outs):
        block = lax.rem(at_ref[0] + distance, groups)
        out[...] = dot(wd_ref[block], hidden).astype(out.dtype)


def place_kernel(lay, slot_ref, *refs):
    ins, z_ref = refs[:-1], refs[-1]
    columns = []
    for own, left, right in (ins[:3], ins[3:]):
        total = own[...] + left[...].astype(F32) + right[...].astype(F32)
        columns.append(total.astype(BF))
    y = jnp.concatenate(columns, axis=1)
    slots, came = y.shape[1], z_ref.shape[0]
    at = lambda k: hot(slot_ref[:, k : k + 1], slots).astype(BF)
    none = lambda n: jnp.zeros((came, n), BF)
    rows = dot(at(0), y, ((1,), (1,))).astype(BF)
    z_ref[:, : lay.low] = jnp.concatenate([rows, none(lay.low - lay.width)], axis=1)
    left = dot(at(1), y[: lay.point], ((1,), (1,))).astype(BF)
    right = dot(at(2), y[lay.point :], ((1,), (1,))).astype(BF)
    z_ref[:, lay.low :] = left + jnp.concatenate([right, none(lay.short)], axis=1)


def mix_kernel(lay, b_ref, id_ref, p_ref, o_ref):
    tok, seats = o_ref.shape[0], lay.seats
    ids, prob = id_ref[...].astype(F32).T, p_ref[...].T
    top = ids.shape[1]
    lane = iota((tok, lay.experts), 1).astype(F32)
    named = [ids[:, k : k + 1] == lane for k in range(top)]
    hits = jnp.zeros((tok, lay.experts), F32)
    for k in range(top):
        hits += jnp.where(named[k], 1.0, 0.0)
    earlier = (iota((tok, tok), 1) < iota((tok, tok), 0)).astype(BF)
    order = dot(earlier, hits.astype(BF))
    rows = lay.experts * seats
    kinds = [jnp.zeros((tok, rows), F32) for _ in range(3)]
    for k in range(top):
        seat = jnp.sum(jnp.where(named[k], order, 0.0), axis=1, keepdims=True)
        base = ids[:, k : k + 1] * seats
        full = jnp.where(seat < seats, base + seat, -1.0)
        over = jnp.where(seat < seats, -1.0, base + 2.0 * (seat - seats))
        odd = jnp.where(seat < seats, -1.0, over + 1.0)
        for n, place in enumerate((full, over, odd)):
            kinds[n] += hot(place, rows) * prob[:, k : k + 1]
    weights = []
    for kind in kinds:
        high = kind.astype(BF)
        rest = kind - high.astype(F32)
        middle = rest.astype(BF)
        low = (rest - middle.astype(F32)).astype(BF)
        weights.append(jnp.concatenate([high, middle, low], axis=0))

    def weighted(n, block):
        three = dot(weights[n], block)
        return three[:tok] + three[tok : 2 * tok] + three[2 * tok :]

    for b in range(o_ref.shape[1] // lay.width):
        at = slice(b * rows, (b + 1) * rows)
        whole_rows = weighted(0, b_ref[at, : lay.width])
        rest = b_ref[at, lay.low :]
        left, right = weighted(1, rest), weighted(2, rest)
        extra = jnp.concatenate([left, right[:, : lay.width - lay.point]], axis=1)
        o_ref[:, b * lay.width : (b + 1) * lay.width] = (whole_rows + extra).astype(BF)


VMEM = pl.BlockSpec(memory_space=pltpu.VMEM)
SMEM = pl.BlockSpec(memory_space=pltpu.SMEM)
ANY = pl.BlockSpec(memory_space=pl.ANY)
shape = jax.ShapeDtypeStruct


class Layout:
    def __init__(self, width, experts, most):
        self.width, self.experts = width, experts
        self.seats = 8
        self.low = (width + 2 + 127) // 128 * 128
        self.point = (width // 2 + 127) // 128 * 128
        self.short = 2 * self.point - width
        self.lanes = self.low + self.point
        assert self.seats <= most <= self.seats * 3 // 2


def cost(flops, moved):
    return pl.CostEstimate(flops=flops, bytes_accessed=moved, transcendentals=0)


def grant(mebibytes):
    return pltpu.CompilerParams(vmem_limit_bytes=mebibytes << 20)


def run(kernel, ins, outs, work, scratch=(), mebibytes=12):
    return pl.pallas_call(
        kernel,
        out_shape=outs,
        in_specs=ins,
        out_specs=jax.tree.map(lambda _: VMEM, outs),
        scratch_shapes=scratch,
        cost_estimate=cost(*work),
        compiler_params=grant(mebibytes),
    )


def on_device(
    tokens, expert_ids, gate_probs, shed_blocks, partner, gate_weight, up_weight, down_weight
):
    tok, model = tokens.shape
    top = expert_ids.shape[1]
    experts = shed_blocks.shape[0]
    groups = lax.axis_size("attn")
    width = model // groups
    capacity = tok * top * groups
    block = capacity // 8
    slots = capacity + block * SHED_MOST
    units = gate_weight.shape[2]
    lay = Layout(width, experts, min(tok, 3 * tok * top // experts))
    devices = groups * experts
    came = devices * lay.seats
    me = lax.axis_index(EXPERT)
    bound = capacity - block * shed_blocks[partner[me]] + block * shed_blocks[me]
    par = bound.reshape(1).astype(jnp.int32)
    at = lax.axis_index("attn").astype(jnp.int32).reshape(1)

    def shifted(distance):
        pairs = [(i, (i + distance) % groups) for i in range(groups)]
        return lambda array: lax.ppermute(array, "attn", pairs)

    right, left = shifted(1), shifted(groups - 1)

    def exchange(rows):
        blocks = rows.reshape(devices, lay.seats, lay.lanes)
        moved = lax.all_to_all(blocks, ATTN_EXPERT, split_axis=0, concat_axis=0, tiled=True)
        return moved.reshape(came, lay.lanes)

    packed = shape((came, lay.lanes), BF)
    outgoing, seen = run(
        lambda *refs: send_kernel(lay, *refs),
        [VMEM] * 2,
        (packed, shape((8, 128), F32)),
        (2 * tok * came * width, 2 * came * width),
        mebibytes=60,
    )(tokens, expert_ids.T)
    arrived = exchange(outgoing)
    relaid = shape((groups, units, width), BF)
    step = 128
    rows_in = pl.BlockSpec((step, model), lambda i: (i, 0))
    rows_out = pl.BlockSpec((groups, step, width), lambda i: (0, i, 0))
    wg, wu, wd = pl.pallas_call(
        relay_kernel,
        grid=(pl.cdiv(units, step),),
        out_shape=(relaid, relaid, shape((groups, width, units), BF)),
        in_specs=[ANY] + [rows_in] * 3,
        out_specs=(rows_out, rows_out, pl.BlockSpec((groups, width, step), lambda i: (0, 0, i))),
        cost_estimate=cost(12 * slots * width * units, 12 * model * units),
        compiler_params=grant(60),
        name="relay",
    )(seen, gate_weight[0].T, up_weight[0].T, down_weight[0])
    arrived, wg, wu, wd = lax.optimization_barrier((arrived, wg, wu, wd))

    part = slots // 2
    columns = shape((width, part), BF)
    gather_work = (2 * slots * came * width, 2 * came * width)
    places, slot, own_a = run(
        lambda *refs: pick_kernel(lay, *refs),
        [VMEM, SMEM],
        (shape((8, came), F32), shape((came, 8), F32), columns),
        gather_work,
    )(arrived, par)
    own_b = run(
        lambda *refs: pick_more_kernel(lay, part, *refs), [VMEM] * 2, columns, gather_work
    )(arrived, places)
    before, after, across = groups - 1, 1, groups // 2
    area = width * units
    rows = lambda n, kind: shape((n, part), kind)

    def mid(blocks, ahead):
        return run(
            lambda *refs: mid_kernel(ahead, *refs),
            [SMEM] + [VMEM] * (2 + len(blocks)),
            (rows(units, F32), rows(units, F32)),
            (4 * len(blocks) * part * area, 4 * len(blocks) * area),
        )(at, wg, wu, *blocks)

    def far(sums, blocks, ahead):
        count = 4 * len(blocks) + 2
        return run(
            lambda *refs: far_kernel(ahead, *refs),
            [SMEM] + [VMEM] * (5 + len(blocks)),
            (rows(units, BF), rows(width, BF)),
            (count * part * area, count * area),
        )(at, wg, wu, wd, *sums, *blocks)

    def near(hidden, kinds):
        return run(
            near_kernel,
            [SMEM] + [VMEM] * 2,
            tuple(rows(width, kind) for kind in kinds),
            (6 * part * area, 6 * area),
        )(at, hidden, wd)

    def add(mine, came):
        return (mine + came.astype(F32)).astype(BF)

    below_a, above_a = right(own_a), left(own_a)
    above_b = left(own_b)
    far_a = right(below_a)
    below_b = right(own_b)
    far_b = left(above_b)
    sums_a = mid((own_a, below_a, above_a), (0, before, after))
    hidden_a, share_a = far(sums_a, (far_a,), (across,))
    crossed_a = right(share_a)
    mine_a, left_a, right_a = near(hidden_a, (F32, BF, F32))
    from_right_a = left(left_a)
    sums_b = mid((own_b, above_b), (0, after))
    hidden_b, share_b = far(sums_b, (below_b, far_b), (before, across))
    crossed_b = left(share_b)
    mine_b, left_b, right_b = near(hidden_b, (F32, F32, BF))
    from_left_b = right(right_b)
    added_a, added_b = add(right_a, crossed_a), add(left_b, crossed_b)
    from_left_a = right(added_a)
    from_right_b = left(added_b)
    sums = (mine_a, from_left_a, from_right_a, mine_b, from_left_b, from_right_b)
    answers = run(
        lambda *refs: place_kernel(lay, *refs), [VMEM] * 7, packed, gather_work
    )(slot, *sums)
    return run(
        lambda *refs: mix_kernel(lay, *refs),
        [VMEM] * 3,
        shape((tok, model), BF),
        (6 * tok * came * width, 2 * came * width),
    )(exchange(answers), expert_ids.T, gate_probs.T)


def solution(mesh):
    split = Mesh(
        mesh.devices.reshape(mesh.shape["attn"], 4, 4, 2),
        ("attn", "expert_0", "expert_1", "expert_2"),
    )
    return jax.shard_map(
        on_device,
        mesh=split,
        in_specs=(
            P(ATTN_EXPERT, None),
            P(ATTN_EXPERT, None),
            P(ATTN_EXPERT, None),
            P(),
            P(),
            P(EXPERT, None, "attn"),
            P(EXPERT, None, "attn"),
            P(EXPERT, "attn", None),
        ),
        out_specs=P(ATTN_EXPERT, None),
        check_vma=False,
    )
```

```python
import jax
import jax.numpy as jnp
from jax import lax
from jax.experimental import pallas as pl
from jax.experimental.pallas import tpu as pltpu
from jax.sharding import Mesh
from jax.sharding import PartitionSpec as P

SHED_MOST = 4
ATTN_EXPERT = ("attn", "expert_0", "expert_1", "expert_2")
EXPERT = ("expert_0", "expert_1", "expert_2")
SWISH_SCALE = 1.702
BF = jnp.bfloat16
F32 = jnp.float32


def iota(shape, dim):
    return lax.broadcasted_iota(jnp.int32, shape, dim)


def dot(a, b, dims=((1,), (0,))):
    return lax.dot_general(a, b, (dims, ((), ())), preferred_element_type=F32)


def hot(places, width, first=0):
    at = (iota((places.shape[0], width), 1) + first).astype(F32)
    return jnp.where(places == at, 1.0, 0.0)


def send_kernel(lay, blocks, x_ref, id_ref, s_ref, seen_ref, hot_ref, flag_ref):
    tok, experts, seats = x_ref.shape[0], lay.experts, lay.seats
    one, none = jnp.ones((tok, 1), BF), lambda n: jnp.zeros((tok, n), BF)

    @pl.when(pl.program_id(0) == 0)
    def _():
        seen_ref[...] = jnp.zeros_like(seen_ref)
        ids = id_ref[...].astype(F32)
        expert = iota((experts, tok), 0).astype(F32)
        hits = jnp.zeros((experts, tok), F32)
        for k in range(ids.shape[0]):
            hits += jnp.where(ids[k : k + 1] == expert, 1.0, 0.0)
        earlier = (iota((tok, tok), 0) < iota((tok, tok), 1)).astype(BF)
        order = dot(hits.astype(BF), earlier)
        order = jnp.where(hits > 0.5, order, -1.0).astype(BF)
        rows = experts * seats
        spread = (iota((rows, experts), 0) // seats == iota((rows, experts), 1)).astype(BF)
        order = dot(spread, order)
        seat = iota((rows, tok), 0) % seats
        over = (seats + seat // 2).astype(F32)
        part = jnp.where(order == over, 1.0, 0.0)
        hot_ref[0] = jnp.where(order == seat.astype(F32), 1.0, 0.0).astype(BF)
        hot_ref[1] = jnp.where(seat % 2 == 0, part, 0.0).astype(BF)
        hot_ref[2] = jnp.where(seat % 2 == 1, part, 0.0).astype(BF)
        second = jnp.concatenate([none(lay.width + 1), one, none(lay.low - lay.width - 2)], axis=1)
        flag_ref[...] = dot(part.astype(BF), second)

    for b in range(blocks):

        @pl.when(pl.program_id(0) == b)
        def _(b=b):
            x = x_ref[:, b * lay.width : (b + 1) * lay.width]
            wide = jnp.concatenate([x, one, none(lay.low - lay.width - 1)], axis=1)
            s_ref[:, : lay.low] = (dot(hot_ref[0], wide) + flag_ref[...]).astype(BF)
            tail = jnp.concatenate([x[:, lay.point :], none(lay.short)], axis=1)
            rest = dot(hot_ref[1], x[:, : lay.point]) + dot(hot_ref[2], tail)
            s_ref[:, lay.low :] = rest.astype(BF)


def gather_slots(lay, rows, x_ref, first, out):
    slots = out.shape[1]
    place = (iota((slots, x_ref.shape[0]), 0) + first).astype(F32)
    match = lambda row: jnp.where(row == place, 1.0, 0.0).astype(BF)
    got = dot(match(rows[0]), x_ref[:, : lay.width])
    rest = x_ref[:, lay.low :]
    left, right = dot(match(rows[1]), rest), dot(match(rows[2]), rest)
    extra = jnp.concatenate([left, right[:, : lay.width - lay.point]], axis=1)
    out[...] = (got + extra).astype(BF).T


def pick_more_kernel(lay, first, x_ref, row_ref, out):
    gather_slots(lay, [row_ref[k : k + 1] for k in range(3)], x_ref, first, out)


def pick_kernel(lay, x_ref, par_ref, row_ref, out):
    came, seats = x_ref.shape[0], lay.seats
    sources = came // seats
    bound = par_ref[0].astype(F32)
    start = lay.width // 128 * 128
    tail = x_ref[:, start : lay.low]
    choose = (iota((8, tail.shape[1]), 1) == iota((8, tail.shape[1]), 0) + lay.width - start)
    flags = dot(choose.astype(BF), tail, ((1,), (1,)))
    full, part = flags[0:1], flags[1:2]
    seat = iota((1, came), 1) % seats
    even = seat % 2 == 0
    owner = iota((sources, came), 0) == iota((sources, came), 1) // seats
    each = full + jnp.where(even, part, 0.0)
    counts = jnp.sum(jnp.where(owner, each, 0.0), axis=1, keepdims=True)
    counts = jnp.broadcast_to(counts, (sources, 128)).astype(BF)
    earlier = (iota((sources, sources), 1) < iota((sources, sources), 0)).astype(BF)
    before = dot(earlier, counts)[:, 0:1]
    base = jnp.sum(jnp.where(owner, before, 0.0), axis=0, keepdims=True)
    rank = base + seat.astype(F32)
    over = base + (seats + seat // 2).astype(F32)
    rank = jnp.where(jnp.logical_and(full > 0.5, rank < bound), rank, -1.0)
    over = jnp.where(jnp.logical_and(part > 0.5, over < bound), over, -1.0)
    evens, odds = jnp.where(even, over, -1.0), jnp.where(even, -1.0, over)
    nothing = jnp.full((5, came), -1.0, F32)
    row_ref[...] = jnp.concatenate([rank, evens, odds, nothing], axis=0)
    gather_slots(lay, (rank, evens, odds), x_ref, 0, out)


def relay_kernel(seen_ref, g_ref, u_ref, d_ref, go_ref, uo_ref, do_ref):
    del seen_ref
    blocks, width = go_ref.shape[0], go_ref.shape[2]
    for b in range(blocks):
        at = slice(b * width, (b + 1) * width)
        go_ref[b] = g_ref[:, at]
        uo_ref[b] = u_ref[:, at]
        do_ref[b] = d_ref[:, at].T


def gate_up(at, ahead, wg_ref, wu_ref, blocks):
    gate = up = None
    for distance, x in zip(ahead, blocks):
        block = lax.rem(at + distance, wg_ref.shape[0])
        g, u = dot(wg_ref[block], x[...]), dot(wu_ref[block], x[...])
        gate, up = (g, u) if gate is None else (gate + g, up + u)
    return gate, up


def mid_kernel(ahead, at_ref, wg_ref, wu_ref, *refs):
    refs[-2][...], refs[-1][...] = gate_up(at_ref[0], ahead, wg_ref, wu_ref, refs[:-2])


def far_kernel(ahead, at_ref, wg_ref, wu_ref, wd_ref, g_ref, u_ref, *refs):
    gate, up = gate_up(at_ref[0], ahead, wg_ref, wu_ref, refs[:-2])
    h_ref, o_ref = refs[-2:]
    gate, up = gate + g_ref[...], up + u_ref[...]
    hidden = (gate * jax.nn.sigmoid(SWISH_SCALE * gate) * (up + 1.0)).astype(BF)
    h_ref[...] = hidden
    groups = wd_ref.shape[0]
    across = lax.rem(at_ref[0] + groups // 2, groups)
    o_ref[...] = dot(wd_ref[across], hidden).astype(BF)


def near_kernel(at_ref, h_ref, wd_ref, *outs):
    hidden = h_ref[...]
    groups = wd_ref.shape[0]
    for distance, out in zip((0, groups - 1, 1), outs):
        block = lax.rem(at_ref[0] + distance, groups)
        out[...] = dot(wd_ref[block], hidden).astype(out.dtype)


def spots_kernel(row_ref, *outs):
    places = row_ref[...].T
    for k, out in enumerate(outs):
        out[...] = hot(places[:, k : k + 1], out.shape[1]).astype(BF)


def place_kernel(lay, whole_ref, even_ref, odd_ref, *refs):
    ins, z_ref = refs[:-1], refs[-1]
    columns = []
    for own, left, right in (ins[:3], ins[3:]):
        total = own[...] + left[...].astype(F32) + right[...].astype(F32)
        columns.append(total.astype(BF))
    y = jnp.concatenate(columns, axis=1)
    came = z_ref.shape[0]
    none = lambda n: jnp.zeros((came, n), BF)
    rows = dot(whole_ref[...], y, ((1,), (1,))).astype(BF)
    z_ref[:, : lay.low] = jnp.concatenate([rows, none(lay.low - lay.width)], axis=1)
    left = dot(even_ref[...], y[: lay.point], ((1,), (1,))).astype(BF)
    right = dot(odd_ref[...], y[lay.point :], ((1,), (1,))).astype(BF)
    z_ref[:, lay.low :] = left + jnp.concatenate([right, none(lay.short)], axis=1)


def router_kernel(lay, id_ref, p_ref, w_ref):
    tok, seats = id_ref.shape[1], lay.seats
    ids, prob = id_ref[...].astype(F32).T, p_ref[...].T
    top = ids.shape[1]
    lane = iota((tok, lay.experts), 1).astype(F32)
    named = [ids[:, k : k + 1] == lane for k in range(top)]
    hits = jnp.zeros((tok, lay.experts), F32)
    for k in range(top):
        hits += jnp.where(named[k], 1.0, 0.0)
    earlier = (iota((tok, tok), 1) < iota((tok, tok), 0)).astype(BF)
    order = dot(earlier, hits.astype(BF))
    rows = lay.experts * seats
    kinds = [jnp.zeros((tok, rows), F32) for _ in range(3)]
    for k in range(top):
        seat = jnp.sum(jnp.where(named[k], order, 0.0), axis=1, keepdims=True)
        base = ids[:, k : k + 1] * seats
        full = jnp.where(seat < seats, base + seat, -1.0)
        over = jnp.where(seat < seats, -1.0, base + 2.0 * (seat - seats))
        odd = jnp.where(seat < seats, -1.0, over + 1.0)
        for n, place in enumerate((full, over, odd)):
            kinds[n] += hot(place, rows) * prob[:, k : k + 1]
    for n, kind in enumerate(kinds):
        high = kind.astype(BF)
        rest = kind - high.astype(F32)
        middle = rest.astype(BF)
        low = (rest - middle.astype(F32)).astype(BF)
        w_ref[n] = jnp.concatenate([high, middle, low], axis=0)


def mix_kernel(lay, b_ref, w_ref, o_ref):
    tok, rows = o_ref.shape[0], w_ref.shape[2]

    def weighted(n, block):
        three = dot(w_ref[n], block)
        return three[:tok] + three[tok : 2 * tok] + three[2 * tok :]

    for b in range(o_ref.shape[1] // lay.width):
        at = slice(b * rows, (b + 1) * rows)
        whole_rows = weighted(0, b_ref[at, : lay.width])
        rest = b_ref[at, lay.low :]
        left, right = weighted(1, rest), weighted(2, rest)
        extra = jnp.concatenate([left, right[:, : lay.width - lay.point]], axis=1)
        o_ref[:, b * lay.width : (b + 1) * lay.width] = (whole_rows + extra).astype(BF)


VMEM = pl.BlockSpec(memory_space=pltpu.VMEM)
SMEM = pl.BlockSpec(memory_space=pltpu.SMEM)
ANY = pl.BlockSpec(memory_space=pl.ANY)
shape = jax.ShapeDtypeStruct


class Layout:
    def __init__(self, width, experts, most):
        self.width, self.experts = width, experts
        self.seats = 8
        self.low = (width + 2 + 127) // 128 * 128
        self.point = (width // 2 + 127) // 128 * 128
        self.short = 2 * self.point - width
        self.lanes = self.low + self.point
        assert self.seats <= most <= self.seats * 3 // 2


def cost(flops, moved):
    return pl.CostEstimate(flops=flops, bytes_accessed=moved, transcendentals=0)


def grant(mebibytes):
    return pltpu.CompilerParams(vmem_limit_bytes=mebibytes << 20)


def run(kernel, ins, outs, work, scratch=(), mebibytes=12):
    return pl.pallas_call(
        kernel,
        out_shape=outs,
        in_specs=ins,
        out_specs=jax.tree.map(lambda _: VMEM, outs),
        scratch_shapes=scratch,
        cost_estimate=cost(*work),
        compiler_params=grant(mebibytes),
    )


def on_device(
    tokens, expert_ids, gate_probs, shed_blocks, partner, gate_weight, up_weight, down_weight
):
    tok, model = tokens.shape
    top = expert_ids.shape[1]
    experts = shed_blocks.shape[0]
    groups = lax.axis_size("attn")
    width = model // groups
    capacity = tok * top * groups
    block = capacity // 8
    slots = capacity + block * SHED_MOST
    units = gate_weight.shape[2]
    lay = Layout(width, experts, min(tok, 3 * tok * top // experts))
    devices = groups * experts
    came = devices * lay.seats
    me = lax.axis_index(EXPERT)
    bound = capacity - block * shed_blocks[partner[me]] + block * shed_blocks[me]
    par = bound.reshape(1).astype(jnp.int32)
    at = lax.axis_index("attn").astype(jnp.int32).reshape(1)

    def shifted(distance):
        pairs = [(i, (i + distance) % groups) for i in range(groups)]
        return lambda array: lax.ppermute(array, "attn", pairs)

    right, left = shifted(1), shifted(groups - 1)

    def exchange(rows):
        blocks = rows.reshape(devices, lay.seats, lay.lanes)
        moved = lax.all_to_all(blocks, ATTN_EXPERT, split_axis=0, concat_axis=0, tiled=True)
        return moved.reshape(came, lay.lanes)

    packed = shape((came, lay.lanes), BF)
    block_rows = experts * lay.seats
    outgoing, seen = pl.pallas_call(
        lambda *refs: send_kernel(lay, groups, *refs),
        grid=(groups,),
        out_shape=(packed, shape((8, 128), F32)),
        in_specs=[
            pl.BlockSpec((tok, model), lambda i: (0, 0)),
            pl.BlockSpec((top, tok), lambda i: (0, 0)),
        ],
        out_specs=(
            pl.BlockSpec((block_rows, lay.lanes), lambda i: (i, 0)),
            pl.BlockSpec((8, 128), lambda i: (0, 0)),
        ),
        scratch_shapes=[
            pltpu.VMEM((3, block_rows, tok), BF),
            pltpu.VMEM((block_rows, lay.low), F32),
        ],
        cost_estimate=cost(2 * tok * came * width, 2 * came * width),
        compiler_params=grant(60),
        name="send",
    )(tokens, expert_ids.T)
    arrived = exchange(outgoing)
    relaid = shape((groups, units, width), BF)
    step = 128
    rows_in = pl.BlockSpec((step, model), lambda i: (i, 0))
    rows_out = pl.BlockSpec((groups, step, width), lambda i: (0, i, 0))
    wg, wu, wd = pl.pallas_call(
        relay_kernel,
        grid=(pl.cdiv(units, step),),
        out_shape=(relaid, relaid, shape((groups, width, units), BF)),
        in_specs=[ANY] + [rows_in] * 3,
        out_specs=(rows_out, rows_out, pl.BlockSpec((groups, width, step), lambda i: (0, 0, i))),
        cost_estimate=cost(12 * slots * width * units, 12 * model * units),
        compiler_params=grant(60),
        name="relay",
    )(seen, gate_weight[0].T, up_weight[0].T, down_weight[0])
    arrived, wg, wu, wd = lax.optimization_barrier((arrived, wg, wu, wd))

    weights = run(
        lambda *refs: router_kernel(lay, *refs),
        [VMEM] * 2,
        shape((3, 3 * tok, block_rows), BF),
        (12 * tok * block_rows, 18 * tok * block_rows),
    )(expert_ids.T, gate_probs.T)
    part = slots // 2
    columns = shape((width, part), BF)
    gather_work = (2 * slots * came * width, 2 * came * width)
    places, own_a = run(
        lambda *refs: pick_kernel(lay, *refs),
        [VMEM, SMEM],
        (shape((8, came), F32), columns),
        gather_work,
    )(arrived, par)
    own_b = run(
        lambda *refs: pick_more_kernel(lay, part, *refs), [VMEM] * 2, columns, gather_work
    )(arrived, places)
    spot = shape((came, slots), BF)
    spots = run(spots_kernel, [VMEM], (spot,) * 3, (6 * came * slots, 6 * came * slots))(places)
    before, after, across = groups - 1, 1, groups // 2
    area = width * units
    rows = lambda n, kind: shape((n, part), kind)

    def mid(blocks, ahead):
        return run(
            lambda *refs: mid_kernel(ahead, *refs),
            [SMEM] + [VMEM] * (2 + len(blocks)),
            (rows(units, F32), rows(units, F32)),
            (4 * len(blocks) * part * area, 4 * len(blocks) * area),
        )(at, wg, wu, *blocks)

    def far(sums, blocks, ahead):
        count = 4 * len(blocks) + 2
        return run(
            lambda *refs: far_kernel(ahead, *refs),
            [SMEM] + [VMEM] * (5 + len(blocks)),
            (rows(units, BF), rows(width, BF)),
            (count * part * area, count * area),
        )(at, wg, wu, wd, *sums, *blocks)

    def near(hidden, kinds):
        return run(
            near_kernel,
            [SMEM] + [VMEM] * 2,
            tuple(rows(width, kind) for kind in kinds),
            (6 * part * area, 6 * area),
        )(at, hidden, wd)

    def add(mine, came):
        return (mine + came.astype(F32)).astype(BF)

    below_a, above_a = right(own_a), left(own_a)
    above_b = left(own_b)
    far_a = right(below_a)
    below_b = right(own_b)
    far_b = left(above_b)
    sums_a = mid((own_a, below_a, above_a), (0, before, after))
    hidden_a, share_a = far(sums_a, (far_a,), (across,))
    crossed_a = right(share_a)
    mine_a, left_a, right_a = near(hidden_a, (F32, BF, F32))
    from_right_a = left(left_a)
    sums_b = mid((own_b, above_b), (0, after))
    hidden_b, share_b = far(sums_b, (below_b, far_b), (before, across))
    crossed_b = left(share_b)
    mine_b, left_b, right_b = near(hidden_b, (F32, F32, BF))
    from_left_b = right(right_b)
    added_a, added_b = add(right_a, crossed_a), add(left_b, crossed_b)
    from_left_a = right(added_a)
    from_right_b = left(added_b)
    sums = (mine_a, from_left_a, from_right_a, mine_b, from_left_b, from_right_b)
    answers = run(
        lambda *refs: place_kernel(lay, *refs), [VMEM] * 9, packed, gather_work
    )(*spots, *sums)
    return run(
        lambda *refs: mix_kernel(lay, *refs),
        [VMEM] * 2,
        shape((tok, model), BF),
        (6 * tok * came * width, 2 * came * width),
    )(exchange(answers), weights)


def solution(mesh):
    split = Mesh(
        mesh.devices.reshape(mesh.shape["attn"], 4, 4, 2),
        ("attn", "expert_0", "expert_1", "expert_2"),
    )
    return jax.shard_map(
        on_device,
        mesh=split,
        in_specs=(
            P(ATTN_EXPERT, None),
            P(ATTN_EXPERT, None),
            P(ATTN_EXPERT, None),
            P(),
            P(),
            P(EXPERT, None, "attn"),
            P(EXPERT, None, "attn"),
            P(EXPERT, "attn", None),
        ),
        out_specs=P(ATTN_EXPERT, None),
        check_vma=False,
    )
```

```python
import jax
import jax.numpy as jnp
from jax import lax
from jax.experimental import pallas as pl
from jax.experimental.pallas import tpu as pltpu
from jax.sharding import Mesh
from jax.sharding import PartitionSpec as P

SHED_MOST = 4
ATTN_EXPERT = ("attn", "expert_0", "expert_1", "expert_2")
EXPERT = ("expert_0", "expert_1", "expert_2")
SWISH_SCALE = 1.702
BF = jnp.bfloat16
F32 = jnp.float32


def iota(shape, dim):
    return lax.broadcasted_iota(jnp.int32, shape, dim)


def dot(a, b, dims=((1,), (0,))):
    return lax.dot_general(a, b, (dims, ((), ())), preferred_element_type=F32)


def hot(places, width, first=0):
    at = (iota((places.shape[0], width), 1) + first).astype(F32)
    return jnp.where(places == at, 1.0, 0.0)


def send_kernel(lay, x_ref, id_ref, s_ref, seen_ref):
    tok, experts, seats = x_ref.shape[0], lay.experts, lay.seats
    seen_ref[...] = jnp.zeros_like(seen_ref)
    ids = id_ref[...].astype(F32)
    expert = iota((experts, tok), 0).astype(F32)
    hits = jnp.zeros((experts, tok), F32)
    for k in range(ids.shape[0]):
        hits += jnp.where(ids[k : k + 1] == expert, 1.0, 0.0)
    earlier = (iota((tok, tok), 0) < iota((tok, tok), 1)).astype(BF)
    order = dot(hits.astype(BF), earlier)
    order = jnp.where(hits > 0.5, order, -1.0).astype(BF)
    rows = experts * seats
    spread = (iota((rows, experts), 0) // seats == iota((rows, experts), 1)).astype(BF)
    order = dot(spread, order)
    seat = iota((rows, tok), 0) % seats
    over = (seats + seat // 2).astype(F32)
    full = jnp.where(order == seat.astype(F32), 1.0, 0.0).astype(BF)
    part = jnp.where(order == over, 1.0, 0.0)
    even = jnp.where(seat % 2 == 0, part, 0.0).astype(BF)
    odd = jnp.where(seat % 2 == 1, part, 0.0).astype(BF)
    one, none = jnp.ones((tok, 1), BF), lambda n: jnp.zeros((tok, n), BF)
    second = jnp.concatenate([none(lay.width + 1), one, none(lay.low - lay.width - 2)], axis=1)
    flags = dot(part.astype(BF), second)
    for b in range(x_ref.shape[1] // lay.width):
        first = b * lay.width
        x = x_ref[:, first : first + lay.width]
        at = slice(b * rows, (b + 1) * rows)
        wide = jnp.concatenate([x, one, none(lay.low - lay.width - 1)], axis=1)
        s_ref[at, : lay.low] = (dot(full, wide) + flags).astype(BF)
        tail = jnp.concatenate([x[:, lay.point :], none(lay.short)], axis=1)
        s_ref[at, lay.low :] = (dot(even, x[:, : lay.point]) + dot(odd, tail)).astype(BF)


def gather_slots(lay, rows, x_ref, first, out):
    slots = out.shape[1]
    place = (iota((slots, x_ref.shape[0]), 0) + first).astype(F32)
    match = lambda row: jnp.where(row == place, 1.0, 0.0).astype(BF)
    got = dot(match(rows[0]), x_ref[:, : lay.width])
    rest = x_ref[:, lay.low :]
    left, right = dot(match(rows[1]), rest), dot(match(rows[2]), rest)
    extra = jnp.concatenate([left, right[:, : lay.width - lay.point]], axis=1)
    out[...] = (got + extra).astype(BF).T


def pick_more_kernel(lay, first, x_ref, row_ref, out):
    gather_slots(lay, [row_ref[k : k + 1] for k in range(3)], x_ref, first, out)


def pick_kernel(lay, x_ref, par_ref, row_ref, out):
    came, seats = x_ref.shape[0], lay.seats
    sources = came // seats
    bound = par_ref[0].astype(F32)
    start = lay.width // 128 * 128
    tail = x_ref[:, start : lay.low]
    choose = (iota((8, tail.shape[1]), 1) == iota((8, tail.shape[1]), 0) + lay.width - start)
    flags = dot(choose.astype(BF), tail, ((1,), (1,)))
    full, part = flags[0:1], flags[1:2]
    seat = iota((1, came), 1) % seats
    even = seat % 2 == 0
    owner = iota((sources, came), 0) == iota((sources, came), 1) // seats
    each = full + jnp.where(even, part, 0.0)
    counts = jnp.sum(jnp.where(owner, each, 0.0), axis=1, keepdims=True)
    counts = jnp.broadcast_to(counts, (sources, 128)).astype(BF)
    earlier = (iota((sources, sources), 1) < iota((sources, sources), 0)).astype(BF)
    before = dot(earlier, counts)[:, 0:1]
    base = jnp.sum(jnp.where(owner, before, 0.0), axis=0, keepdims=True)
    rank = base + seat.astype(F32)
    over = base + (seats + seat // 2).astype(F32)
    rank = jnp.where(jnp.logical_and(full > 0.5, rank < bound), rank, -1.0)
    over = jnp.where(jnp.logical_and(part > 0.5, over < bound), over, -1.0)
    evens, odds = jnp.where(even, over, -1.0), jnp.where(even, -1.0, over)
    nothing = jnp.full((5, came), -1.0, F32)
    row_ref[...] = jnp.concatenate([rank, evens, odds, nothing], axis=0)
    gather_slots(lay, (rank, evens, odds), x_ref, 0, out)


def relay_kernel(seen_ref, g_ref, u_ref, d_ref, go_ref, uo_ref, do_ref):
    del seen_ref
    blocks, width = go_ref.shape[0], go_ref.shape[2]
    for b in range(blocks):
        at = slice(b * width, (b + 1) * width)
        go_ref[b] = g_ref[:, at]
        uo_ref[b] = u_ref[:, at]
        do_ref[b] = d_ref[:, at].T


def gate_up(at, ahead, wg_ref, wu_ref, blocks):
    gate = up = None
    for distance, x in zip(ahead, blocks):
        block = lax.rem(at + distance, wg_ref.shape[0])
        g, u = dot(wg_ref[block], x[...]), dot(wu_ref[block], x[...])
        gate, up = (g, u) if gate is None else (gate + g, up + u)
    return gate, up


def mid_kernel(ahead, at_ref, wg_ref, wu_ref, *refs):
    refs[-2][...], refs[-1][...] = gate_up(at_ref[0], ahead, wg_ref, wu_ref, refs[:-2])


def far_kernel(ahead, at_ref, wg_ref, wu_ref, wd_ref, g_ref, u_ref, *refs):
    gate, up = gate_up(at_ref[0], ahead, wg_ref, wu_ref, refs[:-2])
    h_ref, o_ref = refs[-2:]
    gate, up = gate + g_ref[...], up + u_ref[...]
    hidden = (gate * jax.nn.sigmoid(SWISH_SCALE * gate) * (up + 1.0)).astype(BF)
    h_ref[...] = hidden
    groups = wd_ref.shape[0]
    across = lax.rem(at_ref[0] + groups // 2, groups)
    o_ref[...] = dot(wd_ref[across], hidden).astype(BF)


def near_kernel(at_ref, h_ref, wd_ref, *outs):
    hidden = h_ref[...]
    groups = wd_ref.shape[0]
    for distance, out in zip((0, groups - 1, 1), outs):
        block = lax.rem(at_ref[0] + distance, groups)
        out[...] = dot(wd_ref[block], hidden).astype(out.dtype)


def spots_kernel(row_ref, *outs):
    places = row_ref[...].T
    for k, out in enumerate(outs):
        out[...] = hot(places[:, k : k + 1], out.shape[1]).astype(BF)


def place_kernel(lay, whole_ref, even_ref, odd_ref, *refs):
    ins, z_ref = refs[:-1], refs[-1]
    columns = []
    for own, left, right in (ins[:3], ins[3:]):
        total = own[...] + left[...].astype(F32) + right[...].astype(F32)
        columns.append(total.astype(BF))
    y = jnp.concatenate(columns, axis=1)
    came = z_ref.shape[0]
    none = lambda n: jnp.zeros((came, n), BF)
    rows = dot(whole_ref[...], y, ((1,), (1,))).astype(BF)
    z_ref[:, : lay.low] = jnp.concatenate([rows, none(lay.low - lay.width)], axis=1)
    left = dot(even_ref[...], y[: lay.point], ((1,), (1,))).astype(BF)
    right = dot(odd_ref[...], y[lay.point :], ((1,), (1,))).astype(BF)
    z_ref[:, lay.low :] = left + jnp.concatenate([right, none(lay.short)], axis=1)


def router_kernel(lay, id_ref, p_ref, w_ref):
    tok, seats = id_ref.shape[1], lay.seats
    ids, prob = id_ref[...].astype(F32).T, p_ref[...].T
    top = ids.shape[1]
    lane = iota((tok, lay.experts), 1).astype(F32)
    named = [ids[:, k : k + 1] == lane for k in range(top)]
    hits = jnp.zeros((tok, lay.experts), F32)
    for k in range(top):
        hits += jnp.where(named[k], 1.0, 0.0)
    earlier = (iota((tok, tok), 1) < iota((tok, tok), 0)).astype(BF)
    order = dot(earlier, hits.astype(BF))
    rows = lay.experts * seats
    kinds = [jnp.zeros((tok, rows), F32) for _ in range(3)]
    for k in range(top):
        seat = jnp.sum(jnp.where(named[k], order, 0.0), axis=1, keepdims=True)
        base = ids[:, k : k + 1] * seats
        full = jnp.where(seat < seats, base + seat, -1.0)
        over = jnp.where(seat < seats, -1.0, base + 2.0 * (seat - seats))
        odd = jnp.where(seat < seats, -1.0, over + 1.0)
        for n, place in enumerate((full, over, odd)):
            kinds[n] += hot(place, rows) * prob[:, k : k + 1]
    for n, kind in enumerate(kinds):
        high = kind.astype(BF)
        rest = kind - high.astype(F32)
        middle = rest.astype(BF)
        low = (rest - middle.astype(F32)).astype(BF)
        w_ref[n] = jnp.concatenate([high, middle, low], axis=0)


def mix_kernel(lay, b_ref, w_ref, o_ref):
    tok, rows = o_ref.shape[0], w_ref.shape[2]

    def weighted(n, block):
        three = dot(w_ref[n], block)
        return three[:tok] + three[tok : 2 * tok] + three[2 * tok :]

    for b in range(o_ref.shape[1] // lay.width):
        at = slice(b * rows, (b + 1) * rows)
        whole_rows = weighted(0, b_ref[at, : lay.width])
        rest = b_ref[at, lay.low :]
        left, right = weighted(1, rest), weighted(2, rest)
        extra = jnp.concatenate([left, right[:, : lay.width - lay.point]], axis=1)
        o_ref[:, b * lay.width : (b + 1) * lay.width] = (whole_rows + extra).astype(BF)


VMEM = pl.BlockSpec(memory_space=pltpu.VMEM)
SMEM = pl.BlockSpec(memory_space=pltpu.SMEM)
ANY = pl.BlockSpec(memory_space=pl.ANY)
shape = jax.ShapeDtypeStruct


class Layout:
    def __init__(self, width, experts, most):
        self.width, self.experts = width, experts
        self.seats = 8
        self.low = (width + 2 + 127) // 128 * 128
        self.point = (width // 2 + 127) // 128 * 128
        self.short = 2 * self.point - width
        self.lanes = self.low + self.point
        assert self.seats <= most <= self.seats * 3 // 2


def cost(flops, moved):
    return pl.CostEstimate(flops=flops, bytes_accessed=moved, transcendentals=0)


def grant(mebibytes):
    return pltpu.CompilerParams(vmem_limit_bytes=mebibytes << 20)


def run(kernel, ins, outs, work, scratch=(), mebibytes=12):
    return pl.pallas_call(
        kernel,
        out_shape=outs,
        in_specs=ins,
        out_specs=jax.tree.map(lambda _: VMEM, outs),
        scratch_shapes=scratch,
        cost_estimate=cost(*work),
        compiler_params=grant(mebibytes),
    )


def on_device(
    tokens, expert_ids, gate_probs, shed_blocks, partner, gate_weight, up_weight, down_weight
):
    tok, model = tokens.shape
    top = expert_ids.shape[1]
    experts = shed_blocks.shape[0]
    groups = lax.axis_size("attn")
    width = model // groups
    capacity = tok * top * groups
    block = capacity // 8
    slots = capacity + block * SHED_MOST
    units = gate_weight.shape[2]
    lay = Layout(width, experts, min(tok, 3 * tok * top // experts))
    devices = groups * experts
    came = devices * lay.seats
    me = lax.axis_index(EXPERT)
    bound = capacity - block * shed_blocks[partner[me]] + block * shed_blocks[me]
    par = bound.reshape(1).astype(jnp.int32)
    at = lax.axis_index("attn").astype(jnp.int32).reshape(1)

    def shifted(distance):
        pairs = [(i, (i + distance) % groups) for i in range(groups)]
        return lambda array: lax.ppermute(array, "attn", pairs)

    right, left = shifted(1), shifted(groups - 1)

    def exchange(rows):
        blocks = rows.reshape(devices, lay.seats, lay.lanes)
        moved = lax.all_to_all(blocks, ATTN_EXPERT, split_axis=0, concat_axis=0, tiled=True)
        return moved.reshape(came, lay.lanes)

    packed = shape((came, lay.lanes), BF)
    block_rows = experts * lay.seats
    block_rows = experts * lay.seats
    outgoing, seen = run(
        lambda *refs: send_kernel(lay, *refs),
        [VMEM] * 2,
        (packed, shape((8, 128), F32)),
        (2 * tok * came * width, 2 * came * width),
        mebibytes=60,
    )(tokens, expert_ids.T)
    arrived = exchange(outgoing)
    relaid = shape((groups, units, width), BF)
    step = 128
    rows_in = pl.BlockSpec((step, model), lambda i: (i, 0))
    rows_out = pl.BlockSpec((groups, step, width), lambda i: (0, i, 0))
    wg, wu, wd = pl.pallas_call(
        relay_kernel,
        grid=(pl.cdiv(units, step),),
        out_shape=(relaid, relaid, shape((groups, width, units), BF)),
        in_specs=[ANY] + [rows_in] * 3,
        out_specs=(rows_out, rows_out, pl.BlockSpec((groups, width, step), lambda i: (0, 0, i))),
        cost_estimate=cost(12 * slots * width * units, 12 * model * units),
        compiler_params=grant(60),
        name="relay",
    )(seen, gate_weight[0].T, up_weight[0].T, down_weight[0])
    arrived, wg, wu, wd = lax.optimization_barrier((arrived, wg, wu, wd))

    weights = run(
        lambda *refs: router_kernel(lay, *refs),
        [VMEM] * 2,
        shape((3, 3 * tok, block_rows), BF),
        (12 * tok * block_rows, 18 * tok * block_rows),
    )(expert_ids.T, gate_probs.T)
    part = slots // 2
    columns = shape((width, part), BF)
    gather_work = (2 * slots * came * width, 2 * came * width)
    places, own_a = run(
        lambda *refs: pick_kernel(lay, *refs),
        [VMEM, SMEM],
        (shape((8, came), F32), columns),
        gather_work,
    )(arrived, par)
    own_b = run(
        lambda *refs: pick_more_kernel(lay, part, *refs), [VMEM] * 2, columns, gather_work
    )(arrived, places)
    spot = shape((came, slots), BF)
    spots = run(spots_kernel, [VMEM], (spot,) * 3, (6 * came * slots, 6 * came * slots))(places)
    before, after, across = groups - 1, 1, groups // 2
    area = width * units
    rows = lambda n, kind: shape((n, part), kind)

    def mid(blocks, ahead):
        return run(
            lambda *refs: mid_kernel(ahead, *refs),
            [SMEM] + [VMEM] * (2 + len(blocks)),
            (rows(units, F32), rows(units, F32)),
            (4 * len(blocks) * part * area, 4 * len(blocks) * area),
        )(at, wg, wu, *blocks)

    def far(sums, blocks, ahead):
        count = 4 * len(blocks) + 2
        return run(
            lambda *refs: far_kernel(ahead, *refs),
            [SMEM] + [VMEM] * (5 + len(blocks)),
            (rows(units, BF), rows(width, BF)),
            (count * part * area, count * area),
        )(at, wg, wu, wd, *sums, *blocks)

    def near(hidden, kinds):
        return run(
            near_kernel,
            [SMEM] + [VMEM] * 2,
            tuple(rows(width, kind) for kind in kinds),
            (6 * part * area, 6 * area),
        )(at, hidden, wd)

    def add(mine, came):
        return (mine + came.astype(F32)).astype(BF)

    above_a = left(own_a)
    below_b = right(own_b)
    above_b = left(own_b)
    below_a = right(own_a)
    far_a = left(above_a)
    far_b = right(below_b)
    sums_a = mid((own_a, below_a, above_a), (0, before, after))
    sums_b = mid((own_b, below_b, above_b), (0, before, after))
    hidden_a, share_a = far(sums_a, (far_a,), (across,))
    crossed_a = right(share_a)
    hidden_b, share_b = far(sums_b, (far_b,), (across,))
    crossed_b = left(share_b)
    mine_b, left_b, right_b = near(hidden_b, (F32, F32, BF))
    from_left_b = right(right_b)
    mine_a, left_a, right_a = near(hidden_a, (F32, BF, F32))
    from_right_a = left(left_a)
    added_a, added_b = add(right_a, crossed_a), add(left_b, crossed_b)
    from_left_a = right(added_a)
    from_right_b = left(added_b)
    sums = (mine_a, from_left_a, from_right_a, mine_b, from_left_b, from_right_b)
    answers = run(
        lambda *refs: place_kernel(lay, *refs), [VMEM] * 9, packed, gather_work
    )(*spots, *sums)
    return run(
        lambda *refs: mix_kernel(lay, *refs),
        [VMEM] * 2,
        shape((tok, model), BF),
        (6 * tok * came * width, 2 * came * width),
    )(exchange(answers), weights)


def solution(mesh):
    split = Mesh(
        mesh.devices.reshape(mesh.shape["attn"], 4, 4, 2),
        ("attn", "expert_0", "expert_1", "expert_2"),
    )
    return jax.shard_map(
        on_device,
        mesh=split,
        in_specs=(
            P(ATTN_EXPERT, None),
            P(ATTN_EXPERT, None),
            P(ATTN_EXPERT, None),
            P(),
            P(),
            P(EXPERT, None, "attn"),
            P(EXPERT, None, "attn"),
            P(EXPERT, "attn", None),
        ),
        out_specs=P(ATTN_EXPERT, None),
        check_vma=False,
    )
```

```python
import jax
import jax.numpy as jnp
from jax import lax
from jax.experimental import pallas as pl
from jax.experimental.pallas import tpu as pltpu
from jax.sharding import Mesh
from jax.sharding import PartitionSpec as P

SHED_MOST = 4
ATTN_EXPERT = ("attn", "expert_0", "expert_1", "expert_2")
EXPERT = ("expert_0", "expert_1", "expert_2")
SWISH_SCALE = 1.702
BF = jnp.bfloat16
F32 = jnp.float32


def iota(shape, dim):
    return lax.broadcasted_iota(jnp.int32, shape, dim)


def dot(a, b, dims=((1,), (0,))):
    return lax.dot_general(a, b, (dims, ((), ())), preferred_element_type=F32)


def hot(places, width, first=0):
    at = (iota((places.shape[0], width), 1) + first).astype(F32)
    return jnp.where(places == at, 1.0, 0.0)


def send_kernel(lay, x_ref, id_ref, s_ref, seen_ref):
    tok, experts, seats = x_ref.shape[0], lay.experts, lay.seats
    seen_ref[...] = jnp.zeros_like(seen_ref)
    ids = id_ref[...].astype(F32)
    expert = iota((experts, tok), 0).astype(F32)
    hits = jnp.zeros((experts, tok), F32)
    for k in range(ids.shape[0]):
        hits += jnp.where(ids[k : k + 1] == expert, 1.0, 0.0)
    earlier = (iota((tok, tok), 0) < iota((tok, tok), 1)).astype(BF)
    order = dot(hits.astype(BF), earlier)
    order = jnp.where(hits > 0.5, order, -1.0).astype(BF)
    rows = experts * seats
    spread = (iota((rows, experts), 0) // seats == iota((rows, experts), 1)).astype(BF)
    order = dot(spread, order)
    seat = iota((rows, tok), 0) % seats
    over = (seats + seat // 2).astype(F32)
    full = jnp.where(order == seat.astype(F32), 1.0, 0.0).astype(BF)
    part = jnp.where(order == over, 1.0, 0.0)
    even = jnp.where(seat % 2 == 0, part, 0.0).astype(BF)
    odd = jnp.where(seat % 2 == 1, part, 0.0).astype(BF)
    one, none = jnp.ones((tok, 1), BF), lambda n: jnp.zeros((tok, n), BF)
    second = jnp.concatenate([none(lay.width + 1), one, none(lay.low - lay.width - 2)], axis=1)
    flags = dot(part.astype(BF), second)
    for b in range(x_ref.shape[1] // lay.width):
        first = b * lay.width
        x = x_ref[:, first : first + lay.width]
        at = slice(b * rows, (b + 1) * rows)
        wide = jnp.concatenate([x, one, none(lay.low - lay.width - 1)], axis=1)
        s_ref[at, : lay.low] = (dot(full, wide) + flags).astype(BF)
        tail = jnp.concatenate([x[:, lay.point :], none(lay.short)], axis=1)
        s_ref[at, lay.low :] = (dot(even, x[:, : lay.point]) + dot(odd, tail)).astype(BF)


def gather_slots(lay, rows, x_ref, first, out):
    slots = out.shape[1]
    place = (iota((slots, x_ref.shape[0]), 0) + first).astype(F32)
    match = lambda row: jnp.where(row == place, 1.0, 0.0).astype(BF)
    got = dot(match(rows[0]), x_ref[:, : lay.width])
    rest = x_ref[:, lay.low :]
    left, right = dot(match(rows[1]), rest), dot(match(rows[2]), rest)
    extra = jnp.concatenate([left, right[:, : lay.width - lay.point]], axis=1)
    out[...] = (got + extra).astype(BF).T


def pick_more_kernel(lay, first, x_ref, row_ref, out):
    gather_slots(lay, [row_ref[k : k + 1] for k in range(3)], x_ref, first, out)


def pick_kernel(lay, x_ref, par_ref, row_ref, out):
    came, seats = x_ref.shape[0], lay.seats
    sources = came // seats
    bound = par_ref[0].astype(F32)
    start = lay.width // 128 * 128
    tail = x_ref[:, start : lay.low]
    choose = (iota((8, tail.shape[1]), 1) == iota((8, tail.shape[1]), 0) + lay.width - start)
    flags = dot(choose.astype(BF), tail, ((1,), (1,)))
    full, part = flags[0:1], flags[1:2]
    seat = iota((1, came), 1) % seats
    even = seat % 2 == 0
    owner = iota((sources, came), 0) == iota((sources, came), 1) // seats
    each = full + jnp.where(even, part, 0.0)
    counts = jnp.sum(jnp.where(owner, each, 0.0), axis=1, keepdims=True)
    counts = jnp.broadcast_to(counts, (sources, 128)).astype(BF)
    earlier = (iota((sources, sources), 1) < iota((sources, sources), 0)).astype(BF)
    before = dot(earlier, counts)[:, 0:1]
    base = jnp.sum(jnp.where(owner, before, 0.0), axis=0, keepdims=True)
    rank = base + seat.astype(F32)
    over = base + (seats + seat // 2).astype(F32)
    rank = jnp.where(jnp.logical_and(full > 0.5, rank < bound), rank, -1.0)
    over = jnp.where(jnp.logical_and(part > 0.5, over < bound), over, -1.0)
    evens, odds = jnp.where(even, over, -1.0), jnp.where(even, -1.0, over)
    nothing = jnp.full((5, came), -1.0, F32)
    row_ref[...] = jnp.concatenate([rank, evens, odds, nothing], axis=0)
    gather_slots(lay, (rank, evens, odds), x_ref, 0, out)


def relay_kernel(seen_ref, g_ref, u_ref, d_ref, go_ref, uo_ref, do_ref):
    del seen_ref
    blocks, width = go_ref.shape[0], go_ref.shape[2]
    for b in range(blocks):
        at = slice(b * width, (b + 1) * width)
        go_ref[b] = g_ref[:, at]
        uo_ref[b] = u_ref[:, at]
        do_ref[b] = d_ref[:, at].T


def gate_up(at, ahead, wg_ref, wu_ref, blocks):
    gate = up = None
    for distance, x in zip(ahead, blocks):
        block = lax.rem(at + distance, wg_ref.shape[0])
        g, u = dot(wg_ref[block], x[...]), dot(wu_ref[block], x[...])
        gate, up = (g, u) if gate is None else (gate + g, up + u)
    return gate, up


def mid_kernel(ahead, at_ref, wg_ref, wu_ref, *refs):
    refs[-2][...], refs[-1][...] = gate_up(at_ref[0], ahead, wg_ref, wu_ref, refs[:-2])


def far_kernel(ahead, at_ref, wg_ref, wu_ref, wd_ref, g_ref, u_ref, *refs):
    gate, up = gate_up(at_ref[0], ahead, wg_ref, wu_ref, refs[:-2])
    h_ref, o_ref = refs[-2:]
    gate, up = gate + g_ref[...], up + u_ref[...]
    hidden = (gate * jax.nn.sigmoid(SWISH_SCALE * gate) * (up + 1.0)).astype(BF)
    h_ref[...] = hidden
    groups = wd_ref.shape[0]
    across = lax.rem(at_ref[0] + groups // 2, groups)
    o_ref[...] = dot(wd_ref[across], hidden).astype(BF)


def near_kernel(at_ref, h_ref, wd_ref, *outs):
    hidden = h_ref[...]
    groups = wd_ref.shape[0]
    for distance, out in zip((0, groups - 1, 1), outs):
        block = lax.rem(at_ref[0] + distance, groups)
        out[...] = dot(wd_ref[block], hidden).astype(out.dtype)


def spots_kernel(row_ref, *outs):
    places = row_ref[...].T
    for k, out in enumerate(outs):
        out[...] = hot(places[:, k : k + 1], out.shape[1]).astype(BF)


def place_kernel(lay, whole_ref, even_ref, odd_ref, *refs):
    ins, z_ref = refs[:-1], refs[-1]
    columns = []
    for own, left, right in (ins[:3], ins[3:]):
        total = own[...] + left[...].astype(F32) + right[...].astype(F32)
        columns.append(total.astype(BF))
    y = jnp.concatenate(columns, axis=1)
    came = z_ref.shape[0]
    none = lambda n: jnp.zeros((came, n), BF)
    rows = dot(whole_ref[...], y, ((1,), (1,))).astype(BF)
    z_ref[:, : lay.low] = jnp.concatenate([rows, none(lay.low - lay.width)], axis=1)
    left = dot(even_ref[...], y[: lay.point], ((1,), (1,))).astype(BF)
    right = dot(odd_ref[...], y[lay.point :], ((1,), (1,))).astype(BF)
    z_ref[:, lay.low :] = left + jnp.concatenate([right, none(lay.short)], axis=1)


def router_kernel(lay, id_ref, p_ref, w_ref):
    tok, seats = id_ref.shape[1], lay.seats
    ids, prob = id_ref[...].astype(F32).T, p_ref[...].T
    top = ids.shape[1]
    lane = iota((tok, lay.experts), 1).astype(F32)
    named = [ids[:, k : k + 1] == lane for k in range(top)]
    hits = jnp.zeros((tok, lay.experts), F32)
    for k in range(top):
        hits += jnp.where(named[k], 1.0, 0.0)
    earlier = (iota((tok, tok), 1) < iota((tok, tok), 0)).astype(BF)
    order = dot(earlier, hits.astype(BF))
    rows = lay.experts * seats
    kinds = [jnp.zeros((tok, rows), F32) for _ in range(3)]
    for k in range(top):
        seat = jnp.sum(jnp.where(named[k], order, 0.0), axis=1, keepdims=True)
        base = ids[:, k : k + 1] * seats
        full = jnp.where(seat < seats, base + seat, -1.0)
        over = jnp.where(seat < seats, -1.0, base + 2.0 * (seat - seats))
        odd = jnp.where(seat < seats, -1.0, over + 1.0)
        for n, place in enumerate((full, over, odd)):
            kinds[n] += hot(place, rows) * prob[:, k : k + 1]
    for n, kind in enumerate(kinds):
        high = kind.astype(BF)
        rest = kind - high.astype(F32)
        middle = rest.astype(BF)
        low = (rest - middle.astype(F32)).astype(BF)
        w_ref[n] = jnp.concatenate([high, middle, low], axis=0)


def mix_kernel(lay, b_ref, w_ref, o_ref):
    tok, rows = o_ref.shape[0], w_ref.shape[2]

    def weighted(n, block):
        three = dot(w_ref[n], block)
        return three[:tok] + three[tok : 2 * tok] + three[2 * tok :]

    for b in range(o_ref.shape[1] // lay.width):
        at = slice(b * rows, (b + 1) * rows)
        whole_rows = weighted(0, b_ref[at, : lay.width])
        rest = b_ref[at, lay.low :]
        left, right = weighted(1, rest), weighted(2, rest)
        extra = jnp.concatenate([left, right[:, : lay.width - lay.point]], axis=1)
        o_ref[:, b * lay.width : (b + 1) * lay.width] = (whole_rows + extra).astype(BF)


VMEM = pl.BlockSpec(memory_space=pltpu.VMEM)
SMEM = pl.BlockSpec(memory_space=pltpu.SMEM)
ANY = pl.BlockSpec(memory_space=pl.ANY)
shape = jax.ShapeDtypeStruct


class Layout:
    def __init__(self, width, experts, most):
        self.width, self.experts = width, experts
        self.seats = 8
        self.low = (width + 2 + 127) // 128 * 128
        self.point = (width // 2 + 127) // 128 * 128
        self.short = 2 * self.point - width
        self.lanes = self.low + self.point
        assert self.seats <= most <= self.seats * 3 // 2


def cost(flops, moved):
    return pl.CostEstimate(flops=flops, bytes_accessed=moved, transcendentals=0)


def grant(mebibytes):
    return pltpu.CompilerParams(vmem_limit_bytes=mebibytes << 20)


def run(kernel, ins, outs, work, scratch=(), mebibytes=12):
    return pl.pallas_call(
        kernel,
        out_shape=outs,
        in_specs=ins,
        out_specs=jax.tree.map(lambda _: VMEM, outs),
        scratch_shapes=scratch,
        cost_estimate=cost(*work),
        compiler_params=grant(mebibytes),
    )


def on_device(
    tokens, expert_ids, gate_probs, shed_blocks, partner, gate_weight, up_weight, down_weight
):
    tok, model = tokens.shape
    top = expert_ids.shape[1]
    experts = shed_blocks.shape[0]
    groups = lax.axis_size("attn")
    width = model // groups
    capacity = tok * top * groups
    block = capacity // 8
    slots = capacity + block * SHED_MOST
    units = gate_weight.shape[2]
    lay = Layout(width, experts, min(tok, 3 * tok * top // experts))
    devices = groups * experts
    came = devices * lay.seats
    me = lax.axis_index(EXPERT)
    bound = capacity - block * shed_blocks[partner[me]] + block * shed_blocks[me]
    par = bound.reshape(1).astype(jnp.int32)
    at = lax.axis_index("attn").astype(jnp.int32).reshape(1)

    def shifted(distance):
        pairs = [(i, (i + distance) % groups) for i in range(groups)]
        return lambda array: lax.ppermute(array, "attn", pairs)

    right, left = shifted(1), shifted(groups - 1)

    def exchange(rows):
        blocks = rows.reshape(devices, lay.seats, lay.lanes)
        moved = lax.all_to_all(blocks, ATTN_EXPERT, split_axis=0, concat_axis=0, tiled=True)
        return moved.reshape(came, lay.lanes)

    packed = shape((came, lay.lanes), BF)
    block_rows = experts * lay.seats
    block_rows = experts * lay.seats
    outgoing, seen = run(
        lambda *refs: send_kernel(lay, *refs),
        [VMEM] * 2,
        (packed, shape((8, 128), F32)),
        (2 * tok * came * width, 2 * came * width),
        mebibytes=60,
    )(tokens, expert_ids.T)
    arrived = exchange(outgoing)
    relaid = shape((groups, units, width), BF)
    step = 128
    rows_in = pl.BlockSpec((step, model), lambda i: (i, 0))
    rows_out = pl.BlockSpec((groups, step, width), lambda i: (0, i, 0))
    wg, wu, wd = pl.pallas_call(
        relay_kernel,
        grid=(pl.cdiv(units, step),),
        out_shape=(relaid, relaid, shape((groups, width, units), BF)),
        in_specs=[ANY] + [rows_in] * 3,
        out_specs=(rows_out, rows_out, pl.BlockSpec((groups, width, step), lambda i: (0, 0, i))),
        cost_estimate=cost(12 * slots * width * units, 12 * model * units),
        compiler_params=grant(60),
        name="relay",
    )(seen, gate_weight[0].T, up_weight[0].T, down_weight[0])
    arrived, wg, wu, wd = lax.optimization_barrier((arrived, wg, wu, wd))

    weights = run(
        lambda *refs: router_kernel(lay, *refs),
        [VMEM] * 2,
        shape((3, 3 * tok, block_rows), BF),
        (12 * tok * block_rows, 18 * tok * block_rows),
    )(expert_ids.T, gate_probs.T)
    part = slots // 2
    columns = shape((width, part), BF)
    gather_work = (2 * slots * came * width, 2 * came * width)
    places, own_a = run(
        lambda *refs: pick_kernel(lay, *refs),
        [VMEM, SMEM],
        (shape((8, came), F32), columns),
        gather_work,
    )(arrived, par)
    own_b = run(
        lambda *refs: pick_more_kernel(lay, part, *refs), [VMEM] * 2, columns, gather_work
    )(arrived, places)
    spot = shape((came, slots), BF)
    spots = run(spots_kernel, [VMEM], (spot,) * 3, (6 * came * slots, 6 * came * slots))(places)
    before, after, across = groups - 1, 1, groups // 2
    area = width * units
    rows = lambda n, kind: shape((n, part), kind)

    def mid(blocks, ahead):
        return run(
            lambda *refs: mid_kernel(ahead, *refs),
            [SMEM] + [VMEM] * (2 + len(blocks)),
            (rows(units, F32), rows(units, F32)),
            (4 * len(blocks) * part * area, 4 * len(blocks) * area),
        )(at, wg, wu, *blocks)

    def far(sums, blocks, ahead):
        count = 4 * len(blocks) + 2
        return run(
            lambda *refs: far_kernel(ahead, *refs),
            [SMEM] + [VMEM] * (5 + len(blocks)),
            (rows(units, BF), rows(width, BF)),
            (count * part * area, count * area),
        )(at, wg, wu, wd, *sums, *blocks)

    def near(hidden, kinds):
        return run(
            near_kernel,
            [SMEM] + [VMEM] * 2,
            tuple(rows(width, kind) for kind in kinds),
            (6 * part * area, 6 * area),
        )(at, hidden, wd)

    def add(mine, came):
        return (mine + came.astype(F32)).astype(BF)

    below_a, above_a = right(own_a), left(own_a)
    above_b = left(own_b)
    far_a = right(below_a)
    below_b = right(own_b)
    far_b = left(above_b)
    sums_a = mid((own_a, below_a, above_a), (0, before, after))
    hidden_a, share_a = far(sums_a, (far_a,), (across,))
    crossed_a = right(share_a)
    mine_a, left_a, right_a = near(hidden_a, (F32, BF, F32))
    from_right_a = left(left_a)
    sums_b = mid((own_b, above_b), (0, after))
    hidden_b, share_b = far(sums_b, (below_b, far_b), (before, across))
    crossed_b = left(share_b)
    mine_b, left_b, right_b = near(hidden_b, (F32, F32, BF))
    from_left_b = right(right_b)
    added_a, added_b = add(right_a, crossed_a), add(left_b, crossed_b)
    from_left_a = right(added_a)
    from_right_b = left(added_b)
    sums = (mine_a, from_left_a, from_right_a, mine_b, from_left_b, from_right_b)
    answers = run(
        lambda *refs: place_kernel(lay, *refs), [VMEM] * 9, packed, gather_work
    )(*spots, *sums)
    return run(
        lambda *refs: mix_kernel(lay, *refs),
        [VMEM] * 2,
        shape((tok, model), BF),
        (6 * tok * came * width, 2 * came * width),
    )(exchange(answers), weights)


def solution(mesh):
    split = Mesh(
        mesh.devices.reshape(mesh.shape["attn"], 4, 4, 2),
        ("attn", "expert_0", "expert_1", "expert_2"),
    )
    return jax.shard_map(
        on_device,
        mesh=split,
        in_specs=(
            P(ATTN_EXPERT, None),
            P(ATTN_EXPERT, None),
            P(ATTN_EXPERT, None),
            P(),
            P(),
            P(EXPERT, None, "attn"),
            P(EXPERT, None, "attn"),
            P(EXPERT, "attn", None),
        ),
        out_specs=P(ATTN_EXPERT, None),
        check_vma=False,
    )
```

```python
import jax
import jax.numpy as jnp
from jax import lax
from jax.experimental import pallas as pl
from jax.experimental.pallas import tpu as pltpu
from jax.sharding import Mesh
from jax.sharding import PartitionSpec as P

SHED_MOST = 4
ATTN_EXPERT = ("attn", "expert_0", "expert_1", "expert_2")
EXPERT = ("expert_0", "expert_1", "expert_2")
SWISH_SCALE = 1.702
BF = jnp.bfloat16
F32 = jnp.float32


def iota(shape, dim):
    return lax.broadcasted_iota(jnp.int32, shape, dim)


def dot(a, b, dims=((1,), (0,))):
    return lax.dot_general(a, b, (dims, ((), ())), preferred_element_type=F32)


def hot(places, width, first=0):
    at = (iota((places.shape[0], width), 1) + first).astype(F32)
    return jnp.where(places == at, 1.0, 0.0)


def send_kernel(lay, x_ref, id_ref, s_ref, seen_ref):
    tok, experts, seats = x_ref.shape[0], lay.experts, lay.seats
    seen_ref[...] = jnp.zeros_like(seen_ref)
    ids = id_ref[...].astype(F32)
    expert = iota((experts, tok), 0).astype(F32)
    hits = jnp.zeros((experts, tok), F32)
    for k in range(ids.shape[0]):
        hits += jnp.where(ids[k : k + 1] == expert, 1.0, 0.0)
    earlier = (iota((tok, tok), 0) < iota((tok, tok), 1)).astype(BF)
    order = dot(hits.astype(BF), earlier)
    order = jnp.where(hits > 0.5, order, -1.0).astype(BF)
    rows = experts * seats
    spread = (iota((rows, experts), 0) // seats == iota((rows, experts), 1)).astype(BF)
    order = dot(spread, order)
    seat = iota((rows, tok), 0) % seats
    over = (seats + seat // 2).astype(F32)
    full = jnp.where(order == seat.astype(F32), 1.0, 0.0).astype(BF)
    part = jnp.where(order == over, 1.0, 0.0)
    even = jnp.where(seat % 2 == 0, part, 0.0).astype(BF)
    odd = jnp.where(seat % 2 == 1, part, 0.0).astype(BF)
    one, none = jnp.ones((tok, 1), BF), lambda n: jnp.zeros((tok, n), BF)
    second = jnp.concatenate([none(lay.width + 1), one, none(lay.low - lay.width - 2)], axis=1)
    flags = dot(part.astype(BF), second)
    for b in range(x_ref.shape[1] // lay.width):
        first = b * lay.width
        x = x_ref[:, first : first + lay.width]
        at = slice(b * rows, (b + 1) * rows)
        wide = jnp.concatenate([x, one, none(lay.low - lay.width - 1)], axis=1)
        s_ref[at, : lay.low] = (dot(full, wide) + flags).astype(BF)
        tail = jnp.concatenate([x[:, lay.point :], none(lay.short)], axis=1)
        s_ref[at, lay.low :] = (dot(even, x[:, : lay.point]) + dot(odd, tail)).astype(BF)


def gather_slots(lay, rows, x_ref, first, out):
    slots = out.shape[1]
    place = (iota((slots, x_ref.shape[0]), 0) + first).astype(F32)
    match = lambda row: jnp.where(row == place, 1.0, 0.0).astype(BF)
    got = dot(match(rows[0]), x_ref[:, : lay.width])
    rest = x_ref[:, lay.low :]
    left, right = dot(match(rows[1]), rest), dot(match(rows[2]), rest)
    extra = jnp.concatenate([left, right[:, : lay.width - lay.point]], axis=1)
    out[...] = (got + extra).astype(BF).T


def pick_more_kernel(lay, first, x_ref, row_ref, *outs):
    for out in outs:
        gather_slots(lay, [row_ref[k : k + 1] for k in range(3)], x_ref, first, out)
        first += out.shape[1]


def joined(refs):
    return jnp.concatenate([ref[...] for ref in refs], axis=1)


def spread_out(values, refs):
    first = 0
    for ref in refs:
        ref[...] = values[:, first : first + ref.shape[1]].astype(ref.dtype)
        first += ref.shape[1]


def pick_kernel(lay, x_ref, par_ref, row_ref, out):
    came, seats = x_ref.shape[0], lay.seats
    sources = came // seats
    bound = par_ref[0].astype(F32)
    start = lay.width // 128 * 128
    tail = x_ref[:, start : lay.low]
    choose = (iota((8, tail.shape[1]), 1) == iota((8, tail.shape[1]), 0) + lay.width - start)
    flags = dot(choose.astype(BF), tail, ((1,), (1,)))
    full, part = flags[0:1], flags[1:2]
    seat = iota((1, came), 1) % seats
    even = seat % 2 == 0
    owner = iota((sources, came), 0) == iota((sources, came), 1) // seats
    each = full + jnp.where(even, part, 0.0)
    counts = jnp.sum(jnp.where(owner, each, 0.0), axis=1, keepdims=True)
    counts = jnp.broadcast_to(counts, (sources, 128)).astype(BF)
    earlier = (iota((sources, sources), 1) < iota((sources, sources), 0)).astype(BF)
    before = dot(earlier, counts)[:, 0:1]
    base = jnp.sum(jnp.where(owner, before, 0.0), axis=0, keepdims=True)
    rank = base + seat.astype(F32)
    over = base + (seats + seat // 2).astype(F32)
    rank = jnp.where(jnp.logical_and(full > 0.5, rank < bound), rank, -1.0)
    over = jnp.where(jnp.logical_and(part > 0.5, over < bound), over, -1.0)
    evens, odds = jnp.where(even, over, -1.0), jnp.where(even, -1.0, over)
    nothing = jnp.full((5, came), -1.0, F32)
    row_ref[...] = jnp.concatenate([rank, evens, odds, nothing], axis=0)
    gather_slots(lay, (rank, evens, odds), x_ref, 0, out)


def relay_kernel(seen_ref, g_ref, u_ref, d_ref, go_ref, uo_ref, do_ref):
    del seen_ref
    blocks, width = go_ref.shape[0], go_ref.shape[2]
    for b in range(blocks):
        at = slice(b * width, (b + 1) * width)
        go_ref[b] = g_ref[:, at]
        uo_ref[b] = u_ref[:, at]
        do_ref[b] = d_ref[:, at].T


def gate_up(at, ahead, wg_ref, wu_ref, refs):
    gate = up = None
    pieces = len(refs) // len(ahead)
    for n, distance in enumerate(ahead):
        block = lax.rem(at + distance, wg_ref.shape[0])
        x = joined(refs[n * pieces : (n + 1) * pieces])
        g, u = dot(wg_ref[block], x), dot(wu_ref[block], x)
        gate, up = (g, u) if gate is None else (gate + g, up + u)
    return gate, up


def mid_kernel(ahead, at_ref, wg_ref, wu_ref, *refs):
    refs[-2][...], refs[-1][...] = gate_up(at_ref[0], ahead, wg_ref, wu_ref, refs[:-2])


def far_kernel(ahead, pieces, at_ref, wg_ref, wu_ref, wd_ref, g_ref, u_ref, *refs):
    ins, h_ref, outs = refs[: -pieces - 1], refs[-pieces - 1], refs[-pieces:]
    gate, up = gate_up(at_ref[0], ahead, wg_ref, wu_ref, ins)
    gate, up = gate + g_ref[...], up + u_ref[...]
    hidden = (gate * jax.nn.sigmoid(SWISH_SCALE * gate) * (up + 1.0)).astype(BF)
    h_ref[...] = hidden
    groups = wd_ref.shape[0]
    across = lax.rem(at_ref[0] + groups // 2, groups)
    spread_out(dot(wd_ref[across], hidden), outs)


def near_kernel(pieces, at_ref, h_ref, wd_ref, own_ref, *outs):
    hidden = h_ref[...]
    groups = wd_ref.shape[0]
    targets = ((0, (own_ref,)), (groups - 1, outs[:pieces]), (1, outs[pieces:]))
    for distance, refs in targets:
        block = lax.rem(at_ref[0] + distance, groups)
        spread_out(dot(wd_ref[block], hidden), refs)


def spots_kernel(row_ref, *outs):
    places = row_ref[...].T
    for k, out in enumerate(outs):
        out[...] = hot(places[:, k : k + 1], out.shape[1]).astype(BF)


def place_kernel(lay, pieces, whole_ref, even_ref, odd_ref, *refs):
    ins, z_ref = refs[:-1], refs[-1]
    columns = []
    for count in pieces:
        own, left, right = ins[0], ins[1 : 1 + count], ins[1 + count : 1 + 2 * count]
        ins = ins[1 + 2 * count :]
        total = own[...] + joined(left).astype(F32) + joined(right).astype(F32)
        columns.append(total.astype(BF))
    y = jnp.concatenate(columns, axis=1)
    came = z_ref.shape[0]
    none = lambda n: jnp.zeros((came, n), BF)
    rows = dot(whole_ref[...], y, ((1,), (1,))).astype(BF)
    z_ref[:, : lay.low] = jnp.concatenate([rows, none(lay.low - lay.width)], axis=1)
    left = dot(even_ref[...], y[: lay.point], ((1,), (1,))).astype(BF)
    right = dot(odd_ref[...], y[lay.point :], ((1,), (1,))).astype(BF)
    z_ref[:, lay.low :] = left + jnp.concatenate([right, none(lay.short)], axis=1)


def router_kernel(lay, id_ref, p_ref, w_ref):
    tok, seats = id_ref.shape[1], lay.seats
    ids, prob = id_ref[...].astype(F32).T, p_ref[...].T
    top = ids.shape[1]
    lane = iota((tok, lay.experts), 1).astype(F32)
    named = [ids[:, k : k + 1] == lane for k in range(top)]
    hits = jnp.zeros((tok, lay.experts), F32)
    for k in range(top):
        hits += jnp.where(named[k], 1.0, 0.0)
    earlier = (iota((tok, tok), 1) < iota((tok, tok), 0)).astype(BF)
    order = dot(earlier, hits.astype(BF))
    rows = lay.experts * seats
    kinds = [jnp.zeros((tok, rows), F32) for _ in range(3)]
    for k in range(top):
        seat = jnp.sum(jnp.where(named[k], order, 0.0), axis=1, keepdims=True)
        base = ids[:, k : k + 1] * seats
        full = jnp.where(seat < seats, base + seat, -1.0)
        over = jnp.where(seat < seats, -1.0, base + 2.0 * (seat - seats))
        odd = jnp.where(seat < seats, -1.0, over + 1.0)
        for n, place in enumerate((full, over, odd)):
            kinds[n] += hot(place, rows) * prob[:, k : k + 1]
    for n, kind in enumerate(kinds):
        high = kind.astype(BF)
        rest = kind - high.astype(F32)
        middle = rest.astype(BF)
        low = (rest - middle.astype(F32)).astype(BF)
        w_ref[n] = jnp.concatenate([high, middle, low], axis=0)


def mix_kernel(lay, b_ref, w_ref, o_ref):
    tok, rows = o_ref.shape[0], w_ref.shape[2]

    def weighted(n, block):
        three = dot(w_ref[n], block)
        return three[:tok] + three[tok : 2 * tok] + three[2 * tok :]

    for b in range(o_ref.shape[1] // lay.width):
        at = slice(b * rows, (b + 1) * rows)
        whole_rows = weighted(0, b_ref[at, : lay.width])
        rest = b_ref[at, lay.low :]
        left, right = weighted(1, rest), weighted(2, rest)
        extra = jnp.concatenate([left, right[:, : lay.width - lay.point]], axis=1)
        o_ref[:, b * lay.width : (b + 1) * lay.width] = (whole_rows + extra).astype(BF)


VMEM = pl.BlockSpec(memory_space=pltpu.VMEM)
SMEM = pl.BlockSpec(memory_space=pltpu.SMEM)
ANY = pl.BlockSpec(memory_space=pl.ANY)
shape = jax.ShapeDtypeStruct


class Layout:
    def __init__(self, width, experts, most):
        self.width, self.experts = width, experts
        self.seats = 8
        self.low = (width + 2 + 127) // 128 * 128
        self.point = (width // 2 + 127) // 128 * 128
        self.short = 2 * self.point - width
        self.lanes = self.low + self.point
        assert self.seats <= most <= self.seats * 3 // 2


def cost(flops, moved):
    return pl.CostEstimate(flops=flops, bytes_accessed=moved, transcendentals=0)


def grant(mebibytes):
    return pltpu.CompilerParams(vmem_limit_bytes=mebibytes << 20)


def run(kernel, ins, outs, work, scratch=(), mebibytes=12):
    return pl.pallas_call(
        kernel,
        out_shape=outs,
        in_specs=ins,
        out_specs=jax.tree.map(lambda _: VMEM, outs),
        scratch_shapes=scratch,
        cost_estimate=cost(*work),
        compiler_params=grant(mebibytes),
    )


def on_device(
    tokens, expert_ids, gate_probs, shed_blocks, partner, gate_weight, up_weight, down_weight
):
    tok, model = tokens.shape
    top = expert_ids.shape[1]
    experts = shed_blocks.shape[0]
    groups = lax.axis_size("attn")
    width = model // groups
    capacity = tok * top * groups
    block = capacity // 8
    slots = capacity + block * SHED_MOST
    units = gate_weight.shape[2]
    lay = Layout(width, experts, min(tok, 3 * tok * top // experts))
    devices = groups * experts
    came = devices * lay.seats
    me = lax.axis_index(EXPERT)
    bound = capacity - block * shed_blocks[partner[me]] + block * shed_blocks[me]
    par = bound.reshape(1).astype(jnp.int32)
    at = lax.axis_index("attn").astype(jnp.int32).reshape(1)

    def shifted(distance):
        pairs = [(i, (i + distance) % groups) for i in range(groups)]
        return lambda array: lax.ppermute(array, "attn", pairs)

    right, left = shifted(1), shifted(groups - 1)

    def exchange(rows):
        blocks = rows.reshape(devices, lay.seats, lay.lanes)
        moved = lax.all_to_all(blocks, ATTN_EXPERT, split_axis=0, concat_axis=0, tiled=True)
        return moved.reshape(came, lay.lanes)

    packed = shape((came, lay.lanes), BF)
    block_rows = experts * lay.seats
    block_rows = experts * lay.seats
    outgoing, seen = run(
        lambda *refs: send_kernel(lay, *refs),
        [VMEM] * 2,
        (packed, shape((8, 128), F32)),
        (2 * tok * came * width, 2 * came * width),
        mebibytes=60,
    )(tokens, expert_ids.T)
    arrived = exchange(outgoing)
    relaid = shape((groups, units, width), BF)
    step = 128
    rows_in = pl.BlockSpec((step, model), lambda i: (i, 0))
    rows_out = pl.BlockSpec((groups, step, width), lambda i: (0, i, 0))
    wg, wu, wd = pl.pallas_call(
        relay_kernel,
        grid=(pl.cdiv(units, step),),
        out_shape=(relaid, relaid, shape((groups, width, units), BF)),
        in_specs=[ANY] + [rows_in] * 3,
        out_specs=(rows_out, rows_out, pl.BlockSpec((groups, width, step), lambda i: (0, 0, i))),
        cost_estimate=cost(12 * slots * width * units, 12 * model * units),
        compiler_params=grant(60),
        name="relay",
    )(seen, gate_weight[0].T, up_weight[0].T, down_weight[0])
    arrived, wg, wu, wd = lax.optimization_barrier((arrived, wg, wu, wd))

    weights = run(
        lambda *refs: router_kernel(lay, *refs),
        [VMEM] * 2,
        shape((3, 3 * tok, block_rows), BF),
        (12 * tok * block_rows, 18 * tok * block_rows),
    )(expert_ids.T, gate_probs.T)
    part = slots // 2
    columns = shape((width, part), BF)
    cuts = (part // 3, part - part // 3)
    gather_work = (2 * slots * came * width, 2 * came * width)
    places, own_a = run(
        lambda *refs: pick_kernel(lay, *refs),
        [VMEM, SMEM],
        (shape((8, came), F32), columns),
        gather_work,
    )(arrived, par)
    own_b = run(
        lambda *refs: pick_more_kernel(lay, part, *refs),
        [VMEM] * 2,
        tuple(shape((width, n), BF) for n in cuts),
        gather_work,
    )(arrived, places)
    spot = shape((came, slots), BF)
    spots = run(spots_kernel, [VMEM], (spot,) * 3, (6 * came * slots, 6 * came * slots))(places)
    before, after, across = groups - 1, 1, groups // 2
    area = width * units
    rows = lambda n, kind: shape((n, part), kind)

    def mid(blocks, ahead):
        return run(
            lambda *refs: mid_kernel(ahead, *refs),
            [SMEM] + [VMEM] * (2 + len(blocks)),
            (rows(units, F32), rows(units, F32)),
            (4 * len(ahead) * part * area, 4 * len(ahead) * area),
        )(at, wg, wu, *blocks)

    def far(sums, blocks, ahead, sizes):
        count = 4 * len(ahead) + 2
        hidden, *shares = run(
            lambda *refs: far_kernel(ahead, len(sizes), *refs),
            [SMEM] + [VMEM] * (5 + len(blocks)),
            (rows(units, BF), *(shape((width, n), BF) for n in sizes)),
            (count * part * area, count * area),
        )(at, wg, wu, wd, *sums, *blocks)
        return hidden, shares

    def near(hidden, kinds, sizes):
        own, *shares = run(
            lambda *refs: near_kernel(len(sizes), *refs),
            [SMEM] + [VMEM] * 2,
            (rows(width, F32), *(shape((width, n), kind) for kind in kinds for n in sizes)),
            (6 * part * area, 6 * area),
        )(at, hidden, wd)
        return own, shares[: len(sizes)], shares[len(sizes) :]

    def add(mine, came):
        return (mine + came.astype(F32)).astype(BF)

    below_a, above_a = right(own_a), left(own_a)
    above_b = [left(own_b[0])]
    above_b += [left(own_b[1])]
    far_a = right(below_a)
    below_b = [right(piece) for piece in own_b]
    far_b = [left(above_b[0])]
    far_b += [left(above_b[1])]
    sums_a = mid((own_a, below_a, above_a), (0, before, after))
    hidden_a, (share_a,) = far(sums_a, (far_a,), (across,), (part,))
    crossed_a = right(share_a)
    mine_a, (left_a,), (right_a,) = near(hidden_a, (BF, F32), (part,))
    from_right_a = left(left_a)
    sums_b = mid((*own_b, *above_b), (0, after))
    hidden_b, share_b = far(sums_b, (*below_b, *far_b), (before, across), cuts)
    crossed_b = [left(piece) for piece in share_b]
    mine_b, left_b, right_b = near(hidden_b, (F32, BF), cuts)
    from_left_b = [right(piece) for piece in right_b]
    added_a = add(right_a, crossed_a)
    added_b = [add(mine, came) for mine, came in zip(left_b, crossed_b)]
    from_left_a = right(added_a)
    from_right_b = [left(piece) for piece in added_b]
    sums = (mine_a, from_left_a, from_right_a, mine_b, *from_left_b, *from_right_b)
    answers = run(
        lambda *refs: place_kernel(lay, (1, len(cuts)), *refs), [VMEM] * (3 + len(sums)), packed, gather_work
    )(*spots, *sums)
    return run(
        lambda *refs: mix_kernel(lay, *refs),
        [VMEM] * 2,
        shape((tok, model), BF),
        (6 * tok * came * width, 2 * came * width),
    )(exchange(answers), weights)


def solution(mesh):
    split = Mesh(
        mesh.devices.reshape(mesh.shape["attn"], 4, 4, 2),
        ("attn", "expert_0", "expert_1", "expert_2"),
    )
    return jax.shard_map(
        on_device,
        mesh=split,
        in_specs=(
            P(ATTN_EXPERT, None),
            P(ATTN_EXPERT, None),
            P(ATTN_EXPERT, None),
            P(),
            P(),
            P(EXPERT, None, "attn"),
            P(EXPERT, None, "attn"),
            P(EXPERT, "attn", None),
        ),
        out_specs=P(ATTN_EXPERT, None),
        check_vma=False,
    )
```
